32 devices in a mesh: section: 4 (over y, x), dp: 8 (over z, core).
Axes of the slice: x: 2, y: 2, z: 4, core: 2. Of those that a mesh axis runs over, the one named last changes fastest.
Arguments:
- saved_inputs: bfloat16 [4, 2, 1024, 320], P('section', None, 'dp'), may hold values from -6 to 6
- timesteps: int32 [2, 1024], P(None, 'dp'), may hold values from 0 to 999
- time_table: bfloat16 [1000, 320], replicated, may hold values from -6 to 6
- skip_weight: bfloat16 [4, 320, 320], P('section'), may hold values from -0.3125 to 0.3125
- ff_in: bfloat16 [4, 1280, 320], P('section'), may hold values from -0.3125 to 0.3125
- ff_out: bfloat16 [4, 1280, 320], P('section'), may hold values from -0.15625 to 0.15625
- output_cotangent: bfloat16 [2, 1024, 320], P(None, 'dp'), may hold values from -6 to 6
Outputs:
- input_grads: bfloat16 [4, 2, 1024, 320], P('section', None, 'dp')
- skip_weight_grad: float32 [4, 102400], P('section', 'dp')
- ff_in_grad: float32 [4, 1280, 320], P('section', 'dp')
- ff_out_grad: float32 [4, 1280, 320], P('section', 'dp')
The draws below stay inside these ranges and needn't reach their ends.
All inputs are finite; a program needn't handle non-finite values.
Results may differ from the reference program's by a relative error of at most 0.01.
Values may be sent and summed in bfloat16 or wider, within the bound.
No kernel may reach another device: no remote copies, remote signals or barrier semaphores. Data moves between devices by JAX's collectives and lax.ppermute only.
A program may use at most 128 MiB of HBM per device.

```python
import jax
import jax.numpy as jnp
from jax import lax

C = 320
F = 1280
NT = 1000
M = 2
ROWS = 1024
N_SECTION = 4


def touch_ends(values, own_key, low, largest):
    longest = values.shape.index(max(values.shape))
    spots = []
    for shift in (0, 1):
        where = [jax.random.randint(jax.random.fold_in(own_key, axis), (), 0, length) for axis, length in enumerate(values.shape)]
        where[longest] = (where[longest] + shift) % values.shape[longest]
        spots.append(tuple(where))
    return values.at[spots[0]].set(low).at[spots[1]].set(largest)


def block_levels(stream_key, shape, cuts, least, top_value):
    def one(axis_at, blocks):
        draws = jax.random.uniform(jax.random.fold_in(jax.random.fold_in(stream_key, 6), axis_at), (blocks,), jnp.float32, least / len(cuts), top_value / len(cuts))
        return jnp.repeat(jnp.exp(draws), shape[axis_at] // blocks).reshape((-1,) + (1,) * (len(shape) - axis_at - 1))

    gain = one(*cuts[0])
    for cut in cuts[1:]:
        gain = gain * one(*cut)
    return gain


def normal_values(stream_key, extent, spread, reach, shards=(), kind=jnp.bfloat16):
    array = spread * jax.random.normal(stream_key, extent, jnp.float32)
    if shards:
        array = array * block_levels(stream_key, extent, shards, -0.22, 0.18)
    return jnp.clip(array, -reach, reach).astype(kind)


def setup_inputs(seed: int = 0) -> dict:
    key_list = jax.random.split(jax.random.key(seed), 8)
    return {
        "saved_inputs": normal_values(key_list[0], (N_SECTION, M, ROWS, C), 1.0, 6.0, ((0, 4), (2, 8))),
        "timesteps": touch_ends(jax.random.randint(key_list[1], (M, ROWS), 0, NT), jax.random.fold_in(key_list[1], 1), 0, NT - 1).astype(jnp.int32),
        "time_table": normal_values(key_list[2], (NT, C), 1.0, 6.0),
        "skip_weight": normal_values(key_list[3], (N_SECTION, C, C), C ** -0.5, 0.3125, ((0, 4),)),
        "ff_in": normal_values(key_list[4], (N_SECTION, F, C), C ** -0.5, 0.3125, ((0, 4),)),
        "ff_out": normal_values(key_list[5], (N_SECTION, F, C), F ** -0.5, 0.15625, ((0, 4),)),
        "output_cotangent": normal_values(key_list[6], (M, ROWS, C), 1.0, 6.0, ((1, 8),)),
    }


EPS = 1e-06

def contract(left, right, dims):
    return lax.dot_general(left, right, ((dims[0], dims[1]), ((), ())), preferred_element_type=jnp.float32)

def forward(inputs, source, w_skip, w_in, w_out):
    united = inputs.astype(jnp.float32) + jnp.dot(source, w_skip, preferred_element_type=jnp.float32)
    recip = lax.rsqrt(lax.optimization_barrier(jnp.mean(united * united, axis=-1, keepdims=True)) + EPS)
    normed = (united * recip).astype(jnp.bfloat16)
    preact = contract(normed, w_in, ((1,), (1,)))
    active = jax.nn.silu(preact).astype(jnp.bfloat16)
    output = united + jnp.dot(active, w_out, preferred_element_type=jnp.float32)
    return (united, recip, normed, preact, active, output)

def backward(grad_out, inputs, source, w_skip, w_in, w_out):
    united, recip, normed, preact, active, output = forward(inputs, source, w_skip, w_in, w_out)
    grad_low = grad_out.astype(jnp.bfloat16)
    grad_act = contract(grad_low, w_out, ((1,), (1,)))
    sigma = jax.nn.sigmoid(preact)
    grad_pre = (grad_act * sigma * (1.0 + preact * (1.0 - sigma))).astype(jnp.bfloat16)
    d_in = contract(grad_pre, normed, ((0,), (0,)))
    d_out = contract(active, grad_low, ((0,), (0,)))
    grad_norm = jnp.dot(grad_pre, w_in, preferred_element_type=jnp.float32)
    grad_united = grad_out + recip * grad_norm - united * recip ** 3 * lax.optimization_barrier(jnp.mean(grad_norm * united, axis=-1, keepdims=True))
    united_low = grad_united.astype(jnp.bfloat16)
    d_skip = contract(source, united_low, ((0,), (0,)))
    grad_source = contract(united_low, w_skip, ((1,), (1,))).astype(jnp.bfloat16)
    return (united_low, grad_source, d_in, d_out, d_skip)

def reference(saved_inputs, timesteps, time_table, skip_weight, ff_in, ff_out, output_cotangent):
    grads = [[None] * M for section in range(4)]
    sum_in = [jnp.zeros((F, C), jnp.float32) for section in range(4)]
    sum_out = [jnp.zeros((F, C), jnp.float32) for section in range(4)]
    sum_skip = [jnp.zeros((C, C), jnp.float32) for section in range(4)]
    for micro in range(M):
        embeds = jnp.take(time_table, timesteps[micro], axis=0)
        values = []
        for section in range(2):
            output = forward(saved_inputs[section, micro], embeds, skip_weight[section], ff_in[section], ff_out[section])[5]
            values.append(output.astype(jnp.bfloat16))
        pending = [None, None]
        chain = None
        for section in (3, 2, 1, 0):
            if section == 3:
                grad_out = output_cotangent[micro].astype(jnp.float32)
            elif section == 2:
                grad_out = chain.astype(jnp.float32)
            else:
                grad_out = chain.astype(jnp.float32) + pending[section].astype(jnp.float32)
            source = values[3 - section] if section >= 2 else embeds
            parts = backward(grad_out, saved_inputs[section, micro], source, skip_weight[section], ff_in[section], ff_out[section])
            chain = parts[0]
            if section >= 2:
                pending[3 - section] = parts[1]
            grads[section][micro] = chain
            sum_in[section] = sum_in[section] + parts[2]
            sum_out[section] = sum_out[section] + parts[3]
            sum_skip[section] = sum_skip[section] + parts[4]
    input_grads = jnp.stack([jnp.stack(grads[section]) for section in range(4)])
    skip_grad = jnp.stack([sum_skip[section].reshape(-1) for section in range(4)])
    return (input_grads, skip_grad, jnp.stack(sum_in), jnp.stack(sum_out))
```

```python
import jax
import jax.numpy as jnp
from jax import lax
from jax.sharding import PartitionSpec as P

EPS = 1e-06
LOW = jnp.bfloat16


def contract(left, right, dims):
    return lax.dot_general(
        left, right, ((dims[0], dims[1]), ((), ())), preferred_element_type=jnp.float32
    )


def forward_norm(inputs, source, w_skip, w_in):
    united = inputs.astype(jnp.float32) + jnp.dot(
        source, w_skip, preferred_element_type=jnp.float32
    )
    recip = lax.rsqrt(jnp.mean(united * united, axis=-1, keepdims=True) + EPS)
    normed = (united * recip).astype(LOW)
    preact = contract(normed, w_in, ((1,), (1,)))
    return united, recip, normed, preact


def slope_of(preact):
    sigma = jax.nn.sigmoid(preact)
    return sigma * (1.0 + preact * (1.0 - sigma))


def stage(grad_out, united, recip, slope, w_in, w_out):
    grad_low = grad_out.astype(LOW)
    grad_act = contract(grad_low, w_out, ((1,), (1,)))
    grad_pre = (grad_act * slope).astype(LOW)
    grad_norm = jnp.dot(grad_pre, w_in, preferred_element_type=jnp.float32)
    grad_united = (
        grad_out
        + recip * grad_norm
        - united * recip**3 * jnp.mean(grad_norm * united, axis=-1, keepdims=True)
    )
    return grad_low, grad_pre, grad_united.astype(LOW)


def exchange(value, count, mask):
    return lax.ppermute(value, "dp", [(i, i ^ mask) for i in range(count)])


def gather_blocks(value, count):
    blocks = [value]
    masks = [k for k in range(2, count, 2)]
    blocks = blocks + [exchange(value, count, mask) for mask in masks]
    other = [exchange(block, count, 1) for block in blocks]
    return jnp.concatenate(blocks + other, axis=0)


def scatter_sum(partial, count):
    place = lax.axis_index("dp")
    core = place % 2
    pairs = partial.reshape(count // 2, 2, -1)
    give = lax.dynamic_index_in_dim(pairs, 1 - core, 1, keepdims=False).astype(LOW)
    keep = lax.dynamic_index_in_dim(pairs, core, 1, keepdims=False)
    joined = keep + exchange(give, count, 1).astype(jnp.float32)
    chip = place // 2
    total = lax.dynamic_index_in_dim(joined, chip, 0, keepdims=False)
    for mask in range(1, count // 2):
        piece = lax.dynamic_index_in_dim(joined, chip ^ mask, 0, keepdims=False)
        total = total + exchange(piece.astype(LOW), count, 2 * mask).astype(jnp.float32)
    return total


def shards(saved_inputs, timesteps, time_table, skip_weight, ff_in, ff_out, output_cotangent):
    section = lax.axis_index("section")
    count = lax.axis_size("dp")
    n_micro = saved_inputs.shape[1]
    width = saved_inputs.shape[3]
    rows = n_micro * saved_inputs.shape[2]
    hidden = ff_in.shape[1]
    inputs = saved_inputs.reshape(rows, width)
    w_skip = skip_weight[0]
    w_in = ff_in[0]
    w_out = ff_out[0]
    levels = lax.broadcasted_iota(jnp.int32, (1, time_table.shape[0]), 1)
    onehot = (timesteps.reshape(rows)[:, None] == levels).astype(LOW)
    embed = jnp.dot(onehot, time_table, preferred_element_type=jnp.float32).astype(LOW)

    united, recip, normed, preact = forward_norm(inputs, embed, w_skip, w_in)
    active = jax.nn.silu(preact).astype(LOW)
    value = (united + jnp.dot(active, w_out, preferred_element_type=jnp.float32)).astype(LOW)
    received = lax.ppermute(value, "section", [(0, 3), (1, 2)])
    w_mirror = lax.ppermute(w_skip, "section", [(2, 1)])
    source = jnp.where(section >= 2, received, embed)
    united, recip, normed, preact = forward_norm(inputs, source, w_skip, w_in)
    slope = slope_of(preact)

    grad_out = output_cotangent.reshape(rows, width).astype(jnp.float32)
    grad_low = None
    for tick in range(4):
        owner = 3 - tick
        low, pre, chain = stage(grad_out, united, recip, slope, w_in, w_out)
        if tick == 0:
            grad_low, grad_pre, kept = low, pre, chain
            back = contract(chain, w_skip, ((1,), (1,))).astype(LOW)
            skip_far = lax.ppermute(back, "section", [(3, 0)])
        else:
            mine = section == owner
            grad_low = jnp.where(mine, low, grad_low)
            grad_pre = jnp.where(mine, pre, grad_pre)
            kept = jnp.where(mine, chain, kept)
        if tick < 3:
            chain = lax.ppermute(chain, "section", [(owner, owner - 1)])
            grad_out = chain.astype(jnp.float32)
            if tick == 1:
                back = contract(chain, w_mirror, ((1,), (1,))).astype(LOW)
                grad_out = grad_out + back.astype(jnp.float32)
            if tick == 2:
                grad_out = grad_out + skip_far.astype(jnp.float32)

    skip_part = contract(source, kept, ((0,), (0,)))
    if count * rows <= 4096:
        part = hidden // count
        start = lax.axis_index("dp") * part
        own_in = lax.dynamic_slice_in_dim(w_in, start, part, 0)
        own_out = lax.dynamic_slice_in_dim(w_out, start, part, 0)
        normed_all = gather_blocks(normed, count)
        pre_all = contract(normed_all, own_in, ((1,), (1,)))
        act_all = jax.nn.silu(pre_all).astype(LOW)
        slope_all = slope_of(pre_all)
        low_all = gather_blocks(grad_low, count)
        grad_pre_all = (contract(low_all, own_out, ((1,), (1,))) * slope_all).astype(LOW)
        grad_in = contract(grad_pre_all, normed_all, ((0,), (0,)))
        grad_out_w = contract(act_all, low_all, ((0,), (0,)))
        grad_skip = scatter_sum(skip_part.reshape(count, -1), count)
    else:
        active = jax.nn.silu(preact).astype(LOW)
        grad_in, grad_out_w, grad_skip = (
            lax.psum_scatter(value, "dp", scatter_dimension=0, tiled=True)
            for value in (
                contract(grad_pre, normed, ((0,), (0,))),
                contract(active, grad_low, ((0,), (0,))),
                skip_part.reshape(-1),
            )
        )
    return (kept.reshape(saved_inputs.shape), grad_skip[None], grad_in[None], grad_out_w[None])


def solution(mesh):
    in_specs = (
        P("section", None, "dp", None),
        P(None, "dp"),
        P(),
        P("section", None, None),
        P("section", None, None),
        P("section", None, None),
        P(None, "dp", None),
    )
    out_specs = (
        P("section", None, "dp", None),
        P("section", "dp"),
        P("section", "dp", None),
        P("section", "dp", None),
    )
    return jax.shard_map(shards, mesh=mesh, in_specs=in_specs, out_specs=out_specs, check_vma=False)
```

```python
import jax
import jax.numpy as jnp
from jax import lax
from jax.experimental import pallas as pl
from jax.experimental.pallas import tpu as pltpu
from jax.sharding import PartitionSpec as P

EPS = 1e-06
LOW = jnp.bfloat16
F32 = jnp.float32
VMEM_BYTES = 20 * 1024 * 1024


def contract(left, right, dims):
    return lax.dot_general(left, right, ((dims[0], dims[1]), ((), ())), preferred_element_type=F32)


def dot(left, right, on_left, on_right):
    return contract(left, right, ((on_left,), (on_right,)))


def call(body, outs, *args):
    specs = [
        pl.BlockSpec(memory_space=pltpu.SMEM if arg.ndim == 1 else pltpu.VMEM) for arg in args
    ]
    return pl.pallas_call(
        body,
        out_shape=[jax.ShapeDtypeStruct(shape, kind) for shape, kind in outs],
        in_specs=specs,
        out_specs=[pl.BlockSpec(memory_space=pltpu.VMEM) for _ in outs],
        compiler_params=pltpu.CompilerParams(vmem_limit_bytes=VMEM_BYTES),
    )(*args)


def side_by_side(ref):
    return jnp.concatenate([ref[m] for m in range(ref.shape[0])], axis=1)


def norm_of(united):
    return lax.rsqrt(jnp.mean(united * united, axis=0, keepdims=True) + EPS)


def sigmoid(value):
    return 1.0 / (1.0 + jnp.exp(-value))


def encode_body(times, table, inputs, w_skip, w_in, w_out, embed_out, value_out):
    levels = lax.broadcasted_iota(jnp.int32, (table.shape[1], times.shape[1]), 0)
    hot = [
        jnp.where(levels == times[m : m + 1, :], 1.0, 0.0).astype(LOW)
        for m in range(times.shape[0])
    ]
    embed = dot(table[...], jnp.concatenate(hot, axis=1), 1, 0).astype(LOW)
    embed_out[...] = embed
    united = side_by_side(inputs).astype(F32) + dot(w_skip[...], embed, 0, 0)
    normed = (united * norm_of(united)).astype(LOW)
    preact = dot(w_in[...], normed, 0, 0)
    active = (preact * sigmoid(preact)).astype(LOW)
    value_out[...] = (united + dot(w_out[...], active, 1, 0)).astype(LOW)


def back_through(grad_out, grad_low, united, slope, w_in, w_out):
    grad_pre = (dot(w_out[...], grad_low, 0, 0) * slope).astype(LOW)
    grad_norm = dot(w_in[...], grad_pre, 1, 0)
    recip = norm_of(united)
    along = jnp.mean(grad_norm * united, axis=0, keepdims=True)
    return (grad_out + recip * grad_norm - united * (recip * recip * recip * along)).astype(LOW)


def decode_body(
    flags, received, embed, inputs, upstream, w_skip, w_in, w_out,
    source_out, normed_out, united_out, slope_out, chain_out,
):
    source = jnp.where(flags[0] >= 2, received[...], embed[...])
    source_out[...] = source
    united = side_by_side(inputs).astype(F32) + dot(w_skip[...], source, 0, 0)
    united_out[...] = united
    normed = (united * norm_of(united)).astype(LOW)
    normed_out[...] = normed
    preact = dot(w_in[...], normed, 0, 0)
    sigma = sigmoid(preact)
    slope = sigma * (1.0 + preact * (1.0 - sigma))
    slope_out[...] = slope
    low = side_by_side(upstream)
    chain_out[...] = back_through(low.astype(F32), low, united, slope, w_in, w_out)


def back_body(chain, w_skip, back_out):
    back_out[...] = dot(w_skip[...], chain[...], 1, 0).astype(LOW)


def tick_body(received, united, slope, w_in, w_out, chain_out):
    low = received[...]
    chain_out[...] = back_through(low.astype(F32), low, united[...], slope[...], w_in, w_out)


def mirror_tick_body(received, w_mirror, united, slope, w_in, w_out, chain_out, low_out):
    back = dot(w_mirror[...], received[...], 1, 0).astype(LOW)
    grad_out = received[...].astype(F32) + back.astype(F32)
    low = grad_out.astype(LOW)
    low_out[...] = low
    chain_out[...] = back_through(grad_out, low, united[...], slope[...], w_in, w_out)


def pick_body(flags, received, skip_far, low_1, low_2, upstream, grad_low_out):
    own = (received[...].astype(F32) + skip_far[...].astype(F32)).astype(LOW)
    section = flags[0]
    own = jnp.where(section == 1, low_1[...], own)
    own = jnp.where(section == 2, low_2[...], own)
    grad_low_out[...] = jnp.where(section == 3, side_by_side(upstream), own)


def last_body(
    flags, received, skip_far, united, slope, w_in, w_out, source, chain_1, chain_2, chain_3,
    kept_out, keep_out, give_out, parts,
):
    grad_out = received[...].astype(F32) + skip_far[...].astype(F32)
    low = grad_out.astype(LOW)
    section = flags[0]
    kept = back_through(grad_out, low, united[...], slope[...], w_in, w_out)
    kept = jnp.where(section == 1, chain_1[...], kept)
    kept = jnp.where(section == 2, chain_2[...], kept)
    kept = jnp.where(section == 3, chain_3[...], kept)
    span = kept_out.shape[2]
    for m in range(kept_out.shape[0]):
        kept_out[m] = kept[:, m * span : (m + 1) * span]
    partial = dot(source[...], kept, 1, 1)
    size = parts.shape[2]
    for block in range(parts.shape[0]):
        for core in range(2):
            first = (2 * block + core) * size
            parts[block, core] = partial[first : first + size, :]
    core = flags[1]
    for block in range(parts.shape[0]):
        keep_out[block] = parts[block, core]
        give_out[block] = parts[block, 1 - core].astype(LOW)


def join_body(flags, keep, given, own_out, *piece_outs):
    chip = flags[2]
    own_out[...] = keep[chip] + given[chip].astype(F32)
    for mask, piece_out in enumerate(piece_outs, 1):
        far = chip ^ mask
        piece_out[...] = (keep[far] + given[far].astype(F32)).astype(LOW)


def slice_forward_body(own_in, *refs):
    count = len(refs) // 3
    for block in range(count):
        preact = dot(own_in[...], refs[block][...], 0, 0)
        sigma = sigmoid(preact)
        refs[count + block][...] = (preact * sigma).astype(LOW)
        refs[2 * count + block][...] = sigma * (1.0 + preact * (1.0 - sigma))


def slice_grad_body(own_out, *refs):
    count = (len(refs) - 2) // 4
    total_in = total_out = None
    for block in range(count):
        normed, active, slope, low = (refs[block + part * count][...] for part in range(4))
        grad_pre = (dot(own_out[...], low, 0, 0) * slope).astype(LOW)
        part_in = dot(grad_pre, normed, 1, 1)
        part_out = dot(active, low, 1, 1)
        total_in = part_in if total_in is None else total_in + part_in
        total_out = part_out if total_out is None else total_out + part_out
    refs[-2][...] = total_in
    refs[-1][...] = total_out


def exchange(value, count, mask):
    return lax.ppermute(value, "dp", [(i, i ^ mask) for i in range(count)])


def gather_blocks(value, count):
    blocks = [value] + [exchange(value, count, mask) for mask in range(2, count, 2)]
    return blocks + [exchange(block, count, 1) for block in blocks]


def shards(saved_inputs, timesteps, time_table, skip_weight, ff_in, ff_out, output_cotangent):
    section = lax.axis_index("section")
    place = lax.axis_index("dp")
    count = lax.axis_size("dp")
    n_micro = saved_inputs.shape[1]
    width = saved_inputs.shape[3]
    span = saved_inputs.shape[2]
    rows = n_micro * span
    hidden = ff_in.shape[1]
    flags = jnp.stack([section, place % 2, place // 2]).astype(jnp.int32)
    inputs = jnp.swapaxes(saved_inputs[0], 1, 2)
    upstream = jnp.swapaxes(output_cotangent, 1, 2)
    table = time_table.T
    w_skip = skip_weight[0]
    w_in = ff_in[0].T
    w_out = ff_out[0].T
    low = ((width, rows), LOW)
    wide = ((hidden, rows), F32)

    embed, value = call(encode_body, [low, low], timesteps, table, inputs, w_skip, w_in, w_out)
    received = lax.ppermute(value, "section", [(0, 3), (1, 2)])
    source, normed, united, slope, chain_3 = call(
        decode_body, [low, low, ((width, rows), F32), wide, low],
        flags, received, embed, inputs, upstream, w_skip, w_in, w_out,
    )
    chain = lax.ppermute(chain_3, "section", [(3, 2)])
    w_mirror = lax.ppermute(w_skip, "section", [(2, 1)])
    (back,) = call(back_body, [low], chain_3, w_skip)
    skip_far = lax.ppermute(back, "section", [(3, 0)])
    low_2 = chain
    (chain_2,) = call(tick_body, [low], chain, united, slope, w_in, w_out)
    chain = lax.ppermute(chain_2, "section", [(2, 1)])
    chain_1, low_1 = call(
        mirror_tick_body, [low, low], chain, w_mirror, united, slope, w_in, w_out
    )
    chain = lax.ppermute(chain_1, "section", [(1, 0)])
    (grad_low,) = call(pick_body, [low], flags, chain, skip_far, low_1, low_2, upstream)

    sliced = count * rows <= 4096 and count % 2 == 0 and width % count == 0
    if not sliced:
        return by_reduction(
            section, flags, chain, skip_far, united, slope, w_in, w_out, source, normed, grad_low,
            (chain_1, chain_2, chain_3), saved_inputs.shape,
        )

    part = hidden // count
    own_in = lax.dynamic_slice_in_dim(w_in, place * part, part, 1)
    own_out = lax.dynamic_slice_in_dim(w_out, place * part, part, 1)
    normed_all = gather_blocks(normed, count)
    forward_all = call(
        slice_forward_body, [((part, rows), LOW)] * count + [((part, rows), F32)] * count,
        own_in, *normed_all,
    )
    low_all = gather_blocks(grad_low, count)

    block = ((count // 2, width // count, width), F32)
    kept, keep, give = pl.pallas_call(
        last_body,
        out_shape=[
            jax.ShapeDtypeStruct((n_micro, width, span), LOW),
            jax.ShapeDtypeStruct(*block),
            jax.ShapeDtypeStruct(block[0], LOW),
        ],
        in_specs=[pl.BlockSpec(memory_space=pltpu.SMEM)]
        + [pl.BlockSpec(memory_space=pltpu.VMEM)] * 10,
        out_specs=[pl.BlockSpec(memory_space=pltpu.VMEM)] * 3,
        scratch_shapes=[pltpu.VMEM((count // 2, 2, width // count, width), F32)],
        compiler_params=pltpu.CompilerParams(vmem_limit_bytes=VMEM_BYTES),
    )(flags, chain, skip_far, united, slope, w_in, w_out, source, chain_1, chain_2, chain_3)
    given = exchange(give, count, 1)
    piece = block[0][1:]
    pieces = call(
        join_body, [(piece, F32)] + [(piece, LOW)] * (count // 2 - 1), flags, keep, given
    )
    grad_skip = pieces[0]
    for mask in range(1, count // 2):
        grad_skip = grad_skip + exchange(pieces[mask], count, 2 * mask).astype(F32)
    grad_in, grad_out_w = call(
        slice_grad_body, [((part, width), F32)] * 2, own_out, *normed_all, *forward_all, *low_all
    )
    kept = jnp.swapaxes(kept, 1, 2)
    return (kept[None], grad_skip.reshape(1, -1), grad_in[None], grad_out_w[None])


def by_reduction(
    section, flags, chain, skip_far, united, slope, w_in, w_out, source, normed, grad_low, chains,
    shape,
):
    grad_out = chain.astype(F32) + skip_far.astype(F32)
    grad_pre = (dot(w_out, grad_low, 0, 0) * slope).astype(LOW)
    preact = dot(w_in, normed, 0, 0)
    active = (preact * jax.nn.sigmoid(preact)).astype(LOW)
    own_pre = (dot(w_out, grad_out.astype(LOW), 0, 0) * slope).astype(LOW)
    grad_norm = dot(w_in, own_pre, 1, 0)
    recip = norm_of(united)
    along = jnp.mean(grad_norm * united, axis=0, keepdims=True)
    kept = (grad_out + recip * grad_norm - united * (recip * recip * recip * along)).astype(LOW)
    for owner, other in enumerate(chains, 1):
        kept = jnp.where(section == owner, other, kept)
    grad_in, grad_out_w, grad_skip = (
        lax.psum_scatter(value, "dp", scatter_dimension=0, tiled=True)
        for value in (
            dot(grad_pre, normed, 1, 1),
            dot(active, grad_low, 1, 1),
            dot(source, kept, 1, 1).reshape(-1),
        )
    )
    kept = kept.reshape(shape[3], shape[1], shape[2]).transpose(1, 2, 0)
    return (kept[None], grad_skip[None], grad_in[None], grad_out_w[None])


def solution(mesh):
    in_specs = (
        P("section", None, "dp", None),
        P(None, "dp"),
        P(),
        P("section", None, None),
        P("section", None, None),
        P("section", None, None),
        P(None, "dp", None),
    )
    out_specs = (
        P("section", None, "dp", None),
        P("section", "dp"),
        P("section", "dp", None),
        P("section", "dp", None),
    )
    return jax.shard_map(shards, mesh=mesh, in_specs=in_specs, out_specs=out_specs, check_vma=False)
```

```python
import jax
import jax.numpy as jnp
from jax import lax
from jax.experimental import pallas as pl
from jax.experimental.pallas import tpu as pltpu
from jax.sharding import PartitionSpec as P


EPS = 1e-06
LOW = jnp.bfloat16
F32 = jnp.float32
VMEM_BYTES = 20 * 1024 * 1024


def contract(left, right, dims):
    return lax.dot_general(left, right, ((dims[0], dims[1]), ((), ())), preferred_element_type=F32)


def dot(left, right, on_left, on_right):
    return contract(left, right, ((on_left,), (on_right,)))


def call(body, outs, *args, scratch=(), far=()):
    places = [
        pltpu.SMEM if arg.ndim == 1 else pltpu.HBM if index in far else pltpu.VMEM
        for index, arg in enumerate(args)
    ]
    args = [
        pltpu.with_memory_space_constraint(arg, pltpu.HBM) if index in far else arg
        for index, arg in enumerate(args)
    ]
    return pl.pallas_call(
        body,
        out_shape=[jax.ShapeDtypeStruct(shape, kind) for shape, kind in outs],
        in_specs=[pl.BlockSpec(memory_space=place) for place in places],
        out_specs=[pl.BlockSpec(memory_space=pltpu.VMEM) for _ in outs],
        scratch_shapes=list(scratch),
        compiler_params=pltpu.CompilerParams(vmem_limit_bytes=VMEM_BYTES),
    )(*args)


def side_by_side(ref):
    return jnp.concatenate([ref[m] for m in range(ref.shape[0])], axis=1)


def norm_of(united):
    return lax.rsqrt(jnp.mean(united * united, axis=0, keepdims=True) + EPS)


def sigmoid(value):
    return 1.0 / (1.0 + jnp.exp(-value))


def encode_body(*refs):
    distant, (embed_out, value_out), local, sems = refs[:6], refs[6:8], refs[8:14], refs[14]
    copies = [
        pltpu.make_async_copy(source, target, sems.at[index])
        for index, (source, target) in enumerate(zip(distant, local))
    ]
    for copy in copies:
        copy.start()
    times, table, w_skip, inputs, w_in, w_out = local
    copies[0].wait()
    levels = lax.broadcasted_iota(jnp.int32, (table.shape[1], times.shape[1]), 0)
    hot = [
        jnp.where(levels == times[m : m + 1, :], 1.0, 0.0).astype(LOW)
        for m in range(times.shape[0])
    ]
    copies[1].wait()
    embed = dot(table[...], jnp.concatenate(hot, axis=1), 1, 0).astype(LOW)
    embed_out[...] = embed
    copies[2].wait()
    copies[3].wait()
    united = side_by_side(inputs).astype(F32) + dot(w_skip[...], embed, 0, 0)
    normed = (united * norm_of(united)).astype(LOW)
    copies[4].wait()
    preact = dot(w_in[...], normed, 0, 0)
    active = (preact * sigmoid(preact)).astype(LOW)
    copies[5].wait()
    value_out[...] = (united + dot(w_out[...], active, 1, 0)).astype(LOW)


def early_body(upstream, w_out, low_out, grad_act_out):
    low = side_by_side(upstream)
    low_out[...] = low
    grad_act_out[...] = dot(w_out[...], low, 0, 0)


def back_through(grad_out, grad_act, united, slope, w_in):
    grad_pre = (grad_act * slope).astype(LOW)
    grad_norm = dot(w_in[...], grad_pre, 1, 0)
    recip = norm_of(united)
    along = jnp.mean(grad_norm * united, axis=0, keepdims=True)
    return (grad_out + recip * grad_norm - united * (recip * recip * recip * along)).astype(LOW)


def decode_body(
    received, embed, inputs, top_low, grad_act, w_skip, w_in,
    source_out, normed_out, united_out, slope_out, chain_out,
):
    source = jnp.where(lax.axis_index("section") >= 2, received[...], embed[...])
    source_out[...] = source
    united = side_by_side(inputs).astype(F32) + dot(w_skip[...], source, 0, 0)
    united_out[...] = united
    normed = (united * norm_of(united)).astype(LOW)
    normed_out[...] = normed
    preact = dot(w_in[...], normed, 0, 0)
    sigma = sigmoid(preact)
    slope = sigma * (1.0 + preact * (1.0 - sigma))
    slope_out[...] = slope
    chain_out[...] = back_through(top_low[...].astype(F32), grad_act[...], united, slope, w_in)


def back_body(chain, w_skip, back_out):
    back_out[...] = dot(w_skip[...], chain[...], 1, 0).astype(LOW)


def tick_body(received, united, slope, w_in, w_out, chain_out):
    low = received[...]
    grad_act = dot(w_out[...], low, 0, 0)
    chain_out[...] = back_through(low.astype(F32), grad_act, united[...], slope[...], w_in)


def mirror_tick_body(
    received, w_mirror, united, slope, w_in, w_out, skip_far, back_2, chain_2, chain_3,
    top_low, chain_out, low_out, next_out,
):
    back = dot(w_mirror[...], received[...], 1, 0).astype(LOW)
    grad_out = received[...].astype(F32) + back.astype(F32)
    low = grad_out.astype(LOW)
    low_out[...] = low
    grad_act = dot(w_out[...], low, 0, 0)
    chain = back_through(grad_out, grad_act, united[...], slope[...], w_in)
    chain_out[...] = chain
    section = lax.axis_index("section")
    ahead = (chain.astype(F32) + skip_far[...].astype(F32)).astype(LOW)
    ahead = jnp.where(
        section == 2, (chain_2[...].astype(F32) + back_2[...].astype(F32)).astype(LOW), ahead
    )
    ahead = jnp.where(section == 3, chain_3[...], ahead)
    next_out[...] = jnp.where(section == 0, top_low[...], ahead)


def pick_body(received, skip_far, low_1, low_2, top_low, grad_low_out):
    own = (received[...].astype(F32) + skip_far[...].astype(F32)).astype(LOW)
    section = lax.axis_index("section")
    own = jnp.where(section == 1, low_1[...], own)
    own = jnp.where(section == 2, low_2[...], own)
    grad_low_out[...] = jnp.where(section == 3, top_low[...], own)


def last_body(
    grad_low, received, skip_far, united, slope, w_in, w_out, source, chain_1, chain_2,
    chain_3, kept_out, keep_out, give_out,
):
    grad_out = received[...].astype(F32) + skip_far[...].astype(F32)
    grad_act = dot(w_out[...], grad_low[...], 0, 0)
    section = lax.axis_index("section")
    kept = back_through(grad_out, grad_act, united[...], slope[...], w_in)
    kept = jnp.where(section == 1, chain_1[...], kept)
    kept = jnp.where(section == 2, chain_2[...], kept)
    kept = jnp.where(section == 3, chain_3[...], kept)
    span = kept_out.shape[2]
    for m in range(kept_out.shape[0]):
        kept_out[m] = kept[:, m * span : (m + 1) * span]
    partial = dot(source[...], kept, 1, 1)
    size = keep_out.shape[1]
    first_core = lax.axis_index("dp") % 2 == 0
    for block in range(keep_out.shape[0]):
        start = 2 * block * size
        even = partial[start : start + size, :]
        odd = partial[start + size : start + 2 * size, :]
        keep_out[block] = jnp.where(first_core, even, odd)
        give_out[block] = jnp.where(first_core, odd, even).astype(LOW)


def join_body(keep, given, own_out, *piece_outs):
    chip = lax.axis_index("dp") // 2
    own_out[...] = keep[chip] + given[chip].astype(F32)
    for mask, piece_out in enumerate(piece_outs, 1):
        far = chip ^ mask
        piece_out[...] = (keep[far] + given[far].astype(F32)).astype(LOW)


def flat_body(own, *refs):
    pieces, out, lanes, square = refs[:-3], refs[-3], refs[-2], refs[-1]
    total = own[...]
    for piece in pieces:
        total = total + piece[...].astype(F32)
    lanes[0] = total[:, :128]
    lanes[1] = total[:, 128:256]
    lanes[2] = jnp.concatenate([total[:, 256:], total[:, 256:]], axis=1)
    half = total.shape[0] // 2
    even = [lanes[part, pl.ds(0, half, stride=2), :] for part in range(3)]
    odd = [lanes[part, pl.ds(1, half, stride=2), :] for part in range(3)]
    lines = [
        even[0],
        even[1],
        jnp.concatenate([even[2][:, :64], odd[0][:, :64]], axis=1),
        jnp.concatenate([odd[0][:, 64:], odd[1][:, :64]], axis=1),
        jnp.concatenate([odd[1][:, 64:], odd[2][:, :64]], axis=1),
    ]
    for place, line in enumerate(lines):
        square[pl.ds(place, half, stride=5), :] = line
    for row in range(square.shape[0]):
        out[:, row * 128 : (row + 1) * 128] = square[row : row + 1, :]


def cut_body(w_in, w_out, own_in, own_out):
    part = own_in.shape[1]
    place = lax.axis_index("dp")
    for index in range(w_in.shape[1] // part):

        @pl.when(place == index)
        def _():
            columns = slice(index * part, (index + 1) * part)
            own_in[...] = w_in[:, columns]
            own_out[...] = w_out[:, columns]


def slice_forward_body(own_in, *refs):
    blocks, active_out, slope_out = refs[:-2], refs[-2], refs[-1]
    rows = blocks[0].shape[1]
    for place, block in enumerate(blocks):
        columns = slice(place * rows, (place + 1) * rows)
        preact = dot(own_in[...], block[...], 0, 0)
        sigma = sigmoid(preact)
        active_out[:, columns] = (preact * sigma).astype(LOW)
        slope_out[:, columns] = sigma * (1.0 + preact * (1.0 - sigma))


def slice_grad(own_out, active, slope, normed, low, first):
    rows = low[0].shape[1]
    columns = slice(first * rows, (first + len(low)) * rows)
    lows = jnp.concatenate([block[...] for block in low], axis=1)
    grad_pre = (dot(own_out[...], lows, 0, 0) * slope[:, columns]).astype(LOW)
    normeds = jnp.concatenate([block[...] for block in normed], axis=1)
    return dot(grad_pre, normeds, 1, 1), dot(active[:, columns], lows, 1, 1)


def half_grad_body(own_out, active, slope, *refs):
    half = (len(refs) - 2) // 2
    refs[-2][...], refs[-1][...] = slice_grad(
        own_out, active, slope, refs[:half], refs[half : 2 * half], 0
    )


def rest_grad_body(own_out, active, slope, sum_in, sum_out, *refs):
    half = (len(refs) - 2) // 2
    part_in, part_out = slice_grad(
        own_out, active, slope, refs[:half], refs[half : 2 * half], half
    )
    refs[-2][...] = sum_in[...] + part_in
    refs[-1][...] = sum_out[...] + part_out


def hop(value, pairs):
    return lax.ppermute(value, "section", pairs)


def exchange(value, count, mask):
    return lax.ppermute(value, "dp", [(i, i ^ mask) for i in range(count)])


def from_next(value, count, mask):
    pairs = [
        (((section + 1) % 4) * count + i, section * count + (i ^ mask))
        for section in range(4)
        for i in range(count)
    ]
    return lax.ppermute(value, ("section", "dp"), pairs)


def program(saved_inputs, timesteps, time_table, skip_weight, ff_in, ff_out, output_cotangent):
    section = lax.axis_index("section")
    count = lax.axis_size("dp")
    n_micro = saved_inputs.shape[1]
    width = saved_inputs.shape[3]
    span = saved_inputs.shape[2]
    rows = n_micro * span
    hidden = ff_in.shape[1]
    inputs = jnp.swapaxes(saved_inputs[0], 1, 2)
    upstream = jnp.swapaxes(output_cotangent, 1, 2)
    table = time_table.T
    w_skip = skip_weight[0]
    w_in = ff_in[0].T
    w_out = ff_out[0].T
    low = ((width, rows), LOW)
    wide = ((hidden, rows), F32)

    distant = (timesteps, table, w_skip, inputs, w_in, w_out)
    embed, value = call(
        encode_body, [low, low], *distant,
        scratch=[pltpu.VMEM(arg.shape, arg.dtype) for arg in distant]
        + [pltpu.SemaphoreType.DMA((len(distant),))],
        far=range(len(distant)),
    )
    received = hop(value, [(0, 3), (1, 2)])
    top_low, grad_act = call(early_body, [low, wide], upstream, w_out)
    source, normed, united, slope, chain_3 = call(
        decode_body, [low, low, ((width, rows), F32), wide, low],
        received, embed, inputs, top_low, grad_act, w_skip, w_in,
    )
    chain = hop(chain_3, [(3, 2)])
    w_mirror = hop(w_skip, [(2, 1)])
    (back,) = call(back_body, [low], chain_3, w_skip)
    skip_far = hop(back, [(3, 0)])
    skip_next = hop(back, [(3, 1)])
    low_2 = chain
    (chain_2,) = call(tick_body, [low], chain, united, slope, w_in, w_out)
    chain = hop(chain_2, [(2, 1)])
    (back_2,) = call(back_body, [low], chain_2, w_skip)
    chain_1, low_1, ahead = call(
        mirror_tick_body, [low, low, low],
        chain, w_mirror, united, slope, w_in, w_out, skip_next, back_2, chain_2, chain_3,
        top_low,
    )
    chain = hop(chain_1, [(1, 0)])
    (grad_low,) = call(pick_body, [low], chain, skip_far, low_1, low_2, top_low)

    if not (count == 8 and count * rows <= 4096 and width % 128 == 64 and width // 128 == 2):
        return by_reduction(
            section, chain, skip_far, united, slope, w_in, w_out, source, normed, grad_low,
            (chain_1, chain_2, chain_3), saved_inputs.shape,
        )

    part = hidden // count
    own_in, own_out = call(cut_body, [((width, part), LOW)] * 2, w_in, w_out)
    normed_all = [normed] + [exchange(normed, count, mask) for mask in (2, 4, 6)]
    normed_all += [exchange(block, count, 1) for block in normed_all]
    active_all, slope_all = call(
        slice_forward_body,
        [((part, count * rows), LOW), ((part, count * rows), F32)], own_in, *normed_all,
    )
    low_all = [
        grad_low,
        from_next(ahead, count, 2),
        exchange(grad_low, count, 4),
        from_next(ahead, count, 6),
    ]
    low_all += [exchange(block, count, 1) for block in low_all]
    block = (count // 2, width // count, width)
    kept, keep, give = call(
        last_body, [((n_micro, width, span), LOW), (block, F32), (block, LOW)],
        grad_low, chain, skip_far, united, slope, w_in, w_out, source, chain_1, chain_2,
        chain_3,
    )
    given = exchange(give, count, 1)
    piece = block[1:]
    own, *pieces = call(
        join_body, [(piece, F32)] + [(piece, LOW)] * (count // 2 - 1),
        keep, given,
    )
    pieces = [exchange(value, count, 2 * i) for i, value in enumerate(pieces, 1)]
    (grad_skip,) = call(
        flat_body, [((1, piece[0] * piece[1]), F32)], own, *pieces,
        scratch=[
            pltpu.VMEM((3, piece[0], 128), F32),
            pltpu.VMEM((piece[0] * piece[1] // 128, 128), F32),
        ],
    )
    grads = ((part, width), F32)
    half = count // 2
    sums = call(
        half_grad_body, [grads] * 2,
        own_out, active_all, slope_all, *normed_all[:half], *low_all[:half],
    )
    grad_in, grad_out_w = call(
        rest_grad_body, [grads] * 2,
        own_out, active_all, slope_all, *sums, *normed_all[half:], *low_all[half:],
    )
    kept = jnp.swapaxes(kept, 1, 2)
    return (kept[None], grad_skip, grad_in[None], grad_out_w[None])


def by_reduction(
    section, chain, skip_far, united, slope, w_in, w_out, source, normed, grad_low, chains,
    shape,
):
    grad_out = chain.astype(F32) + skip_far.astype(F32)
    grad_pre = (dot(w_out, grad_low, 0, 0) * slope).astype(LOW)
    preact = dot(w_in, normed, 0, 0)
    active = (preact * jax.nn.sigmoid(preact)).astype(LOW)
    own_pre = (dot(w_out, grad_out.astype(LOW), 0, 0) * slope).astype(LOW)
    grad_norm = dot(w_in, own_pre, 1, 0)
    recip = norm_of(united)
    along = jnp.mean(grad_norm * united, axis=0, keepdims=True)
    kept = (grad_out + recip * grad_norm - united * (recip * recip * recip * along)).astype(LOW)
    for owner, other in enumerate(chains, 1):
        kept = jnp.where(section == owner, other, kept)
    grad_in, grad_out_w, grad_skip = (
        lax.psum_scatter(value, "dp", scatter_dimension=0, tiled=True)
        for value in (
            dot(grad_pre, normed, 1, 1),
            dot(active, grad_low, 1, 1),
            dot(source, kept, 1, 1).reshape(-1),
        )
    )
    kept = kept.reshape(shape[3], shape[1], shape[2]).transpose(1, 2, 0)
    return (kept[None], grad_skip[None], grad_in[None], grad_out_w[None])


def solution(mesh):
    in_specs = (
        P("section", None, "dp", None),
        P(None, "dp"),
        P(),
        P("section", None, None),
        P("section", None, None),
        P("section", None, None),
        P(None, "dp", None),
    )
    out_specs = (
        P("section", None, "dp", None),
        P("section", "dp"),
        P("section", "dp", None),
        P("section", "dp", None),
    )
    return jax.shard_map(program, mesh=mesh, in_specs=in_specs, out_specs=out_specs, check_vma=False)
```

```python
import jax
import jax.numpy as jnp
from jax import lax
from jax.experimental import pallas as pl
from jax.experimental.pallas import tpu as pltpu
from jax.sharding import PartitionSpec as P


EPS = 1e-06
LOW = jnp.bfloat16
F32 = jnp.float32
VMEM_BYTES = 20 * 1024 * 1024


def contract(left, right, dims):
    return lax.dot_general(left, right, ((dims[0], dims[1]), ((), ())), preferred_element_type=F32)


def dot(left, right, on_left, on_right):
    return contract(left, right, ((on_left,), (on_right,)))


def call(body, outs, *args, scratch=(), far=()):
    places = [
        pltpu.SMEM if arg.ndim == 1 else pltpu.HBM if index in far else pltpu.VMEM
        for index, arg in enumerate(args)
    ]
    args = [
        pltpu.with_memory_space_constraint(arg, pltpu.HBM) if index in far else arg
        for index, arg in enumerate(args)
    ]
    return pl.pallas_call(
        body,
        out_shape=[jax.ShapeDtypeStruct(shape, kind) for shape, kind in outs],
        in_specs=[pl.BlockSpec(memory_space=place) for place in places],
        out_specs=[pl.BlockSpec(memory_space=pltpu.VMEM) for _ in outs],
        scratch_shapes=list(scratch),
        compiler_params=pltpu.CompilerParams(vmem_limit_bytes=VMEM_BYTES),
    )(*args)


def side_by_side(ref):
    return jnp.concatenate([ref[m] for m in range(ref.shape[0])], axis=1)


def norm_of(united):
    return lax.rsqrt(jnp.mean(united * united, axis=0, keepdims=True) + EPS)


def sigmoid(value):
    return 1.0 / (1.0 + jnp.exp(-value))


def encode_body(*refs):
    distant, (embed_out, value_out), kept, local, sems = (
        refs[:6], refs[6:8], refs[8:12], refs[12:14], refs[14],
    )
    local = (*local, *kept)
    copies = [
        pltpu.make_async_copy(source, target, sems.at[index])
        for index, (source, target) in enumerate(zip(distant, local))
    ]
    for copy in copies:
        copy.start()
    times, table, w_skip, inputs, w_in, w_out = local
    copies[0].wait()
    levels = lax.broadcasted_iota(jnp.int32, (table.shape[1], times.shape[1]), 0)
    hot = [
        jnp.where(levels == times[m : m + 1, :], 1.0, 0.0).astype(LOW)
        for m in range(times.shape[0])
    ]
    copies[1].wait()
    embed = dot(table[...], jnp.concatenate(hot, axis=1), 1, 0).astype(LOW)
    embed_out[...] = embed
    copies[2].wait()
    copies[3].wait()
    united = side_by_side(inputs).astype(F32) + dot(w_skip[...], embed, 0, 0)
    normed = (united * norm_of(united)).astype(LOW)
    copies[4].wait()
    preact = dot(w_in[...], normed, 0, 0)
    active = (preact * sigmoid(preact)).astype(LOW)
    copies[5].wait()
    value_out[...] = (united + dot(w_out[...], active, 1, 0)).astype(LOW)


def early_body(upstream, w_out, low_out, grad_act_out):
    low = side_by_side(upstream)
    low_out[...] = low
    grad_act_out[...] = dot(w_out[...], low, 0, 0)


def back_through(grad_out, grad_act, united, slope, w_in):
    grad_pre = (grad_act * slope).astype(LOW)
    grad_norm = dot(w_in[...], grad_pre, 1, 0)
    recip = norm_of(united)
    along = jnp.mean(grad_norm * united, axis=0, keepdims=True)
    return (grad_out + recip * grad_norm - united * (recip * recip * recip * along)).astype(LOW)


def decode_body(
    received, embed, inputs, top_low, grad_act, w_skip, w_in,
    source_out, normed_out, united_out, slope_out, chain_out,
):
    source = jnp.where(lax.axis_index("section") >= 2, received[...], embed[...])
    source_out[...] = source
    united = side_by_side(inputs).astype(F32) + dot(w_skip[...], source, 0, 0)
    united_out[...] = united
    normed = (united * norm_of(united)).astype(LOW)
    normed_out[...] = normed
    preact = dot(w_in[...], normed, 0, 0)
    sigma = sigmoid(preact)
    slope = sigma * (1.0 + preact * (1.0 - sigma))
    slope_out[...] = slope
    chain_out[...] = back_through(top_low[...].astype(F32), grad_act[...], united, slope, w_in)


def back_body(chain, w_skip, back_out):
    back_out[...] = dot(w_skip[...], chain[...], 1, 0).astype(LOW)


def tick_body(received, united, slope, w_in, w_out, chain_out):
    low = received[...]
    grad_act = dot(w_out[...], low, 0, 0)
    chain_out[...] = back_through(low.astype(F32), grad_act, united[...], slope[...], w_in)


def mirror_tick_body(
    received, w_mirror, united, slope, w_in, w_out, skip_far, back_2, chain_2, chain_3,
    chain_out, low_out, next_out,
):
    back = dot(w_mirror[...], received[...], 1, 0).astype(LOW)
    grad_out = received[...].astype(F32) + back.astype(F32)
    low = grad_out.astype(LOW)
    low_out[...] = low
    grad_act = dot(w_out[...], low, 0, 0)
    chain = back_through(grad_out, grad_act, united[...], slope[...], w_in)
    chain_out[...] = chain
    section = lax.axis_index("section")
    ahead = (chain.astype(F32) + skip_far[...].astype(F32)).astype(LOW)
    ahead = jnp.where(
        section == 2, (chain_2[...].astype(F32) + back_2[...].astype(F32)).astype(LOW), ahead
    )
    next_out[...] = jnp.where(section == 3, chain_3[...], ahead)


def pick_body(received, skip_far, low_1, low_2, top_low, grad_low_out):
    own = (received[...].astype(F32) + skip_far[...].astype(F32)).astype(LOW)
    section = lax.axis_index("section")
    own = jnp.where(section == 1, low_1[...], own)
    own = jnp.where(section == 2, low_2[...], own)
    grad_low_out[...] = jnp.where(section == 3, top_low[...], own)


def merge_body(top_2, top_6, next_2, next_6, out_2, out_6):
    last = lax.axis_index("section") == 3
    out_2[...] = jnp.where(last, top_2[...], next_2[...])
    out_6[...] = jnp.where(last, top_6[...], next_6[...])


def last_body(
    grad_low, received, skip_far, united, slope, w_in, w_out, source, chain_1, chain_2,
    chain_3, kept_out, keep_out, give_out,
):
    grad_out = received[...].astype(F32) + skip_far[...].astype(F32)
    grad_act = dot(w_out[...], grad_low[...], 0, 0)
    section = lax.axis_index("section")
    kept = back_through(grad_out, grad_act, united[...], slope[...], w_in)
    kept = jnp.where(section == 1, chain_1[...], kept)
    kept = jnp.where(section == 2, chain_2[...], kept)
    kept = jnp.where(section == 3, chain_3[...], kept)
    span = kept_out.shape[2]
    for m in range(kept_out.shape[0]):
        kept_out[m] = kept[:, m * span : (m + 1) * span]
    partial = dot(source[...], kept, 1, 1)
    size = keep_out.shape[1]
    first_core = lax.axis_index("dp") % 2 == 0
    for block in range(keep_out.shape[0]):
        start = 2 * block * size
        even = partial[start : start + size, :]
        odd = partial[start + size : start + 2 * size, :]
        keep_out[block] = jnp.where(first_core, even, odd)
        give_out[block] = jnp.where(first_core, odd, even).astype(LOW)


def join_body(keep, given, own_out, *piece_outs):
    chip = lax.axis_index("dp") // 2
    own_out[...] = keep[chip] + given[chip].astype(F32)
    for mask, piece_out in enumerate(piece_outs, 1):
        far = chip ^ mask
        piece_out[...] = (keep[far] + given[far].astype(F32)).astype(LOW)


def flat_body(own, *refs):
    pieces, out, lanes, square = refs[:-3], refs[-3], refs[-2], refs[-1]
    total = own[...]
    for piece in pieces:
        total = total + piece[...].astype(F32)
    lanes[0] = total[:, :128]
    lanes[1] = total[:, 128:256]
    lanes[2] = jnp.concatenate([total[:, 256:], total[:, 256:]], axis=1)
    half = total.shape[0] // 2
    even = [lanes[part, pl.ds(0, half, stride=2), :] for part in range(3)]
    odd = [lanes[part, pl.ds(1, half, stride=2), :] for part in range(3)]
    lines = [
        even[0],
        even[1],
        jnp.concatenate([even[2][:, :64], odd[0][:, :64]], axis=1),
        jnp.concatenate([odd[0][:, 64:], odd[1][:, :64]], axis=1),
        jnp.concatenate([odd[1][:, 64:], odd[2][:, :64]], axis=1),
    ]
    for place, line in enumerate(lines):
        square[pl.ds(place, half, stride=5), :] = line
    for row in range(square.shape[0]):
        out[:, row * 128 : (row + 1) * 128] = square[row : row + 1, :]


def cut_body(w_in, w_out, own_in, own_out):
    part = own_in.shape[1]
    place = lax.axis_index("dp")
    for index in range(w_in.shape[1] // part):

        @pl.when(place == index)
        def _():
            columns = slice(index * part, (index + 1) * part)
            own_in[...] = w_in[:, columns]
            own_out[...] = w_out[:, columns]


def slice_forward_body(own_in, *refs):
    blocks, active_out, slope_out = refs[:-2], refs[-2], refs[-1]
    rows = blocks[0].shape[1]
    for place, block in enumerate(blocks):
        columns = slice(place * rows, (place + 1) * rows)
        preact = dot(own_in[...], block[...], 0, 0)
        sigma = sigmoid(preact)
        active_out[:, columns] = (preact * sigma).astype(LOW)
        slope_out[:, columns] = sigma * (1.0 + preact * (1.0 - sigma))


def slice_grad(own_out, active, slope, normed, low, first):
    rows = low[0].shape[1]
    columns = slice(first * rows, (first + len(low)) * rows)
    lows = jnp.concatenate([block[...] for block in low], axis=1)
    grad_pre = (dot(own_out[...], lows, 0, 0) * slope[:, columns]).astype(LOW)
    normeds = jnp.concatenate([block[...] for block in normed], axis=1)
    return dot(grad_pre, normeds, 1, 1), dot(active[:, columns], lows, 1, 1)


def half_grad_body(own_out, active, slope, *refs):
    half = (len(refs) - 2) // 2
    refs[-2][...], refs[-1][...] = slice_grad(
        own_out, active, slope, refs[:half], refs[half : 2 * half], 0
    )


def rest_grad_body(own_out, active, slope, sum_in, sum_out, *refs):
    half = (len(refs) - 2) // 2
    first = active.shape[1] // refs[0].shape[1] - half
    part_in, part_out = slice_grad(
        own_out, active, slope, refs[:half], refs[half : 2 * half], first
    )
    refs[-2][...] = sum_in[...] + part_in
    refs[-1][...] = sum_out[...] + part_out


def hop(value, pairs):
    return lax.ppermute(value, "section", pairs)


def in_turn(near, swapped):
    return [*near[:3], *swapped[:3], near[3], swapped[3]]


def exchange(value, count, mask):
    return lax.ppermute(value, "dp", [(i, i ^ mask) for i in range(count)])


def from_next(value, count, mask):
    pairs = [
        ((section + 1) * count + i, section * count + (i ^ mask))
        for section in range(3)
        for i in range(count)
    ]
    return lax.ppermute(value, ("section", "dp"), pairs)


def in_last(value, count, mask):
    pairs = [(3 * count + i, 3 * count + (i ^ mask)) for i in range(count)]
    return lax.ppermute(value, ("section", "dp"), pairs)


def program(saved_inputs, timesteps, time_table, skip_weight, ff_in, ff_out, output_cotangent):
    section = lax.axis_index("section")
    count = lax.axis_size("dp")
    n_micro = saved_inputs.shape[1]
    width = saved_inputs.shape[3]
    span = saved_inputs.shape[2]
    rows = n_micro * span
    hidden = ff_in.shape[1]
    inputs = jnp.swapaxes(saved_inputs[0], 1, 2)
    upstream = jnp.swapaxes(output_cotangent, 1, 2)
    table = time_table.T
    w_skip = skip_weight[0]
    w_in = ff_in[0].T
    w_out = ff_out[0].T
    low = ((width, rows), LOW)
    wide = ((hidden, rows), F32)

    distant = (timesteps, table, w_skip, inputs, w_in, w_out)
    embed, value, w_skip, inputs, w_in, w_out = call(
        encode_body, [low, low] + [(arg.shape, arg.dtype) for arg in distant[2:]],
        *distant,
        scratch=[pltpu.VMEM(arg.shape, arg.dtype) for arg in distant[:2]]
        + [pltpu.SemaphoreType.DMA((len(distant),))],
        far=range(len(distant)),
    )
    received = hop(value, [(0, 3), (1, 2)])
    top_low, grad_act = call(early_body, [low, wide], upstream, w_out)
    source, normed, united, slope, chain_3 = call(
        decode_body, [low, low, ((width, rows), F32), wide, low],
        received, embed, inputs, top_low, grad_act, w_skip, w_in,
    )
    chain = hop(chain_3, [(3, 2)])
    w_mirror = hop(w_skip, [(2, 1)])
    (back,) = call(back_body, [low], chain_3, w_skip)
    skip_far = hop(back, [(3, 0)])
    skip_next = hop(back, [(3, 1)])
    low_2 = chain
    (chain_2,) = call(tick_body, [low], chain, united, slope, w_in, w_out)
    chain = hop(chain_2, [(2, 1)])
    (back_2,) = call(back_body, [low], chain_2, w_skip)
    chain_1, low_1, ahead = call(
        mirror_tick_body, [low, low, low],
        chain, w_mirror, united, slope, w_in, w_out, skip_next, back_2, chain_2, chain_3,
    )
    chain = hop(chain_1, [(1, 0)])
    (grad_low,) = call(pick_body, [low], chain, skip_far, low_1, low_2, top_low)

    if not (count == 8 and count * rows <= 4096 and width % 128 == 64 and width // 128 == 2):
        return by_reduction(
            section, chain, skip_far, united, slope, w_in, w_out, source, normed, grad_low,
            (chain_1, chain_2, chain_3), saved_inputs.shape,
        )

    part = hidden // count
    own_in, own_out = call(cut_body, [((width, part), LOW)] * 2, w_in, w_out)
    masks = (2, 6, 4)
    normed_near = [normed] + [exchange(normed, count, m) for m in masks]
    normed_all = in_turn(
        normed_near,
        [exchange(x, count, 1) for x in normed_near],
    )
    active_all, slope_all = call(
        slice_forward_body,
        [((part, count * rows), LOW), ((part, count * rows), F32)], own_in, *normed_all,
    )
    tops = [in_last(top_low, count, m) for m in masks[:2]]
    aheads = [from_next(ahead, count, m) for m in masks[:2]]
    low_2, low_6 = call(merge_body, [low, low], *tops, *aheads)
    low_near = [grad_low, low_2, low_6, exchange(grad_low, count, 4)]
    low_all = in_turn(low_near, [exchange(x, count, 1) for x in low_near])
    block = (count // 2, width // count, width)
    kept, keep, give = call(
        last_body, [((n_micro, width, span), LOW), (block, F32), (block, LOW)],
        grad_low, chain, skip_far, united, slope, w_in, w_out, source, chain_1, chain_2,
        chain_3,
    )
    given = exchange(give, count, 1)
    piece = block[1:]
    own, *pieces = call(
        join_body, [(piece, F32)] + [(piece, LOW)] * (count // 2 - 1),
        keep, given,
    )
    pieces = [exchange(value, count, 2 * i) for i, value in enumerate(pieces, 1)]
    (grad_skip,) = call(
        flat_body, [((1, piece[0] * piece[1]), F32)], own, *pieces,
        scratch=[
            pltpu.VMEM((3, piece[0], 128), F32),
            pltpu.VMEM((piece[0] * piece[1] // 128, 128), F32),
        ],
    )
    grads = ((part, width), F32)
    half = 6
    sums = call(
        half_grad_body, [grads] * 2,
        own_out, active_all, slope_all, *normed_all[:half], *low_all[:half],
    )
    grad_in, grad_out_w = call(
        rest_grad_body, [grads] * 2,
        own_out, active_all, slope_all, *sums, *normed_all[half:], *low_all[half:],
    )
    kept = jnp.swapaxes(kept, 1, 2)
    return (kept[None], grad_skip, grad_in[None], grad_out_w[None])


def by_reduction(
    section, chain, skip_far, united, slope, w_in, w_out, source, normed, grad_low, chains,
    shape,
):
    grad_out = chain.astype(F32) + skip_far.astype(F32)
    grad_pre = (dot(w_out, grad_low, 0, 0) * slope).astype(LOW)
    preact = dot(w_in, normed, 0, 0)
    active = (preact * jax.nn.sigmoid(preact)).astype(LOW)
    own_pre = (dot(w_out, grad_out.astype(LOW), 0, 0) * slope).astype(LOW)
    grad_norm = dot(w_in, own_pre, 1, 0)
    recip = norm_of(united)
    along = jnp.mean(grad_norm * united, axis=0, keepdims=True)
    kept = (grad_out + recip * grad_norm - united * (recip * recip * recip * along)).astype(LOW)
    for owner, other in enumerate(chains, 1):
        kept = jnp.where(section == owner, other, kept)
    grad_in, grad_out_w, grad_skip = (
        lax.psum_scatter(value, "dp", scatter_dimension=0, tiled=True)
        for value in (
            dot(grad_pre, normed, 1, 1),
            dot(active, grad_low, 1, 1),
            dot(source, kept, 1, 1).reshape(-1),
        )
    )
    kept = kept.reshape(shape[3], shape[1], shape[2]).transpose(1, 2, 0)
    return (kept[None], grad_skip[None], grad_in[None], grad_out_w[None])


def solution(mesh):
    in_specs = (
        P("section", None, "dp", None),
        P(None, "dp"),
        P(),
        P("section", None, None),
        P("section", None, None),
        P("section", None, None),
        P(None, "dp", None),
    )
    out_specs = (
        P("section", None, "dp", None),
        P("section", "dp"),
        P("section", "dp", None),
        P("section", "dp", None),
    )
    return jax.shard_map(program, mesh=mesh, in_specs=in_specs, out_specs=out_specs, check_vma=False)
```

```python
import jax
import jax.numpy as jnp
from jax import lax
from jax.experimental import pallas as pl
from jax.experimental.pallas import tpu as pltpu
from jax.sharding import PartitionSpec as P


EPS = 1e-06
LOW = jnp.bfloat16
F32 = jnp.float32
VMEM_BYTES = 20 * 1024 * 1024


def contract(left, right, dims):
    return lax.dot_general(left, right, ((dims[0], dims[1]), ((), ())), preferred_element_type=F32)


def dot(left, right, on_left, on_right):
    return contract(left, right, ((on_left,), (on_right,)))


def call(body, outs, *args, scratch=(), far=()):
    places = [
        pltpu.SMEM if arg.ndim == 1 else pltpu.HBM if index in far else pltpu.VMEM
        for index, arg in enumerate(args)
    ]
    args = [
        pltpu.with_memory_space_constraint(arg, pltpu.HBM) if index in far else arg
        for index, arg in enumerate(args)
    ]
    return pl.pallas_call(
        body,
        out_shape=[jax.ShapeDtypeStruct(shape, kind) for shape, kind in outs],
        in_specs=[pl.BlockSpec(memory_space=place) for place in places],
        out_specs=[pl.BlockSpec(memory_space=pltpu.VMEM) for _ in outs],
        scratch_shapes=list(scratch),
        compiler_params=pltpu.CompilerParams(vmem_limit_bytes=VMEM_BYTES),
    )(*args)


def side_by_side(ref):
    return jnp.concatenate([ref[m] for m in range(ref.shape[0])], axis=1)


def norm_of(united):
    return lax.rsqrt(jnp.mean(united * united, axis=0, keepdims=True) + EPS)


def sigmoid(value):
    return 1.0 / (1.0 + jnp.exp(-value))


def encode_body(*refs):
    distant, (embed_out, value_out), kept, local, sems = (
        refs[:6], refs[6:8], refs[8:12], refs[12:14], refs[14],
    )
    local = (*local, *kept)
    copies = [
        pltpu.make_async_copy(source, target, sems.at[index])
        for index, (source, target) in enumerate(zip(distant, local))
    ]
    for copy in copies:
        copy.start()
    times, table, w_skip, inputs, w_in, w_out = local
    copies[0].wait()
    levels = lax.broadcasted_iota(jnp.int32, (table.shape[1], times.shape[1]), 0)
    hot = [
        jnp.where(levels == times[m : m + 1, :], 1.0, 0.0).astype(LOW)
        for m in range(times.shape[0])
    ]
    copies[1].wait()
    embed = dot(table[...], jnp.concatenate(hot, axis=1), 1, 0).astype(LOW)
    embed_out[...] = embed
    copies[2].wait()
    copies[3].wait()
    united = side_by_side(inputs).astype(F32) + dot(w_skip[...], embed, 0, 0)
    normed = (united * norm_of(united)).astype(LOW)
    copies[4].wait()
    preact = dot(w_in[...], normed, 0, 0)
    active = (preact * sigmoid(preact)).astype(LOW)
    copies[5].wait()
    value_out[...] = (united + dot(w_out[...], active, 1, 0)).astype(LOW)


def early_body(upstream, w_out, low_out, grad_act_out):
    low = side_by_side(upstream)
    low_out[...] = low
    grad_act_out[...] = dot(w_out[...], low, 0, 0)


def back_through(grad_out, grad_act, united, slope, w_in):
    grad_pre = (grad_act * slope).astype(LOW)
    grad_norm = dot(w_in[...], grad_pre, 1, 0)
    recip = norm_of(united)
    along = jnp.mean(grad_norm * united, axis=0, keepdims=True)
    return (grad_out + recip * grad_norm - united * (recip * recip * recip * along)).astype(LOW)


def decode_body(
    received, embed, inputs, top_low, grad_act, w_skip, w_in,
    source_out, normed_out, united_out, slope_out, chain_out,
):
    source = jnp.where(lax.axis_index("section") >= 2, received[...], embed[...])
    source_out[...] = source
    united = side_by_side(inputs).astype(F32) + dot(w_skip[...], source, 0, 0)
    united_out[...] = united
    normed = (united * norm_of(united)).astype(LOW)
    normed_out[...] = normed
    preact = dot(w_in[...], normed, 0, 0)
    sigma = sigmoid(preact)
    slope = sigma * (1.0 + preact * (1.0 - sigma))
    slope_out[...] = slope
    chain_out[...] = back_through(top_low[...].astype(F32), grad_act[...], united, slope, w_in)


def back_body(chain, w_skip, back_out):
    back_out[...] = dot(w_skip[...], chain[...], 1, 0).astype(LOW)


def tick_body(received, united, slope, w_in, w_out, chain_out):
    low = received[...]
    grad_act = dot(w_out[...], low, 0, 0)
    chain_out[...] = back_through(low.astype(F32), grad_act, united[...], slope[...], w_in)


def mirror_tick_body(
    received, w_mirror, united, slope, w_in, w_out, skip_far, back_2, chain_2, chain_3,
    chain_out, low_out, next_out,
):
    back = dot(w_mirror[...], received[...], 1, 0).astype(LOW)
    grad_out = received[...].astype(F32) + back.astype(F32)
    low = grad_out.astype(LOW)
    low_out[...] = low
    grad_act = dot(w_out[...], low, 0, 0)
    chain = back_through(grad_out, grad_act, united[...], slope[...], w_in)
    chain_out[...] = chain
    section = lax.axis_index("section")
    ahead = (chain.astype(F32) + skip_far[...].astype(F32)).astype(LOW)
    ahead = jnp.where(
        section == 2, (chain_2[...].astype(F32) + back_2[...].astype(F32)).astype(LOW), ahead
    )
    next_out[...] = jnp.where(section == 3, chain_3[...], ahead)


def pick_body(received, skip_far, low_1, low_2, top_low, grad_low_out):
    own = (received[...].astype(F32) + skip_far[...].astype(F32)).astype(LOW)
    section = lax.axis_index("section")
    own = jnp.where(section == 1, low_1[...], own)
    own = jnp.where(section == 2, low_2[...], own)
    grad_low_out[...] = jnp.where(section == 3, top_low[...], own)


def merge_body(top, following, out):
    out[...] = jnp.where(lax.axis_index("section") == 3, top[...], following[...])


def last_body(
    grad_low, received, skip_far, united, slope, w_in, w_out, source, chain_1, chain_2,
    chain_3, kept_out, keep_out, give_out,
):
    grad_out = received[...].astype(F32) + skip_far[...].astype(F32)
    grad_act = dot(w_out[...], grad_low[...], 0, 0)
    section = lax.axis_index("section")
    kept = back_through(grad_out, grad_act, united[...], slope[...], w_in)
    kept = jnp.where(section == 1, chain_1[...], kept)
    kept = jnp.where(section == 2, chain_2[...], kept)
    kept = jnp.where(section == 3, chain_3[...], kept)
    span = kept_out.shape[2]
    for m in range(kept_out.shape[0]):
        kept_out[m] = kept[:, m * span : (m + 1) * span]
    partial = dot(source[...], kept, 1, 1)
    size = keep_out.shape[1]
    first_core = lax.axis_index("dp") % 2 == 0
    for block in range(keep_out.shape[0]):
        start = 2 * block * size
        even = partial[start : start + size, :]
        odd = partial[start + size : start + 2 * size, :]
        keep_out[block] = jnp.where(first_core, even, odd)
        give_out[block] = jnp.where(first_core, odd, even).astype(LOW)


def join_body(keep, given, own_out, *piece_outs):
    chip = lax.axis_index("dp") // 2
    own_out[...] = keep[chip] + given[chip].astype(F32)
    for mask, piece_out in enumerate(piece_outs, 1):
        far = chip ^ mask
        piece_out[...] = (keep[far] + given[far].astype(F32)).astype(LOW)


def flat_body(own, *refs):
    pieces, out, lanes, square = refs[:-3], refs[-3], refs[-2], refs[-1]
    total = own[...]
    for piece in pieces:
        total = total + piece[...].astype(F32)
    lanes[0] = total[:, :128]
    lanes[1] = total[:, 128:256]
    lanes[2] = jnp.concatenate([total[:, 256:], total[:, 256:]], axis=1)
    half = total.shape[0] // 2
    even = [lanes[part, pl.ds(0, half, stride=2), :] for part in range(3)]
    odd = [lanes[part, pl.ds(1, half, stride=2), :] for part in range(3)]
    lines = [
        even[0],
        even[1],
        jnp.concatenate([even[2][:, :64], odd[0][:, :64]], axis=1),
        jnp.concatenate([odd[0][:, 64:], odd[1][:, :64]], axis=1),
        jnp.concatenate([odd[1][:, 64:], odd[2][:, :64]], axis=1),
    ]
    for place, line in enumerate(lines):
        square[pl.ds(place, half, stride=5), :] = line
    for row in range(square.shape[0]):
        out[:, row * 128 : (row + 1) * 128] = square[row : row + 1, :]


def cut_body(w_in, w_out, own_in, own_out):
    part = own_in.shape[1]
    place = lax.axis_index("dp")
    for index in range(w_in.shape[1] // part):

        @pl.when(place == index)
        def _():
            columns = slice(index * part, (index + 1) * part)
            own_in[...] = w_in[:, columns]
            own_out[...] = w_out[:, columns]


def slice_forward_body(own_in, *refs):
    blocks, active_out, slope_out = refs[:-2], refs[-2], refs[-1]
    rows = blocks[0].shape[1]
    for place, block in enumerate(blocks):
        columns = slice(place * rows, (place + 1) * rows)
        preact = dot(own_in[...], block[...], 0, 0)
        sigma = sigmoid(preact)
        active_out[:, columns] = (preact * sigma).astype(LOW)
        slope_out[:, columns] = sigma * (1.0 + preact * (1.0 - sigma))


def slice_grad(own_out, active, slope, normed, low, first):
    rows = low[0].shape[1]
    columns = slice(first * rows, (first + len(low)) * rows)
    lows = jnp.concatenate([block[...] for block in low], axis=1)
    grad_pre = (dot(own_out[...], lows, 0, 0) * slope[:, columns]).astype(LOW)
    normeds = jnp.concatenate([block[...] for block in normed], axis=1)
    return dot(grad_pre, normeds, 1, 1), dot(active[:, columns], lows, 1, 1)


def half_grad_body(own_out, active, slope, *refs):
    half = (len(refs) - 2) // 2
    refs[-2][...], refs[-1][...] = slice_grad(
        own_out, active, slope, refs[:half], refs[half : 2 * half], 0
    )


def rest_grad_body(own_out, active, slope, sum_in, sum_out, *refs):
    half = (len(refs) - 2) // 2
    first = active.shape[1] // refs[0].shape[1] - half
    part_in, part_out = slice_grad(
        own_out, active, slope, refs[:half], refs[half : 2 * half], first
    )
    refs[-2][...] = sum_in[...] + part_in
    refs[-1][...] = sum_out[...] + part_out


def hop(value, pairs):
    return lax.ppermute(value, "section", pairs)


def in_turn(near, swapped):
    return [*near[:3], *swapped[:3], near[3], swapped[3]]


def exchange(value, count, mask):
    return lax.ppermute(value, "dp", [(i, i ^ mask) for i in range(count)])


def from_next(value, count, mask):
    pairs = [
        ((section + 1) * count + i, section * count + (i ^ mask))
        for section in range(3)
        for i in range(count)
    ]
    return lax.ppermute(value, ("section", "dp"), pairs)


def in_last(value, count, mask):
    pairs = [(3 * count + i, 3 * count + (i ^ mask)) for i in range(count)]
    return lax.ppermute(value, ("section", "dp"), pairs)


def program(saved_inputs, timesteps, time_table, skip_weight, ff_in, ff_out, output_cotangent):
    section = lax.axis_index("section")
    count = lax.axis_size("dp")
    n_micro = saved_inputs.shape[1]
    width = saved_inputs.shape[3]
    span = saved_inputs.shape[2]
    rows = n_micro * span
    hidden = ff_in.shape[1]
    inputs = jnp.swapaxes(saved_inputs[0], 1, 2)
    upstream = jnp.swapaxes(output_cotangent, 1, 2)
    table = time_table.T
    w_skip = skip_weight[0]
    w_in = ff_in[0].T
    w_out = ff_out[0].T
    low = ((width, rows), LOW)
    wide = ((hidden, rows), F32)

    distant = (timesteps, table, w_skip, inputs, w_in, w_out)
    embed, value, w_skip, inputs, w_in, w_out = call(
        encode_body, [low, low] + [(arg.shape, arg.dtype) for arg in distant[2:]],
        *distant,
        scratch=[pltpu.VMEM(arg.shape, arg.dtype) for arg in distant[:2]]
        + [pltpu.SemaphoreType.DMA((len(distant),))],
        far=range(len(distant)),
    )
    received = hop(value, [(0, 3), (1, 2)])
    top_low, grad_act = call(early_body, [low, wide], upstream, w_out)
    source, normed, united, slope, chain_3 = call(
        decode_body, [low, low, ((width, rows), F32), wide, low],
        received, embed, inputs, top_low, grad_act, w_skip, w_in,
    )
    chain = hop(chain_3, [(3, 2)])
    w_mirror = hop(w_skip, [(2, 1)])
    (back,) = call(back_body, [low], chain_3, w_skip)
    skip_far = hop(back, [(3, 0)])
    skip_next = hop(back, [(3, 1)])
    low_2 = chain
    (chain_2,) = call(tick_body, [low], chain, united, slope, w_in, w_out)
    chain = hop(chain_2, [(2, 1)])
    (back_2,) = call(back_body, [low], chain_2, w_skip)
    chain_1, low_1, ahead = call(
        mirror_tick_body, [low, low, low],
        chain, w_mirror, united, slope, w_in, w_out, skip_next, back_2, chain_2, chain_3,
    )
    chain = hop(chain_1, [(1, 0)])
    (grad_low,) = call(pick_body, [low], chain, skip_far, low_1, low_2, top_low)

    if not (count == 8 and count * rows <= 4096 and width % 128 == 64 and width // 128 == 2):
        return by_reduction(
            section, chain, skip_far, united, slope, w_in, w_out, source, normed, grad_low,
            (chain_1, chain_2, chain_3), saved_inputs.shape,
        )

    part = hidden // count
    own_in, own_out = call(cut_body, [((width, part), LOW)] * 2, w_in, w_out)
    normed_near = [normed] + [exchange(normed, count, m) for m in (2, 6, 4)]
    normed_all = in_turn(
        normed_near,
        [exchange(x, count, 1) for x in normed_near],
    )
    active_all, slope_all = call(
        slice_forward_body,
        [((part, count * rows), LOW), ((part, count * rows), F32)], own_in, *normed_all,
    )
    top_6 = in_last(top_low, count, 6)
    next_6 = from_next(ahead, count, 6)
    (low_6,) = call(merge_body, [low], top_6, next_6)
    low_2, low_4 = (exchange(grad_low, count, m) for m in (2, 4))
    low_near = [grad_low, low_2, low_6, low_4]
    low_all = in_turn(low_near, [exchange(x, count, 1) for x in low_near])
    block = (count // 2, width // count, width)
    kept, keep, give = call(
        last_body, [((n_micro, width, span), LOW), (block, F32), (block, LOW)],
        grad_low, chain, skip_far, united, slope, w_in, w_out, source, chain_1, chain_2,
        chain_3,
    )
    given = exchange(give, count, 1)
    piece = block[1:]
    own, *pieces = call(
        join_body, [(piece, F32)] + [(piece, LOW)] * (count // 2 - 1),
        keep, given,
    )
    pieces = [exchange(value, count, 2 * i) for i, value in enumerate(pieces, 1)]
    (grad_skip,) = call(
        flat_body, [((1, piece[0] * piece[1]), F32)], own, *pieces,
        scratch=[
            pltpu.VMEM((3, piece[0], 128), F32),
            pltpu.VMEM((piece[0] * piece[1] // 128, 128), F32),
        ],
    )
    grads = ((part, width), F32)
    half = 6
    sums = call(
        half_grad_body, [grads] * 2,
        own_out, active_all, slope_all, *normed_all[:half], *low_all[:half],
    )
    grad_in, grad_out_w = call(
        rest_grad_body, [grads] * 2,
        own_out, active_all, slope_all, *sums, *normed_all[half:], *low_all[half:],
    )
    kept = jnp.swapaxes(kept, 1, 2)
    return (kept[None], grad_skip, grad_in[None], grad_out_w[None])


def by_reduction(
    section, chain, skip_far, united, slope, w_in, w_out, source, normed, grad_low, chains,
    shape,
):
    grad_out = chain.astype(F32) + skip_far.astype(F32)
    grad_pre = (dot(w_out, grad_low, 0, 0) * slope).astype(LOW)
    preact = dot(w_in, normed, 0, 0)
    active = (preact * jax.nn.sigmoid(preact)).astype(LOW)
    own_pre = (dot(w_out, grad_out.astype(LOW), 0, 0) * slope).astype(LOW)
    grad_norm = dot(w_in, own_pre, 1, 0)
    recip = norm_of(united)
    along = jnp.mean(grad_norm * united, axis=0, keepdims=True)
    kept = (grad_out + recip * grad_norm - united * (recip * recip * recip * along)).astype(LOW)
    for owner, other in enumerate(chains, 1):
        kept = jnp.where(section == owner, other, kept)
    grad_in, grad_out_w, grad_skip = (
        lax.psum_scatter(value, "dp", scatter_dimension=0, tiled=True)
        for value in (
            dot(grad_pre, normed, 1, 1),
            dot(active, grad_low, 1, 1),
            dot(source, kept, 1, 1).reshape(-1),
        )
    )
    kept = kept.reshape(shape[3], shape[1], shape[2]).transpose(1, 2, 0)
    return (kept[None], grad_skip[None], grad_in[None], grad_out_w[None])


def solution(mesh):
    in_specs = (
        P("section", None, "dp", None),
        P(None, "dp"),
        P(),
        P("section", None, None),
        P("section", None, None),
        P("section", None, None),
        P(None, "dp", None),
    )
    out_specs = (
        P("section", None, "dp", None),
        P("section", "dp"),
        P("section", "dp", None),
        P("section", "dp", None),
    )
    return jax.shard_map(program, mesh=mesh, in_specs=in_specs, out_specs=out_specs, check_vma=False)
```

```python
import jax
import jax.numpy as jnp
from jax import lax
from jax.experimental import pallas as pl
from jax.experimental.pallas import tpu as pltpu
from jax.sharding import PartitionSpec as P


EPS = 1e-06
LOW = jnp.bfloat16
F32 = jnp.float32
VMEM_BYTES = 20 * 1024 * 1024


def contract(left, right, dims):
    return lax.dot_general(left, right, ((dims[0], dims[1]), ((), ())), preferred_element_type=F32)


def dot(left, right, on_left, on_right):
    return contract(left, right, ((on_left,), (on_right,)))


def call(body, outs, *args, scratch=(), far=()):
    places = [
        pltpu.SMEM if arg.ndim == 1 else pltpu.HBM if index in far else pltpu.VMEM
        for index, arg in enumerate(args)
    ]
    args = [
        pltpu.with_memory_space_constraint(arg, pltpu.HBM) if index in far else arg
        for index, arg in enumerate(args)
    ]
    return pl.pallas_call(
        body,
        out_shape=[jax.ShapeDtypeStruct(shape, kind) for shape, kind in outs],
        in_specs=[pl.BlockSpec(memory_space=place) for place in places],
        out_specs=[pl.BlockSpec(memory_space=pltpu.VMEM) for _ in outs],
        scratch_shapes=list(scratch),
        compiler_params=pltpu.CompilerParams(vmem_limit_bytes=VMEM_BYTES),
    )(*args)


def side_by_side(ref):
    return jnp.concatenate([ref[m] for m in range(ref.shape[0])], axis=1)


def norm_of(united):
    return lax.rsqrt(jnp.mean(united * united, axis=0, keepdims=True) + EPS)


def sigmoid(value):
    return 1.0 / (1.0 + jnp.exp(-value))


def encode_body(*refs):
    distant, (embed_out, value_out), kept, local, sems = (
        refs[:6], refs[6:8], refs[8:12], refs[12:14], refs[14],
    )
    local = (*local, *kept)
    copies = [
        pltpu.make_async_copy(source, target, sems.at[index])
        for index, (source, target) in enumerate(zip(distant, local))
    ]
    for copy in copies:
        copy.start()
    times, table, w_skip, inputs, w_in, w_out = local
    copies[0].wait()
    levels = lax.broadcasted_iota(jnp.int32, (table.shape[1], times.shape[1]), 0)
    hot = [
        jnp.where(levels == times[m : m + 1, :], 1.0, 0.0).astype(LOW)
        for m in range(times.shape[0])
    ]
    copies[1].wait()
    embed = dot(table[...], jnp.concatenate(hot, axis=1), 1, 0).astype(LOW)
    embed_out[...] = embed
    copies[2].wait()
    copies[3].wait()
    united = side_by_side(inputs).astype(F32) + dot(w_skip[...], embed, 0, 0)
    normed = (united * norm_of(united)).astype(LOW)
    copies[4].wait()
    preact = dot(w_in[...], normed, 0, 0)
    active = (preact * sigmoid(preact)).astype(LOW)
    copies[5].wait()
    value_out[...] = (united + dot(w_out[...], active, 1, 0)).astype(LOW)


def early_body(upstream, w_out, low_out, grad_act_out):
    low = side_by_side(upstream)
    low_out[...] = low
    grad_act_out[...] = dot(w_out[...], low, 0, 0)


def back_through(grad_out, grad_act, united, slope, w_in):
    grad_pre = (grad_act * slope).astype(LOW)
    grad_norm = dot(w_in[...], grad_pre, 1, 0)
    recip = norm_of(united)
    along = jnp.mean(grad_norm * united, axis=0, keepdims=True)
    return (grad_out + recip * grad_norm - united * (recip * recip * recip * along)).astype(LOW)


def decode_body(
    received, embed, inputs, top_low, grad_act, w_skip, w_in,
    source_out, normed_out, united_out, slope_out, chain_out,
):
    source = jnp.where(lax.axis_index("section") >= 2, received[...], embed[...])
    source_out[...] = source
    united = side_by_side(inputs).astype(F32) + dot(w_skip[...], source, 0, 0)
    united_out[...] = united
    normed = (united * norm_of(united)).astype(LOW)
    normed_out[...] = normed
    preact = dot(w_in[...], normed, 0, 0)
    sigma = sigmoid(preact)
    slope = sigma * (1.0 + preact * (1.0 - sigma))
    slope_out[...] = slope
    chain_out[...] = back_through(top_low[...].astype(F32), grad_act[...], united, slope, w_in)


def back_body(chain, w_skip, back_out):
    back_out[...] = dot(w_skip[...], chain[...], 1, 0).astype(LOW)


def tick_body(received, united, slope, w_in, w_out, chain_out):
    low = received[...]
    grad_act = dot(w_out[...], low, 0, 0)
    chain_out[...] = back_through(low.astype(F32), grad_act, united[...], slope[...], w_in)


def mirror_tick_body(
    received, w_mirror, united, slope, w_in, w_out, skip_far, back_2, chain_2, chain_3,
    chain_out, low_out, next_out,
):
    back = dot(w_mirror[...], received[...], 1, 0).astype(LOW)
    grad_out = received[...].astype(F32) + back.astype(F32)
    low = grad_out.astype(LOW)
    low_out[...] = low
    grad_act = dot(w_out[...], low, 0, 0)
    chain = back_through(grad_out, grad_act, united[...], slope[...], w_in)
    chain_out[...] = chain
    section = lax.axis_index("section")
    ahead = (chain.astype(F32) + skip_far[...].astype(F32)).astype(LOW)
    ahead = jnp.where(
        section == 2, (chain_2[...].astype(F32) + back_2[...].astype(F32)).astype(LOW), ahead
    )
    next_out[...] = jnp.where(section == 3, chain_3[...], ahead)


def pick_body(received, skip_far, low_1, low_2, top_low, grad_low_out):
    own = (received[...].astype(F32) + skip_far[...].astype(F32)).astype(LOW)
    section = lax.axis_index("section")
    own = jnp.where(section == 1, low_1[...], own)
    own = jnp.where(section == 2, low_2[...], own)
    grad_low_out[...] = jnp.where(section == 3, top_low[...], own)


def merge_body(following, passed, out):
    out[...] = jnp.where(lax.axis_index("section") == 0, following[...], passed[...])


def last_body(
    grad_low, received, skip_far, united, slope, w_in, w_out, source, chain_1, chain_2,
    chain_3, kept_out, keep_out, give_out,
):
    grad_out = received[...].astype(F32) + skip_far[...].astype(F32)
    grad_act = dot(w_out[...], grad_low[...], 0, 0)
    section = lax.axis_index("section")
    kept = back_through(grad_out, grad_act, united[...], slope[...], w_in)
    kept = jnp.where(section == 1, chain_1[...], kept)
    kept = jnp.where(section == 2, chain_2[...], kept)
    kept = jnp.where(section == 3, chain_3[...], kept)
    kept_out[...] = kept
    partial = dot(source[...], kept, 1, 1)
    size = keep_out.shape[1]
    first_core = lax.axis_index("dp") % 2 == 0
    for block in range(keep_out.shape[0]):
        start = 2 * block * size
        even = partial[start : start + size, :]
        odd = partial[start + size : start + 2 * size, :]
        keep_out[block] = jnp.where(first_core, even, odd)
        give_out[block] = jnp.where(first_core, odd, even).astype(LOW)


def join_body(keep, given, own_out, near_out, pair_out):
    chip = lax.axis_index("dp") // 2

    def joined(mask):
        return keep[chip ^ mask] + given[chip ^ mask].astype(F32)

    own_out[...] = joined(0)
    near_out[...] = joined(1)
    pair_out[0] = joined(2).astype(LOW)
    pair_out[1] = joined(3).astype(LOW)


def meet_body(own, near, pair, own_out, near_out):
    own_out[...] = own[...] + pair[0].astype(F32)
    near_out[...] = (near[...] + pair[1].astype(F32)).astype(LOW)


def flatten(total, out, lanes, square):
    lanes[0] = total[:, :128]
    lanes[1] = total[:, 128:256]
    lanes[2] = jnp.concatenate([total[:, 256:], total[:, 256:]], axis=1)
    half = total.shape[0] // 2
    even = [lanes[part, pl.ds(0, half, stride=2), :] for part in range(3)]
    odd = [lanes[part, pl.ds(1, half, stride=2), :] for part in range(3)]
    lines = [
        even[0],
        even[1],
        jnp.concatenate([even[2][:, :64], odd[0][:, :64]], axis=1),
        jnp.concatenate([odd[0][:, 64:], odd[1][:, :64]], axis=1),
        jnp.concatenate([odd[1][:, 64:], odd[2][:, :64]], axis=1),
    ]
    for place, line in enumerate(lines):
        square[pl.ds(place, half, stride=5), :] = line
    for row in range(square.shape[0]):
        out[:, row * 128 : (row + 1) * 128] = square[row : row + 1, :]


def cut_body(w_in, w_out, own_in, own_out):
    part = own_in.shape[1]
    place = lax.axis_index("dp")
    for index in range(w_in.shape[1] // part):

        @pl.when(place == index)
        def _():
            columns = slice(index * part, (index + 1) * part)
            own_in[...] = w_in[:, columns]
            own_out[...] = w_out[:, columns]


def curve(preact):
    sigma = sigmoid(preact)
    return (preact * sigma).astype(LOW), sigma * (1.0 + preact * (1.0 - sigma))


def slice_forward_body(own_in, *refs):
    blocks, active_out, slope_out = refs[:-2], refs[-2], refs[-1]
    rows = blocks[0].shape[1]
    for place, block in enumerate(blocks):
        columns = slice(place * rows, (place + 1) * rows)
        active_out[:, columns], slope_out[:, columns] = curve(dot(own_in[...], block[...], 0, 0))


def side(refs):
    return jnp.concatenate([block[...] for block in refs], axis=1)


def slice_grad(own_out, active, slope, normed, low):
    grad_pre = (dot(own_out[...], low, 0, 0) * slope).astype(LOW)
    return dot(grad_pre, normed, 1, 1), dot(active, low, 1, 1)


def half_grad_body(own_out, active, slope, *refs):
    half = (len(refs) - 2) // 2
    refs[-2][...], refs[-1][...] = slice_grad(
        own_out, active[...], slope[...], side(refs[:half]), side(refs[half : 2 * half])
    )


def rest_body(
    own_in, own_out, sum_in, sum_out, normed_0, normed_1, low_0, low_1, own, near, kept,
    in_out, out_out, skip_out, kept_out, lanes, square,
):
    span = kept_out.shape[2]
    for m in range(kept_out.shape[0]):
        kept_out[m] = kept[:, m * span : (m + 1) * span]
    flatten(own[...] + near[...].astype(F32), skip_out, lanes, square)
    normed = side([normed_0, normed_1])
    active, slope = curve(dot(own_in[...], normed, 0, 0))
    part_in, part_out = slice_grad(own_out, active, slope, normed, side([low_0, low_1]))
    in_out[...] = sum_in[...] + part_in
    out_out[...] = sum_out[...] + part_out


def hop(value, pairs):
    return lax.ppermute(value, "section", pairs)


def exchange(value, count, mask):
    return lax.ppermute(value, "dp", [(i, i ^ mask) for i in range(count)])


def from_next(value, count, mask):
    return lax.ppermute(
        value, ("section", "dp"), [(count + i, i ^ mask) for i in range(count)]
    )


def forwarded(value, count, mask):
    pairs = [
        (section * count + i, section * count + (i ^ mask))
        for section in range(1, 4)
        for i in range(count)
    ]
    return lax.ppermute(value, ("section", "dp"), pairs)


def program(saved_inputs, timesteps, time_table, skip_weight, ff_in, ff_out, output_cotangent):
    section = lax.axis_index("section")
    count = lax.axis_size("dp")
    n_micro = saved_inputs.shape[1]
    width = saved_inputs.shape[3]
    span = saved_inputs.shape[2]
    rows = n_micro * span
    hidden = ff_in.shape[1]
    inputs = jnp.swapaxes(saved_inputs[0], 1, 2)
    upstream = jnp.swapaxes(output_cotangent, 1, 2)
    table = time_table.T
    w_skip = skip_weight[0]
    w_in = ff_in[0].T
    w_out = ff_out[0].T
    low = ((width, rows), LOW)
    wide = ((hidden, rows), F32)

    distant = (timesteps, table, w_skip, inputs, w_in, w_out)
    embed, value, w_skip, inputs, w_in, w_out = call(
        encode_body, [low, low] + [(arg.shape, arg.dtype) for arg in distant[2:]],
        *distant,
        scratch=[pltpu.VMEM(arg.shape, arg.dtype) for arg in distant[:2]]
        + [pltpu.SemaphoreType.DMA((len(distant),))],
        far=range(len(distant)),
    )
    received = hop(value, [(0, 3), (1, 2)])
    top_low, grad_act = call(early_body, [low, wide], upstream, w_out)
    source, normed, united, slope, chain_3 = call(
        decode_body, [low, low, ((width, rows), F32), wide, low],
        received, embed, inputs, top_low, grad_act, w_skip, w_in,
    )
    chain = hop(chain_3, [(3, 2)])
    w_mirror = hop(w_skip, [(2, 1)])
    (back,) = call(back_body, [low], chain_3, w_skip)
    skip_far = hop(back, [(3, 0)])
    skip_next = hop(back, [(3, 1)])
    low_2 = chain
    (chain_2,) = call(tick_body, [low], chain, united, slope, w_in, w_out)
    chain = hop(chain_2, [(2, 1)])
    (back_2,) = call(back_body, [low], chain_2, w_skip)
    chain_1, low_1, ahead = call(
        mirror_tick_body, [low, low, low],
        chain, w_mirror, united, slope, w_in, w_out, skip_next, back_2, chain_2, chain_3,
    )
    chain = hop(chain_1, [(1, 0)])
    (grad_low,) = call(pick_body, [low], chain, skip_far, low_1, low_2, top_low)

    if not (count == 8 and count * rows <= 4096 and width % 128 == 64 and width // 128 == 2):
        return by_reduction(
            section, chain, skip_far, united, slope, w_in, w_out, source, normed, grad_low,
            (chain_1, chain_2, chain_3), saved_inputs.shape,
        )

    part = hidden // count
    own_in, own_out = call(cut_body, [((width, part), LOW)] * 2, w_in, w_out)
    norm_2, norm_4 = (exchange(normed, count, m) for m in (2, 4))
    normed_near = [normed, norm_2, norm_4, exchange(norm_4, count, 2)]
    normed_swap = [exchange(x, count, 1) for x in normed_near]
    normed_most = normed_near[:3] + normed_swap[:3]
    most = len(normed_most)
    active_most, slope_most = call(
        slice_forward_body,
        [((part, most * rows), LOW), ((part, most * rows), F32)], own_in, *normed_most,
    )
    next_6 = from_next(ahead, count, 6)
    low_2, low_4 = (exchange(grad_low, count, m) for m in (2, 4))
    passed_6 = forwarded(low_4, count, 2)
    (low_6,) = call(merge_body, [low], next_6, passed_6)
    low_near = [grad_low, low_2, low_4, low_6]
    low_swap = [exchange(x, count, 1) for x in low_near]
    block = (count // 2, width // count, width)
    kept, keep, give = call(
        last_body, [low, (block, F32), (block, LOW)],
        grad_low, chain, skip_far, united, slope, w_in, w_out, source, chain_1, chain_2,
        chain_3,
    )
    given = exchange(give, count, 1)
    piece = block[1:]
    own, near, pair = call(join_body, [(piece, F32), (piece, F32), ((2, *piece), LOW)], keep, given)
    pair = exchange(pair, count, 4)
    own, near = call(meet_body, [(piece, F32), (piece, LOW)], own, near, pair)
    near = exchange(near, count, 2)
    grads = ((part, width), F32)
    sums = call(
        half_grad_body, [grads] * 2,
        own_out, active_most, slope_most, *normed_most, *low_near[:3], *low_swap[:3],
    )
    grad_in, grad_out_w, grad_skip, kept = call(
        rest_body,
        [grads, grads, ((1, piece[0] * piece[1]), F32), ((n_micro, width, span), LOW)],
        own_in, own_out, *sums, normed_near[3], normed_swap[3], low_near[3], low_swap[3],
        own, near, kept,
        scratch=[
            pltpu.VMEM((3, piece[0], 128), F32),
            pltpu.VMEM((piece[0] * piece[1] // 128, 128), F32),
        ],
    )
    kept = jnp.swapaxes(kept, 1, 2)
    return (kept[None], grad_skip, grad_in[None], grad_out_w[None])


def by_reduction(
    section, chain, skip_far, united, slope, w_in, w_out, source, normed, grad_low, chains,
    shape,
):
    grad_out = chain.astype(F32) + skip_far.astype(F32)
    grad_pre = (dot(w_out, grad_low, 0, 0) * slope).astype(LOW)
    preact = dot(w_in, normed, 0, 0)
    active = (preact * jax.nn.sigmoid(preact)).astype(LOW)
    own_pre = (dot(w_out, grad_out.astype(LOW), 0, 0) * slope).astype(LOW)
    grad_norm = dot(w_in, own_pre, 1, 0)
    recip = norm_of(united)
    along = jnp.mean(grad_norm * united, axis=0, keepdims=True)
    kept = (grad_out + recip * grad_norm - united * (recip * recip * recip * along)).astype(LOW)
    for owner, other in enumerate(chains, 1):
        kept = jnp.where(section == owner, other, kept)
    grad_in, grad_out_w, grad_skip = (
        lax.psum_scatter(value, "dp", scatter_dimension=0, tiled=True)
        for value in (
            dot(grad_pre, normed, 1, 1),
            dot(active, grad_low, 1, 1),
            dot(source, kept, 1, 1).reshape(-1),
        )
    )
    kept = kept.reshape(shape[3], shape[1], shape[2]).transpose(1, 2, 0)
    return (kept[None], grad_skip[None], grad_in[None], grad_out_w[None])


def solution(mesh):
    in_specs = (
        P("section", None, "dp", None),
        P(None, "dp"),
        P(),
        P("section", None, None),
        P("section", None, None),
        P("section", None, None),
        P(None, "dp", None),
    )
    out_specs = (
        P("section", None, "dp", None),
        P("section", "dp"),
        P("section", "dp", None),
        P("section", "dp", None),
    )
    return jax.shard_map(program, mesh=mesh, in_specs=in_specs, out_specs=out_specs, check_vma=False)
```

```python
from functools import partial


import jax
import jax.numpy as jnp
from jax import lax
from jax.experimental import pallas as pl
from jax.experimental.pallas import tpu as pltpu
from jax.sharding import PartitionSpec as P


EPS = 1e-06
LOW = jnp.bfloat16
F32 = jnp.float32
VMEM_BYTES = 20 * 1024 * 1024


def contract(left, right, dims):
    return lax.dot_general(left, right, ((dims[0], dims[1]), ((), ())), preferred_element_type=F32)


def dot(left, right, on_left, on_right):
    return contract(left, right, ((on_left,), (on_right,)))


def call(body, outs, *args, scratch=(), far=()):
    places = [
        pltpu.SMEM if arg.ndim == 1 else pltpu.HBM if index in far else pltpu.VMEM
        for index, arg in enumerate(args)
    ]
    args = [
        pltpu.with_memory_space_constraint(arg, pltpu.HBM) if index in far else arg
        for index, arg in enumerate(args)
    ]
    return pl.pallas_call(
        body,
        out_shape=[jax.ShapeDtypeStruct(shape, kind) for shape, kind in outs],
        in_specs=[pl.BlockSpec(memory_space=place) for place in places],
        out_specs=[pl.BlockSpec(memory_space=pltpu.VMEM) for _ in outs],
        scratch_shapes=list(scratch),
        compiler_params=pltpu.CompilerParams(vmem_limit_bytes=VMEM_BYTES),
    )(*args)


def side_by_side(ref):
    return jnp.concatenate([ref[m] for m in range(ref.shape[0])], axis=1)


def norm_of(united):
    return lax.rsqrt(jnp.mean(united * united, axis=0, keepdims=True) + EPS)


def sigmoid(value):
    return 1.0 / (1.0 + jnp.exp(-value))


def encode_body(*refs):
    distant, (embed_out, value_out), kept, local, sems = (
        refs[:6], refs[6:8], refs[8:12], refs[12:14], refs[14],
    )
    local = (*local, *kept)
    copies = [
        pltpu.make_async_copy(source, target, sems.at[index])
        for index, (source, target) in enumerate(zip(distant, local))
    ]
    for copy in copies:
        copy.start()
    times, table, w_skip, inputs, w_in, w_out = local
    encoder = lax.axis_index("section") < 2

    @pl.when(encoder)
    def _():
        copies[0].wait()
        levels = lax.broadcasted_iota(jnp.int32, (table.shape[1], times.shape[1]), 0)
        hot = [
            jnp.where(levels == times[m : m + 1, :], 1.0, 0.0).astype(LOW)
            for m in range(times.shape[0])
        ]
        copies[1].wait()
        embed = dot(table[...], jnp.concatenate(hot, axis=1), 1, 0).astype(LOW)
        embed_out[...] = embed
        copies[2].wait()
        copies[3].wait()
        united = side_by_side(inputs).astype(F32) + dot(w_skip[...], embed, 0, 0)
        normed = (united * norm_of(united)).astype(LOW)
        copies[4].wait()
        preact = dot(w_in[...], normed, 0, 0)
        active = (preact * sigmoid(preact)).astype(LOW)
        copies[5].wait()
        value_out[...] = (united + dot(w_out[...], active, 1, 0)).astype(LOW)

    @pl.when(jnp.logical_not(encoder))
    def _():
        for copy in copies:
            copy.wait()


def active_in(section):
    return pl.when(lax.axis_index("section") == section)


def early_body(upstream, w_out, low_out, grad_act_out):
    low = side_by_side(upstream)
    low_out[...] = low

    @active_in(3)
    def _():
        grad_act_out[...] = dot(w_out[...], low, 0, 0)


def back_through(grad_out, grad_act, united, slope, w_in):
    grad_pre = (grad_act * slope).astype(LOW)
    grad_norm = dot(w_in[...], grad_pre, 1, 0)
    recip = norm_of(united)
    along = jnp.mean(grad_norm * united, axis=0, keepdims=True)
    return (grad_out + recip * grad_norm - united * (recip * recip * recip * along)).astype(LOW)


def decode_body(
    received, embed, inputs, top_low, grad_act, w_skip, w_in,
    source_out, normed_out, united_out, slope_out, chain_out,
):
    source = jnp.where(lax.axis_index("section") >= 2, received[...], embed[...])
    source_out[...] = source
    united = side_by_side(inputs).astype(F32) + dot(w_skip[...], source, 0, 0)
    united_out[...] = united
    normed = (united * norm_of(united)).astype(LOW)
    normed_out[...] = normed
    preact = dot(w_in[...], normed, 0, 0)
    sigma = sigmoid(preact)
    slope = sigma * (1.0 + preact * (1.0 - sigma))
    slope_out[...] = slope

    @active_in(3)
    def _():
        chain_out[...] = back_through(
            top_low[...].astype(F32), grad_act[...], united, slope, w_in
        )


def back_body(owner, chain, w_skip, back_out):
    @active_in(owner)
    def _():
        back_out[...] = dot(w_skip[...], chain[...], 1, 0).astype(LOW)


def tick_body(received, united, slope, w_in, w_out, chain_out):
    @active_in(2)
    def _():
        low = received[...]
        grad_act = dot(w_out[...], low, 0, 0)
        chain_out[...] = back_through(low.astype(F32), grad_act, united[...], slope[...], w_in)


def mirror_tick_body(
    received, w_mirror, united, slope, w_in, w_out, skip_far, back_2, chain_2, chain_3,
    chain_out, low_out, next_out,
):
    @active_in(1)
    def _():
        back = dot(w_mirror[...], received[...], 1, 0).astype(LOW)
        grad_out = received[...].astype(F32) + back.astype(F32)
        low = grad_out.astype(LOW)
        low_out[...] = low
        grad_act = dot(w_out[...], low, 0, 0)
        chain = back_through(grad_out, grad_act, united[...], slope[...], w_in)
        chain_out[...] = chain
        next_out[...] = (chain.astype(F32) + skip_far[...].astype(F32)).astype(LOW)

    @active_in(2)
    def _():
        next_out[...] = (chain_2[...].astype(F32) + back_2[...].astype(F32)).astype(LOW)

    @active_in(3)
    def _():
        next_out[...] = chain_3[...]


def pick_body(received, skip_far, low_1, low_2, top_low, grad_low_out):
    own = (received[...].astype(F32) + skip_far[...].astype(F32)).astype(LOW)
    section = lax.axis_index("section")
    own = jnp.where(section == 1, low_1[...], own)
    own = jnp.where(section == 2, low_2[...], own)
    grad_low_out[...] = jnp.where(section == 3, top_low[...], own)


def merge_body(top, following, out):
    out[...] = jnp.where(lax.axis_index("section") == 3, top[...], following[...])


def last_body(
    grad_low, received, skip_far, united, slope, w_in, w_out, source, chain_1, chain_2,
    chain_3, kept_out, keep_out, give_out,
):
    @active_in(0)
    def _():
        grad_out = received[...].astype(F32) + skip_far[...].astype(F32)
        grad_act = dot(w_out[...], grad_low[...], 0, 0)
        kept_out[...] = back_through(grad_out, grad_act, united[...], slope[...], w_in)

    for owner, chain in enumerate((chain_1, chain_2, chain_3), 1):

        @active_in(owner)
        def _():
            kept_out[...] = chain[...]

    product = dot(source[...], kept_out[...], 1, 1)
    size = keep_out.shape[1]
    first_core = lax.axis_index("dp") % 2 == 0
    for block in range(keep_out.shape[0]):
        start = 2 * block * size
        even = product[start : start + size, :]
        odd = product[start + size : start + 2 * size, :]
        keep_out[block] = jnp.where(first_core, even, odd)
        give_out[block] = jnp.where(first_core, odd, even).astype(LOW)


def join_body(keep, given, own_out, *piece_outs):
    chip = lax.axis_index("dp") // 2
    own_out[...] = keep[chip] + given[chip].astype(F32)
    for mask, piece_out in enumerate(piece_outs, 1):
        far = chip ^ mask
        piece_out[...] = (keep[far] + given[far].astype(F32)).astype(LOW)


def flatten(total, out, lanes, square):
    lanes[0] = total[:, :128]
    lanes[1] = total[:, 128:256]
    lanes[2] = jnp.concatenate([total[:, 256:], total[:, 256:]], axis=1)
    half = total.shape[0] // 2
    even = [lanes[part, pl.ds(0, half, stride=2), :] for part in range(3)]
    odd = [lanes[part, pl.ds(1, half, stride=2), :] for part in range(3)]
    lines = [
        even[0],
        even[1],
        jnp.concatenate([even[2][:, :64], odd[0][:, :64]], axis=1),
        jnp.concatenate([odd[0][:, 64:], odd[1][:, :64]], axis=1),
        jnp.concatenate([odd[1][:, 64:], odd[2][:, :64]], axis=1),
    ]
    for place, line in enumerate(lines):
        square[pl.ds(place, half, stride=5), :] = line
    for row in range(square.shape[0]):
        out[:, row * 128 : (row + 1) * 128] = square[row : row + 1, :]


def cut_body(w_in, w_out, own_in, own_out):
    part = own_in.shape[1]
    place = lax.axis_index("dp")
    for index in range(w_in.shape[1] // part):

        @pl.when(place == index)
        def _():
            columns = slice(index * part, (index + 1) * part)
            own_in[...] = w_in[:, columns]
            own_out[...] = w_out[:, columns]


def slice_forward_body(own_in, *refs):
    blocks, active_out, slope_out = refs[:-2], refs[-2], refs[-1]
    rows = blocks[0].shape[1]
    for place, block in enumerate(blocks):
        columns = slice(place * rows, (place + 1) * rows)
        preact = dot(own_in[...], block[...], 0, 0)
        sigma = sigmoid(preact)
        active_out[:, columns] = (preact * sigma).astype(LOW)
        slope_out[:, columns] = sigma * (1.0 + preact * (1.0 - sigma))


def slice_grad(own_out, active, slope, normed, low, first):
    rows = low[0].shape[1]
    columns = slice(first * rows, (first + len(low)) * rows)
    lows = jnp.concatenate([block[...] for block in low], axis=1)
    grad_pre = (dot(own_out[...], lows, 0, 0) * slope[:, columns]).astype(LOW)
    normeds = jnp.concatenate([block[...] for block in normed], axis=1)
    return dot(grad_pre, normeds, 1, 1), dot(active[:, columns], lows, 1, 1)


def half_grad_body(own_out, active, slope, *refs):
    half = (len(refs) - 2) // 2
    refs[-2][...], refs[-1][...] = slice_grad(
        own_out, active, slope, refs[:half], refs[half : 2 * half], 0
    )


def rest_grad_body(
    own_out, active, slope, sum_in, sum_out, normed_0, normed_1, low_0, low_1, own, piece_1,
    piece_2, piece_3, kept, in_out, out_out, skip_out, kept_out, lanes, square,
):
    span = kept_out.shape[2]
    for m in range(kept_out.shape[0]):
        kept_out[m] = kept[:, m * span : (m + 1) * span]
    total = own[...]
    for piece in (piece_1, piece_2, piece_3):
        total = total + piece[...].astype(F32)
    flatten(total, skip_out, lanes, square)
    first = active.shape[1] // normed_0.shape[1] - 2
    part_in, part_out = slice_grad(
        own_out, active, slope, (normed_0, normed_1), (low_0, low_1), first
    )
    in_out[...] = sum_in[...] + part_in
    out_out[...] = sum_out[...] + part_out


def hop(value, pairs):
    return lax.ppermute(value, "section", pairs)


def in_turn(near, swapped):
    return [*near[:3], *swapped[:3], near[3], swapped[3]]


def exchange(value, count, mask):
    return lax.ppermute(value, "dp", [(i, i ^ mask) for i in range(count)])


def from_next(value, count, mask):
    pairs = [
        ((section + 1) * count + i, section * count + (i ^ mask))
        for section in range(3)
        for i in range(count)
    ]
    return lax.ppermute(value, ("section", "dp"), pairs)


def in_last(value, count, mask):
    pairs = [(3 * count + i, 3 * count + (i ^ mask)) for i in range(count)]
    return lax.ppermute(value, ("section", "dp"), pairs)


def program(saved_inputs, timesteps, time_table, skip_weight, ff_in, ff_out, output_cotangent):
    section = lax.axis_index("section")
    count = lax.axis_size("dp")
    n_micro = saved_inputs.shape[1]
    width = saved_inputs.shape[3]
    span = saved_inputs.shape[2]
    rows = n_micro * span
    hidden = ff_in.shape[1]
    inputs = jnp.swapaxes(saved_inputs[0], 1, 2)
    upstream = jnp.swapaxes(output_cotangent, 1, 2)
    table = time_table.T
    w_skip = skip_weight[0]
    w_in = ff_in[0].T
    w_out = ff_out[0].T
    low = ((width, rows), LOW)
    wide = ((hidden, rows), F32)

    distant = (timesteps, table, w_skip, inputs, w_in, w_out)
    embed, value, w_skip, inputs, w_in, w_out = call(
        encode_body, [low, low] + [(arg.shape, arg.dtype) for arg in distant[2:]],
        *distant,
        scratch=[pltpu.VMEM(arg.shape, arg.dtype) for arg in distant[:2]]
        + [pltpu.SemaphoreType.DMA((len(distant),))],
        far=range(len(distant)),
    )
    received = hop(value, [(0, 3), (1, 2)])
    top_low, grad_act = call(early_body, [low, wide], upstream, w_out)
    source, normed, united, slope, chain_3 = call(
        decode_body, [low, low, ((width, rows), F32), wide, low],
        received, embed, inputs, top_low, grad_act, w_skip, w_in,
    )
    chain = hop(chain_3, [(3, 2)])
    w_mirror = hop(w_skip, [(2, 1)])
    (back,) = call(partial(back_body, 3), [low], chain_3, w_skip)
    skip_far = hop(back, [(3, 0)])
    skip_next = hop(back, [(3, 1)])
    low_2 = chain
    (chain_2,) = call(tick_body, [low], chain, united, slope, w_in, w_out)
    chain = hop(chain_2, [(2, 1)])
    (back_2,) = call(partial(back_body, 2), [low], chain_2, w_skip)
    chain_1, low_1, ahead = call(
        mirror_tick_body, [low, low, low],
        chain, w_mirror, united, slope, w_in, w_out, skip_next, back_2, chain_2, chain_3,
    )
    chain = hop(chain_1, [(1, 0)])
    (grad_low,) = call(pick_body, [low], chain, skip_far, low_1, low_2, top_low)

    if not (count == 8 and count * rows <= 4096 and width % 128 == 64 and width // 128 == 2):
        return by_reduction(
            section, chain, skip_far, united, slope, w_in, w_out, source, normed, grad_low,
            (chain_1, chain_2, chain_3), saved_inputs.shape,
        )

    part = hidden // count
    own_in, own_out = call(cut_body, [((width, part), LOW)] * 2, w_in, w_out)
    normed_near = [normed] + [exchange(normed, count, m) for m in (2, 6, 4)]
    normed_all = in_turn(
        normed_near,
        [exchange(x, count, 1) for x in normed_near],
    )
    active_all, slope_all = call(
        slice_forward_body,
        [((part, count * rows), LOW), ((part, count * rows), F32)], own_in, *normed_all,
    )
    top_6 = in_last(top_low, count, 6)
    next_6 = from_next(ahead, count, 6)
    (low_6,) = call(merge_body, [low], top_6, next_6)
    low_2, low_4 = (exchange(grad_low, count, m) for m in (2, 4))
    low_near = [grad_low, low_2, low_6, low_4]
    low_all = in_turn(low_near, [exchange(x, count, 1) for x in low_near])
    block = (count // 2, width // count, width)
    kept, keep, give = call(
        last_body, [low, (block, F32), (block, LOW)],
        grad_low, chain, skip_far, united, slope, w_in, w_out, source, chain_1, chain_2,
        chain_3,
    )
    given = exchange(give, count, 1)
    piece = block[1:]
    own, *pieces = call(
        join_body, [(piece, F32)] + [(piece, LOW)] * (count // 2 - 1),
        keep, given,
    )
    pieces = [exchange(value, count, 2 * i) for i, value in enumerate(pieces, 1)]
    grads = ((part, width), F32)
    half = 6
    sums = call(
        half_grad_body, [grads] * 2,
        own_out, active_all, slope_all, *normed_all[:half], *low_all[:half],
    )
    grad_in, grad_out_w, grad_skip, kept = call(
        rest_grad_body,
        [grads, grads, ((1, piece[0] * piece[1]), F32), ((n_micro, width, span), LOW)],
        own_out, active_all, slope_all, *sums, *normed_all[half:], *low_all[half:], own, *pieces,
        kept,
        scratch=[
            pltpu.VMEM((3, piece[0], 128), F32),
            pltpu.VMEM((piece[0] * piece[1] // 128, 128), F32),
        ],
    )
    kept = jnp.swapaxes(kept, 1, 2)
    return (kept[None], grad_skip, grad_in[None], grad_out_w[None])


def by_reduction(
    section, chain, skip_far, united, slope, w_in, w_out, source, normed, grad_low, chains,
    shape,
):
    grad_out = chain.astype(F32) + skip_far.astype(F32)
    grad_pre = (dot(w_out, grad_low, 0, 0) * slope).astype(LOW)
    preact = dot(w_in, normed, 0, 0)
    active = (preact * jax.nn.sigmoid(preact)).astype(LOW)
    own_pre = (dot(w_out, grad_out.astype(LOW), 0, 0) * slope).astype(LOW)
    grad_norm = dot(w_in, own_pre, 1, 0)
    recip = norm_of(united)
    along = jnp.mean(grad_norm * united, axis=0, keepdims=True)
    kept = (grad_out + recip * grad_norm - united * (recip * recip * recip * along)).astype(LOW)
    for owner, other in enumerate(chains, 1):
        kept = jnp.where(section == owner, other, kept)
    grad_in, grad_out_w, grad_skip = (
        lax.psum_scatter(value, "dp", scatter_dimension=0, tiled=True)
        for value in (
            dot(grad_pre, normed, 1, 1),
            dot(active, grad_low, 1, 1),
            dot(source, kept, 1, 1).reshape(-1),
        )
    )
    kept = kept.reshape(shape[3], shape[1], shape[2]).transpose(1, 2, 0)
    return (kept[None], grad_skip[None], grad_in[None], grad_out_w[None])


def solution(mesh):
    in_specs = (
        P("section", None, "dp", None),
        P(None, "dp"),
        P(),
        P("section", None, None),
        P("section", None, None),
        P("section", None, None),
        P(None, "dp", None),
    )
    out_specs = (
        P("section", None, "dp", None),
        P("section", "dp"),
        P("section", "dp", None),
        P("section", "dp", None),
    )
    return jax.shard_map(program, mesh=mesh, in_specs=in_specs, out_specs=out_specs, check_vma=False)
```

```python
from functools import partial


import jax
import jax.numpy as jnp
from jax import lax
from jax.experimental import pallas as pl
from jax.experimental.pallas import tpu as pltpu
from jax.sharding import PartitionSpec as P


EPS = 1e-06
LOW = jnp.bfloat16
F32 = jnp.float32
VMEM_BYTES = 20 * 1024 * 1024


def contract(left, right, dims):
    return lax.dot_general(left, right, ((dims[0], dims[1]), ((), ())), preferred_element_type=F32)


def dot(left, right, on_left, on_right):
    return contract(left, right, ((on_left,), (on_right,)))


def call(body, outs, *args, scratch=(), far=()):
    places = [
        pltpu.SMEM if arg.ndim == 1 else pltpu.HBM if index in far else pltpu.VMEM
        for index, arg in enumerate(args)
    ]
    args = [
        pltpu.with_memory_space_constraint(arg, pltpu.HBM) if index in far else arg
        for index, arg in enumerate(args)
    ]
    return pl.pallas_call(
        body,
        out_shape=[jax.ShapeDtypeStruct(shape, kind) for shape, kind in outs],
        in_specs=[pl.BlockSpec(memory_space=place) for place in places],
        out_specs=[pl.BlockSpec(memory_space=pltpu.VMEM) for _ in outs],
        scratch_shapes=list(scratch),
        compiler_params=pltpu.CompilerParams(vmem_limit_bytes=VMEM_BYTES),
    )(*args)


def side_by_side(ref):
    return jnp.concatenate([ref[m] for m in range(ref.shape[0])], axis=1)


def norm_of(united):
    return lax.rsqrt(jnp.mean(united * united, axis=0, keepdims=True) + EPS)


def sigmoid(value):
    return 1.0 / (1.0 + jnp.exp(-value))


def encode_body(*refs):
    distant, (embed_out, value_out), kept, local, sems = (
        refs[:6], refs[6:8], refs[8:12], refs[12:14], refs[14],
    )
    local = (*local, *kept)
    copies = [
        pltpu.make_async_copy(source, target, sems.at[index])
        for index, (source, target) in enumerate(zip(distant, local))
    ]
    for copy in copies:
        copy.start()
    times, table, w_skip, inputs, w_in, w_out = local
    encoder = lax.axis_index("section") < 2

    @pl.when(encoder)
    def _():
        copies[0].wait()
        levels = lax.broadcasted_iota(jnp.int32, (table.shape[1], times.shape[1]), 0)
        hot = [
            jnp.where(levels == times[m : m + 1, :], 1.0, 0.0).astype(LOW)
            for m in range(times.shape[0])
        ]
        copies[1].wait()
        embed = dot(table[...], jnp.concatenate(hot, axis=1), 1, 0).astype(LOW)
        embed_out[...] = embed
        copies[2].wait()
        copies[3].wait()
        united = side_by_side(inputs).astype(F32) + dot(w_skip[...], embed, 0, 0)
        normed = (united * norm_of(united)).astype(LOW)
        copies[4].wait()
        preact = dot(w_in[...], normed, 0, 0)
        active = (preact * sigmoid(preact)).astype(LOW)
        copies[5].wait()
        value_out[...] = (united + dot(w_out[...], active, 1, 0)).astype(LOW)

    @pl.when(jnp.logical_not(encoder))
    def _():
        for copy in copies:
            copy.wait()


def active_in(section):
    return pl.when(lax.axis_index("section") == section)


def early_body(upstream, w_out, low_out, grad_act_out):
    low = side_by_side(upstream)
    low_out[...] = low

    @active_in(3)
    def _():
        grad_act_out[...] = dot(w_out[...], low, 0, 0)


def back_through(grad_out, grad_act, united, slope, w_in):
    grad_pre = (grad_act * slope).astype(LOW)
    grad_norm = dot(w_in[...], grad_pre, 1, 0)
    recip = norm_of(united)
    along = jnp.mean(grad_norm * united, axis=0, keepdims=True)
    return (grad_out + recip * grad_norm - united * (recip * recip * recip * along)).astype(LOW)


def decode_body(
    received, embed, inputs, top_low, grad_act, w_skip, w_in,
    source_out, normed_out, united_out, slope_out, chain_out,
):
    source = jnp.where(lax.axis_index("section") >= 2, received[...], embed[...])
    source_out[...] = source
    united = side_by_side(inputs).astype(F32) + dot(w_skip[...], source, 0, 0)
    united_out[...] = united
    normed = (united * norm_of(united)).astype(LOW)
    normed_out[...] = normed
    preact = dot(w_in[...], normed, 0, 0)
    sigma = sigmoid(preact)
    slope = sigma * (1.0 + preact * (1.0 - sigma))
    slope_out[...] = slope

    @active_in(3)
    def _():
        chain_out[...] = back_through(
            top_low[...].astype(F32), grad_act[...], united, slope, w_in
        )


def back_body(owner, chain, w_skip, back_out):
    @active_in(owner)
    def _():
        back_out[...] = dot(w_skip[...], chain[...], 1, 0).astype(LOW)


def tick_body(received, united, slope, w_in, w_out, chain_out):
    @active_in(2)
    def _():
        low = received[...]
        grad_act = dot(w_out[...], low, 0, 0)
        chain_out[...] = back_through(low.astype(F32), grad_act, united[...], slope[...], w_in)


def mirror_tick_body(
    received, w_mirror, united, slope, w_in, w_out, skip_far, back_2, chain_2, chain_3,
    chain_out, low_out, next_out,
):
    @active_in(1)
    def _():
        back = dot(w_mirror[...], received[...], 1, 0).astype(LOW)
        grad_out = received[...].astype(F32) + back.astype(F32)
        low = grad_out.astype(LOW)
        low_out[...] = low
        grad_act = dot(w_out[...], low, 0, 0)
        chain = back_through(grad_out, grad_act, united[...], slope[...], w_in)
        chain_out[...] = chain
        next_out[...] = (chain.astype(F32) + skip_far[...].astype(F32)).astype(LOW)

    @active_in(2)
    def _():
        next_out[...] = (chain_2[...].astype(F32) + back_2[...].astype(F32)).astype(LOW)

    @active_in(3)
    def _():
        next_out[...] = chain_3[...]


def pick_body(received, skip_far, low_1, low_2, top_low, grad_low_out):
    own = (received[...].astype(F32) + skip_far[...].astype(F32)).astype(LOW)
    section = lax.axis_index("section")
    own = jnp.where(section == 1, low_1[...], own)
    own = jnp.where(section == 2, low_2[...], own)
    grad_low_out[...] = jnp.where(section == 3, top_low[...], own)


def merge_body(late, middle, top, out):
    section = lax.axis_index("section")
    out[...] = jnp.where(section == 0, late[...], jnp.where(section == 3, top[...], middle[...]))


def own_body(low_1, low_2, out):
    out[...] = jnp.where(lax.axis_index("section") == 1, low_1[...], low_2[...])


def last_body(
    grad_low, received, skip_far, united, slope, w_in, w_out, source, chain_1, chain_2,
    chain_3, kept_out, keep_out, give_out,
):
    @active_in(0)
    def _():
        grad_out = received[...].astype(F32) + skip_far[...].astype(F32)
        grad_act = dot(w_out[...], grad_low[...], 0, 0)
        kept_out[...] = back_through(grad_out, grad_act, united[...], slope[...], w_in)

    for owner, chain in enumerate((chain_1, chain_2, chain_3), 1):

        @active_in(owner)
        def _():
            kept_out[...] = chain[...]

    product = dot(source[...], kept_out[...], 1, 1)
    size = keep_out.shape[1]
    first_core = lax.axis_index("dp") % 2 == 0
    for block in range(keep_out.shape[0]):
        start = 2 * block * size
        even = product[start : start + size, :]
        odd = product[start + size : start + 2 * size, :]
        keep_out[block] = jnp.where(first_core, even, odd)
        give_out[block] = jnp.where(first_core, odd, even).astype(LOW)


def join_body(keep, given, own_out, *piece_outs):
    chip = lax.axis_index("dp") // 2
    own_out[...] = keep[chip] + given[chip].astype(F32)
    for mask, piece_out in enumerate(piece_outs, 1):
        far = chip ^ mask
        piece_out[...] = (keep[far] + given[far].astype(F32)).astype(LOW)


def flatten(total, out, lanes, square):
    lanes[0] = total[:, :128]
    lanes[1] = total[:, 128:256]
    lanes[2] = jnp.concatenate([total[:, 256:], total[:, 256:]], axis=1)
    half = total.shape[0] // 2
    even = [lanes[part, pl.ds(0, half, stride=2), :] for part in range(3)]
    odd = [lanes[part, pl.ds(1, half, stride=2), :] for part in range(3)]
    lines = [
        even[0],
        even[1],
        jnp.concatenate([even[2][:, :64], odd[0][:, :64]], axis=1),
        jnp.concatenate([odd[0][:, 64:], odd[1][:, :64]], axis=1),
        jnp.concatenate([odd[1][:, 64:], odd[2][:, :64]], axis=1),
    ]
    for place, line in enumerate(lines):
        square[pl.ds(place, half, stride=5), :] = line
    for row in range(square.shape[0]):
        out[:, row * 128 : (row + 1) * 128] = square[row : row + 1, :]


def cut_body(w_in, w_out, own_in, own_out):
    part = own_in.shape[1]
    place = lax.axis_index("dp")
    for index in range(w_in.shape[1] // part):

        @pl.when(place == index)
        def _():
            columns = slice(index * part, (index + 1) * part)
            own_in[...] = w_in[:, columns]
            own_out[...] = w_out[:, columns]


def slice_forward_body(own_in, *refs):
    blocks, active_out, slope_out = refs[:-2], refs[-2], refs[-1]
    rows = blocks[0].shape[1]
    for place, block in enumerate(blocks):
        columns = slice(place * rows, (place + 1) * rows)
        preact = dot(own_in[...], block[...], 0, 0)
        sigma = sigmoid(preact)
        active_out[:, columns] = (preact * sigma).astype(LOW)
        slope_out[:, columns] = sigma * (1.0 + preact * (1.0 - sigma))


def slice_grad(own_out, active, slope, normed, low, first):
    rows = low[0].shape[1]
    columns = slice(first * rows, (first + len(low)) * rows)
    lows = jnp.concatenate([block[...] for block in low], axis=1)
    grad_pre = (dot(own_out[...], lows, 0, 0) * slope[:, columns]).astype(LOW)
    normeds = jnp.concatenate([block[...] for block in normed], axis=1)
    return dot(grad_pre, normeds, 1, 1), dot(active[:, columns], lows, 1, 1)


def half_grad_body(own_out, active, slope, *refs):
    half = (len(refs) - 2) // 2
    refs[-2][...], refs[-1][...] = slice_grad(
        own_out, active, slope, refs[:half], refs[half : 2 * half], 0
    )


def rest_grad_body(
    own_out, active, slope, sum_in, sum_out, normed_0, normed_1, low_0, low_1, own, piece_1,
    piece_2, piece_3, kept, in_out, out_out, skip_out, kept_out, lanes, square,
):
    span = kept_out.shape[2]
    for m in range(kept_out.shape[0]):
        kept_out[m] = kept[:, m * span : (m + 1) * span]
    total = own[...]
    for piece in (piece_1, piece_2, piece_3):
        total = total + piece[...].astype(F32)
    flatten(total, skip_out, lanes, square)
    first = active.shape[1] // normed_0.shape[1] - 2
    part_in, part_out = slice_grad(
        own_out, active, slope, (normed_0, normed_1), (low_0, low_1), first
    )
    in_out[...] = sum_in[...] + part_in
    out_out[...] = sum_out[...] + part_out


def hop(value, pairs):
    return lax.ppermute(value, "section", pairs)


def in_turn(near, swapped):
    return [*near[:3], *swapped[:3], near[3], swapped[3]]


def exchange(value, count, mask):
    return lax.ppermute(value, "dp", [(i, i ^ mask) for i in range(count)])


def from_next(value, count, mask):
    pairs = [
        ((section + 1) * count + i, section * count + (i ^ mask))
        for section in range(3)
        for i in range(count)
    ]
    return lax.ppermute(value, ("section", "dp"), pairs)


def within(value, sections, count, mask):
    pairs = [
        (section * count + i, section * count + (i ^ mask))
        for section in sections
        for i in range(count)
    ]
    return lax.ppermute(value, ("section", "dp"), pairs)


def program(saved_inputs, timesteps, time_table, skip_weight, ff_in, ff_out, output_cotangent):
    section = lax.axis_index("section")
    count = lax.axis_size("dp")
    n_micro = saved_inputs.shape[1]
    width = saved_inputs.shape[3]
    span = saved_inputs.shape[2]
    rows = n_micro * span
    hidden = ff_in.shape[1]
    inputs = jnp.swapaxes(saved_inputs[0], 1, 2)
    upstream = jnp.swapaxes(output_cotangent, 1, 2)
    table = time_table.T
    w_skip = skip_weight[0]
    w_in = ff_in[0].T
    w_out = ff_out[0].T
    low = ((width, rows), LOW)
    wide = ((hidden, rows), F32)

    distant = (timesteps, table, w_skip, inputs, w_in, w_out)
    embed, value, w_skip, inputs, w_in, w_out = call(
        encode_body, [low, low] + [(arg.shape, arg.dtype) for arg in distant[2:]],
        *distant,
        scratch=[pltpu.VMEM(arg.shape, arg.dtype) for arg in distant[:2]]
        + [pltpu.SemaphoreType.DMA((len(distant),))],
        far=range(len(distant)),
    )
    received = hop(value, [(0, 3), (1, 2)])
    top_low, grad_act = call(early_body, [low, wide], upstream, w_out)
    source, normed, united, slope, chain_3 = call(
        decode_body, [low, low, ((width, rows), F32), wide, low],
        received, embed, inputs, top_low, grad_act, w_skip, w_in,
    )
    chain = hop(chain_3, [(3, 2)])
    w_mirror = hop(w_skip, [(2, 1)])
    (back,) = call(partial(back_body, 3), [low], chain_3, w_skip)
    skip_far = hop(back, [(3, 0)])
    skip_next = hop(back, [(3, 1)])
    low_2 = chain
    (chain_2,) = call(tick_body, [low], chain, united, slope, w_in, w_out)
    chain = hop(chain_2, [(2, 1)])
    (back_2,) = call(partial(back_body, 2), [low], chain_2, w_skip)
    chain_1, low_1, ahead = call(
        mirror_tick_body, [low, low, low],
        chain, w_mirror, united, slope, w_in, w_out, skip_next, back_2, chain_2, chain_3,
    )
    chain = hop(chain_1, [(1, 0)])
    (grad_low,) = call(pick_body, [low], chain, skip_far, low_1, low_2, top_low)

    if not (count == 8 and count * rows <= 4096 and width % 128 == 64 and width // 128 == 2):
        return by_reduction(
            section, chain, skip_far, united, slope, w_in, w_out, source, normed, grad_low,
            (chain_1, chain_2, chain_3), saved_inputs.shape,
        )

    part = hidden // count
    own_in, own_out = call(cut_body, [((width, part), LOW)] * 2, w_in, w_out)
    normed_near = [normed] + [exchange(normed, count, m) for m in (2, 6, 4)]
    normed_all = in_turn(
        normed_near,
        [exchange(x, count, 1) for x in normed_near],
    )
    active_all, slope_all = call(
        slice_forward_body,
        [((part, count * rows), LOW), ((part, count * rows), F32)], own_in, *normed_all,
    )
    tops = {mask: within(top_low, [3], count, mask) for mask in (2, 4, 6)}
    (own_low,) = call(own_body, [low], low_1, low_2)
    next_6 = from_next(ahead, count, 6)
    middle = {mask: within(own_low, [1, 2], count, mask) for mask in (2, 4)}
    late = {mask: within(grad_low, [0], count, mask) for mask in (2, 4)}
    late[6] = middle[6] = next_6
    low_2, low_4, low_6 = (
        call(merge_body, [low], late[mask], middle[mask], tops[mask])[0]
        for mask in (2, 4, 6)
    )
    low_near = [grad_low, low_2, low_6, low_4]
    low_all = in_turn(low_near, [exchange(x, count, 1) for x in low_near])
    block = (count // 2, width // count, width)
    kept, keep, give = call(
        last_body, [low, (block, F32), (block, LOW)],
        grad_low, chain, skip_far, united, slope, w_in, w_out, source, chain_1, chain_2,
        chain_3,
    )
    given = exchange(give, count, 1)
    piece = block[1:]
    own, *pieces = call(
        join_body, [(piece, F32)] + [(piece, LOW)] * (count // 2 - 1),
        keep, given,
    )
    pieces = [exchange(value, count, 2 * i) for i, value in enumerate(pieces, 1)]
    grads = ((part, width), F32)
    half = 6
    sums = call(
        half_grad_body, [grads] * 2,
        own_out, active_all, slope_all, *normed_all[:half], *low_all[:half],
    )
    grad_in, grad_out_w, grad_skip, kept = call(
        rest_grad_body,
        [grads, grads, ((1, piece[0] * piece[1]), F32), ((n_micro, width, span), LOW)],
        own_out, active_all, slope_all, *sums, *normed_all[half:], *low_all[half:], own, *pieces,
        kept,
        scratch=[
            pltpu.VMEM((3, piece[0], 128), F32),
            pltpu.VMEM((piece[0] * piece[1] // 128, 128), F32),
        ],
    )
    kept = jnp.swapaxes(kept, 1, 2)
    return (kept[None], grad_skip, grad_in[None], grad_out_w[None])


def by_reduction(
    section, chain, skip_far, united, slope, w_in, w_out, source, normed, grad_low, chains,
    shape,
):
    grad_out = chain.astype(F32) + skip_far.astype(F32)
    grad_pre = (dot(w_out, grad_low, 0, 0) * slope).astype(LOW)
    preact = dot(w_in, normed, 0, 0)
    active = (preact * jax.nn.sigmoid(preact)).astype(LOW)
    own_pre = (dot(w_out, grad_out.astype(LOW), 0, 0) * slope).astype(LOW)
    grad_norm = dot(w_in, own_pre, 1, 0)
    recip = norm_of(united)
    along = jnp.mean(grad_norm * united, axis=0, keepdims=True)
    kept = (grad_out + recip * grad_norm - united * (recip * recip * recip * along)).astype(LOW)
    for owner, other in enumerate(chains, 1):
        kept = jnp.where(section == owner, other, kept)
    grad_in, grad_out_w, grad_skip = (
        lax.psum_scatter(value, "dp", scatter_dimension=0, tiled=True)
        for value in (
            dot(grad_pre, normed, 1, 1),
            dot(active, grad_low, 1, 1),
            dot(source, kept, 1, 1).reshape(-1),
        )
    )
    kept = kept.reshape(shape[3], shape[1], shape[2]).transpose(1, 2, 0)
    return (kept[None], grad_skip[None], grad_in[None], grad_out_w[None])


def solution(mesh):
    in_specs = (
        P("section", None, "dp", None),
        P(None, "dp"),
        P(),
        P("section", None, None),
        P("section", None, None),
        P("section", None, None),
        P(None, "dp", None),
    )
    out_specs = (
        P("section", None, "dp", None),
        P("section", "dp"),
        P("section", "dp", None),
        P("section", "dp", None),
    )
    return jax.shard_map(program, mesh=mesh, in_specs=in_specs, out_specs=out_specs, check_vma=False)
```

```python
from functools import partial


import jax
import jax.numpy as jnp
from jax import lax
from jax.experimental import pallas as pl
from jax.experimental.pallas import tpu as pltpu
from jax.sharding import PartitionSpec as P


EPS = 1e-06
LOW = jnp.bfloat16
F32 = jnp.float32
VMEM_BYTES = 20 * 1024 * 1024


def contract(left, right, dims):
    return lax.dot_general(left, right, ((dims[0], dims[1]), ((), ())), preferred_element_type=F32)


def dot(left, right, on_left, on_right):
    return contract(left, right, ((on_left,), (on_right,)))


def call(body, outs, *args, scratch=(), far=()):
    places = [
        pltpu.SMEM if arg.ndim == 1 else pltpu.HBM if index in far else pltpu.VMEM
        for index, arg in enumerate(args)
    ]
    args = [
        pltpu.with_memory_space_constraint(arg, pltpu.HBM) if index in far else arg
        for index, arg in enumerate(args)
    ]
    return pl.pallas_call(
        body,
        out_shape=[jax.ShapeDtypeStruct(shape, kind) for shape, kind in outs],
        in_specs=[pl.BlockSpec(memory_space=place) for place in places],
        out_specs=[pl.BlockSpec(memory_space=pltpu.VMEM) for _ in outs],
        scratch_shapes=list(scratch),
        compiler_params=pltpu.CompilerParams(vmem_limit_bytes=VMEM_BYTES),
    )(*args)


def side_by_side(ref):
    return jnp.concatenate([ref[m] for m in range(ref.shape[0])], axis=1)


def norm_of(united):
    return lax.rsqrt(jnp.mean(united * united, axis=0, keepdims=True) + EPS)


def sigmoid(value):
    return 1.0 / (1.0 + jnp.exp(-value))


def encode_body(*refs):
    distant, (embed_out, value_out), kept, local, sems = (
        refs[:6], refs[6:8], refs[8:12], refs[12:14], refs[14],
    )
    local = (*local, *kept)
    copies = [
        pltpu.make_async_copy(source, target, sems.at[index])
        for index, (source, target) in enumerate(zip(distant, local))
    ]
    for copy in copies:
        copy.start()
    times, table, w_skip, inputs, w_in, w_out = local
    encoder = lax.axis_index("section") < 2

    @pl.when(encoder)
    def _():
        copies[0].wait()
        levels = lax.broadcasted_iota(jnp.int32, (table.shape[1], times.shape[1]), 0)
        hot = [
            jnp.where(levels == times[m : m + 1, :], 1.0, 0.0).astype(LOW)
            for m in range(times.shape[0])
        ]
        copies[1].wait()
        embed = dot(table[...], jnp.concatenate(hot, axis=1), 1, 0).astype(LOW)
        embed_out[...] = embed
        copies[2].wait()
        copies[3].wait()
        united = side_by_side(inputs).astype(F32) + dot(w_skip[...], embed, 0, 0)
        normed = (united * norm_of(united)).astype(LOW)
        copies[4].wait()
        preact = dot(w_in[...], normed, 0, 0)
        active = (preact * sigmoid(preact)).astype(LOW)
        copies[5].wait()
        value_out[...] = (united + dot(w_out[...], active, 1, 0)).astype(LOW)

    @pl.when(jnp.logical_not(encoder))
    def _():
        for copy in copies:
            copy.wait()


def active_in(section):
    return pl.when(lax.axis_index("section") == section)


def early_body(upstream, w_out, low_out, grad_act_out):
    low = side_by_side(upstream)
    low_out[...] = low

    @active_in(3)
    def _():
        grad_act_out[...] = dot(w_out[...], low, 0, 0)


def back_through(grad_out, grad_act, united, slope, w_in):
    grad_pre = (grad_act * slope).astype(LOW)
    grad_norm = dot(w_in[...], grad_pre, 1, 0)
    recip = norm_of(united)
    along = jnp.mean(grad_norm * united, axis=0, keepdims=True)
    return (grad_out + recip * grad_norm - united * (recip * recip * recip * along)).astype(LOW)


def decode_body(
    received, embed, inputs, top_low, grad_act, w_skip, w_in,
    source_out, normed_out, united_out, slope_out, chain_out,
):
    source = jnp.where(lax.axis_index("section") >= 2, received[...], embed[...])
    source_out[...] = source
    united = side_by_side(inputs).astype(F32) + dot(w_skip[...], source, 0, 0)
    united_out[...] = united
    normed = (united * norm_of(united)).astype(LOW)
    normed_out[...] = normed
    preact = dot(w_in[...], normed, 0, 0)
    sigma = sigmoid(preact)
    slope = sigma * (1.0 + preact * (1.0 - sigma))
    slope_out[...] = slope

    @active_in(3)
    def _():
        chain_out[...] = back_through(
            top_low[...].astype(F32), grad_act[...], united, slope, w_in
        )


def back_body(owner, chain, w_skip, back_out):
    @active_in(owner)
    def _():
        back_out[...] = dot(w_skip[...], chain[...], 1, 0).astype(LOW)


def tick_body(received, united, slope, w_in, w_out, chain_out):
    @active_in(2)
    def _():
        low = received[...]
        grad_act = dot(w_out[...], low, 0, 0)
        chain_out[...] = back_through(low.astype(F32), grad_act, united[...], slope[...], w_in)


def mirror_tick_body(
    received, w_mirror, united, slope, w_in, w_out, skip_far, back_2, chain_2, chain_3,
    chain_out, low_out, next_out,
):
    @active_in(1)
    def _():
        back = dot(w_mirror[...], received[...], 1, 0).astype(LOW)
        grad_out = received[...].astype(F32) + back.astype(F32)
        low = grad_out.astype(LOW)
        low_out[...] = low
        grad_act = dot(w_out[...], low, 0, 0)
        chain = back_through(grad_out, grad_act, united[...], slope[...], w_in)
        chain_out[...] = chain
        next_out[...] = (chain.astype(F32) + skip_far[...].astype(F32)).astype(LOW)

    @active_in(2)
    def _():
        next_out[...] = (chain_2[...].astype(F32) + back_2[...].astype(F32)).astype(LOW)

    @active_in(3)
    def _():
        next_out[...] = chain_3[...]


def pick_body(received, skip_far, low_1, low_2, top_low, grad_low_out):
    own = (received[...].astype(F32) + skip_far[...].astype(F32)).astype(LOW)
    section = lax.axis_index("section")
    own = jnp.where(section == 1, low_1[...], own)
    own = jnp.where(section == 2, low_2[...], own)
    grad_low_out[...] = jnp.where(section == 3, top_low[...], own)


def merge_body(late, middle, top, out):
    section = lax.axis_index("section")
    out[...] = jnp.where(section == 0, late[...], jnp.where(section == 3, top[...], middle[...]))


def own_body(low_1, low_2, out):
    out[...] = jnp.where(lax.axis_index("section") == 1, low_1[...], low_2[...])


def last_body(
    grad_low, received, skip_far, united, slope, w_in, w_out, source, chain_1, chain_2,
    chain_3, kept_out, keep_out, give_out,
):
    @active_in(0)
    def _():
        grad_out = received[...].astype(F32) + skip_far[...].astype(F32)
        grad_act = dot(w_out[...], grad_low[...], 0, 0)
        kept_out[...] = back_through(grad_out, grad_act, united[...], slope[...], w_in)

    for owner, chain in enumerate((chain_1, chain_2, chain_3), 1):

        @active_in(owner)
        def _():
            kept_out[...] = chain[...]

    product = dot(source[...], kept_out[...], 1, 1)
    size = keep_out.shape[1]
    first_core = lax.axis_index("dp") % 2 == 0
    for block in range(keep_out.shape[0]):
        start = 2 * block * size
        even = product[start : start + size, :]
        odd = product[start + size : start + 2 * size, :]
        keep_out[block] = jnp.where(first_core, even, odd)
        give_out[block] = jnp.where(first_core, odd, even).astype(LOW)


def join_body(keep, given, own_out, *piece_outs):
    chip = lax.axis_index("dp") // 2
    own_out[...] = keep[chip] + given[chip].astype(F32)
    for mask, piece_out in enumerate(piece_outs, 1):
        far = chip ^ mask
        piece_out[...] = (keep[far] + given[far].astype(F32)).astype(LOW)


def flatten(total, out, lanes, square):
    lanes[0] = total[:, :128]
    lanes[1] = total[:, 128:256]
    lanes[2] = jnp.concatenate([total[:, 256:], total[:, 256:]], axis=1)
    half = total.shape[0] // 2
    even = [lanes[part, pl.ds(0, half, stride=2), :] for part in range(3)]
    odd = [lanes[part, pl.ds(1, half, stride=2), :] for part in range(3)]
    lines = [
        even[0],
        even[1],
        jnp.concatenate([even[2][:, :64], odd[0][:, :64]], axis=1),
        jnp.concatenate([odd[0][:, 64:], odd[1][:, :64]], axis=1),
        jnp.concatenate([odd[1][:, 64:], odd[2][:, :64]], axis=1),
    ]
    for place, line in enumerate(lines):
        square[pl.ds(place, half, stride=5), :] = line
    for row in range(square.shape[0]):
        out[:, row * 128 : (row + 1) * 128] = square[row : row + 1, :]


def cut_body(w_in, w_out, own_in, own_out):
    part = own_in.shape[1]
    place = lax.axis_index("dp")
    for index in range(w_in.shape[1] // part):

        @pl.when(place == index)
        def _():
            columns = slice(index * part, (index + 1) * part)
            own_in[...] = w_in[:, columns]
            own_out[...] = w_out[:, columns]


def slice_forward_body(own_in, *refs):
    blocks, active_out, slope_out = refs[:-2], refs[-2], refs[-1]
    rows = blocks[0].shape[1]
    for place, block in enumerate(blocks):
        columns = slice(place * rows, (place + 1) * rows)
        preact = dot(own_in[...], block[...], 0, 0)
        sigma = sigmoid(preact)
        active_out[:, columns] = (preact * sigma).astype(LOW)
        slope_out[:, columns] = sigma * (1.0 + preact * (1.0 - sigma))


def slice_grad(own_out, active, slope, normed, low, first):
    rows = low[0].shape[1]
    columns = slice(first * rows, (first + len(low)) * rows)
    lows = jnp.concatenate([block[...] for block in low], axis=1)
    grad_pre = (dot(own_out[...], lows, 0, 0) * slope[:, columns]).astype(LOW)
    normeds = jnp.concatenate([block[...] for block in normed], axis=1)
    return dot(grad_pre, normeds, 1, 1), dot(active[:, columns], lows, 1, 1)


def half_grad_body(own_out, active, slope, *refs):
    half = (len(refs) - 2) // 2
    refs[-2][...], refs[-1][...] = slice_grad(
        own_out, active, slope, refs[:half], refs[half : 2 * half], 0
    )


def rest_grad_body(
    own_out, active, slope, sum_in, sum_out, normed_0, normed_1, low_0, low_1, own, piece_1,
    piece_2, piece_3, kept, in_out, out_out, skip_out, kept_out, lanes, square,
):
    span = kept_out.shape[2]
    for m in range(kept_out.shape[0]):
        kept_out[m] = kept[:, m * span : (m + 1) * span]
    total = own[...]
    for piece in (piece_1, piece_2, piece_3):
        total = total + piece[...].astype(F32)
    flatten(total, skip_out, lanes, square)
    first = active.shape[1] // normed_0.shape[1] - 2
    part_in, part_out = slice_grad(
        own_out, active, slope, (normed_0, normed_1), (low_0, low_1), first
    )
    in_out[...] = sum_in[...] + part_in
    out_out[...] = sum_out[...] + part_out


def hop(value, pairs):
    return lax.ppermute(value, "section", pairs)


def in_turn(near, swapped):
    return [*near[:3], *swapped[:3], near[3], swapped[3]]


def exchange(value, count, mask):
    return lax.ppermute(value, "dp", [(i, i ^ mask) for i in range(count)])


def from_next(value, count, mask):
    pairs = [
        ((section + 1) * count + i, section * count + (i ^ mask))
        for section in range(3)
        for i in range(count)
    ]
    return lax.ppermute(value, ("section", "dp"), pairs)


def within(value, sections, count, mask):
    pairs = [
        (section * count + i, section * count + (i ^ mask))
        for section in sections
        for i in range(count)
    ]
    return lax.ppermute(value, ("section", "dp"), pairs)


def program(saved_inputs, timesteps, time_table, skip_weight, ff_in, ff_out, output_cotangent):
    section = lax.axis_index("section")
    count = lax.axis_size("dp")
    n_micro = saved_inputs.shape[1]
    width = saved_inputs.shape[3]
    span = saved_inputs.shape[2]
    rows = n_micro * span
    hidden = ff_in.shape[1]
    inputs = jnp.swapaxes(saved_inputs[0], 1, 2)
    upstream = jnp.swapaxes(output_cotangent, 1, 2)
    table = time_table.T
    w_skip = skip_weight[0]
    w_in = ff_in[0].T
    w_out = ff_out[0].T
    low = ((width, rows), LOW)
    wide = ((hidden, rows), F32)

    distant = (timesteps, table, w_skip, inputs, w_in, w_out)
    embed, value, w_skip, inputs, w_in, w_out = call(
        encode_body, [low, low] + [(arg.shape, arg.dtype) for arg in distant[2:]],
        *distant,
        scratch=[pltpu.VMEM(arg.shape, arg.dtype) for arg in distant[:2]]
        + [pltpu.SemaphoreType.DMA((len(distant),))],
        far=range(len(distant)),
    )
    received = hop(value, [(0, 3), (1, 2)])
    top_low, grad_act = call(early_body, [low, wide], upstream, w_out)
    source, normed, united, slope, chain_3 = call(
        decode_body, [low, low, ((width, rows), F32), wide, low],
        received, embed, inputs, top_low, grad_act, w_skip, w_in,
    )
    chain = hop(chain_3, [(3, 2)])
    w_mirror = hop(w_skip, [(2, 1)])
    (back,) = call(partial(back_body, 3), [low], chain_3, w_skip)
    skip_far = hop(back, [(3, 0)])
    skip_next = hop(back, [(3, 1)])
    low_2 = chain
    (chain_2,) = call(tick_body, [low], chain, united, slope, w_in, w_out)
    chain = hop(chain_2, [(2, 1)])
    (back_2,) = call(partial(back_body, 2), [low], chain_2, w_skip)
    chain_1, low_1, ahead = call(
        mirror_tick_body, [low, low, low],
        chain, w_mirror, united, slope, w_in, w_out, skip_next, back_2, chain_2, chain_3,
    )
    chain = hop(chain_1, [(1, 0)])
    (grad_low,) = call(pick_body, [low], chain, skip_far, low_1, low_2, top_low)

    if not (count == 8 and count * rows <= 4096 and width % 128 == 64 and width // 128 == 2):
        return by_reduction(
            section, chain, skip_far, united, slope, w_in, w_out, source, normed, grad_low,
            (chain_1, chain_2, chain_3), saved_inputs.shape,
        )

    part = hidden // count
    own_in, own_out = call(cut_body, [((width, part), LOW)] * 2, w_in, w_out)
    normed_near = [normed] + [exchange(normed, count, m) for m in (2, 6, 4)]
    normed_all = in_turn(
        normed_near,
        [exchange(x, count, 1) for x in normed_near],
    )
    active_all, slope_all = call(
        slice_forward_body,
        [((part, count * rows), LOW), ((part, count * rows), F32)], own_in, *normed_all,
    )
    tops = {mask: within(top_low, [3], count, mask) for mask in (2, 4, 6)}
    (own_low,) = call(own_body, [low], low_1, low_2)
    middle = {mask: from_next(ahead, count, mask) for mask in (2, 6)}
    middle[4] = within(own_low, [1, 2], count, 4)
    late = {**middle, 4: within(grad_low, [0], count, 4)}
    low_2, low_4, low_6 = (
        call(merge_body, [low], late[mask], middle[mask], tops[mask])[0]
        for mask in (2, 4, 6)
    )
    low_near = [grad_low, low_2, low_6, low_4]
    low_all = in_turn(low_near, [exchange(x, count, 1) for x in low_near])
    block = (count // 2, width // count, width)
    kept, keep, give = call(
        last_body, [low, (block, F32), (block, LOW)],
        grad_low, chain, skip_far, united, slope, w_in, w_out, source, chain_1, chain_2,
        chain_3,
    )
    given = exchange(give, count, 1)
    piece = block[1:]
    own, *pieces = call(
        join_body, [(piece, F32)] + [(piece, LOW)] * (count // 2 - 1),
        keep, given,
    )
    pieces = [exchange(value, count, 2 * i) for i, value in enumerate(pieces, 1)]
    grads = ((part, width), F32)
    half = 6
    sums = call(
        half_grad_body, [grads] * 2,
        own_out, active_all, slope_all, *normed_all[:half], *low_all[:half],
    )
    grad_in, grad_out_w, grad_skip, kept = call(
        rest_grad_body,
        [grads, grads, ((1, piece[0] * piece[1]), F32), ((n_micro, width, span), LOW)],
        own_out, active_all, slope_all, *sums, *normed_all[half:], *low_all[half:], own, *pieces,
        kept,
        scratch=[
            pltpu.VMEM((3, piece[0], 128), F32),
            pltpu.VMEM((piece[0] * piece[1] // 128, 128), F32),
        ],
    )
    kept = jnp.swapaxes(kept, 1, 2)
    return (kept[None], grad_skip, grad_in[None], grad_out_w[None])


def by_reduction(
    section, chain, skip_far, united, slope, w_in, w_out, source, normed, grad_low, chains,
    shape,
):
    grad_out = chain.astype(F32) + skip_far.astype(F32)
    grad_pre = (dot(w_out, grad_low, 0, 0) * slope).astype(LOW)
    preact = dot(w_in, normed, 0, 0)
    active = (preact * jax.nn.sigmoid(preact)).astype(LOW)
    own_pre = (dot(w_out, grad_out.astype(LOW), 0, 0) * slope).astype(LOW)
    grad_norm = dot(w_in, own_pre, 1, 0)
    recip = norm_of(united)
    along = jnp.mean(grad_norm * united, axis=0, keepdims=True)
    kept = (grad_out + recip * grad_norm - united * (recip * recip * recip * along)).astype(LOW)
    for owner, other in enumerate(chains, 1):
        kept = jnp.where(section == owner, other, kept)
    grad_in, grad_out_w, grad_skip = (
        lax.psum_scatter(value, "dp", scatter_dimension=0, tiled=True)
        for value in (
            dot(grad_pre, normed, 1, 1),
            dot(active, grad_low, 1, 1),
            dot(source, kept, 1, 1).reshape(-1),
        )
    )
    kept = kept.reshape(shape[3], shape[1], shape[2]).transpose(1, 2, 0)
    return (kept[None], grad_skip[None], grad_in[None], grad_out_w[None])


def solution(mesh):
    in_specs = (
        P("section", None, "dp", None),
        P(None, "dp"),
        P(),
        P("section", None, None),
        P("section", None, None),
        P("section", None, None),
        P(None, "dp", None),
    )
    out_specs = (
        P("section", None, "dp", None),
        P("section", "dp"),
        P("section", "dp", None),
        P("section", "dp", None),
    )
    return jax.shard_map(program, mesh=mesh, in_specs=in_specs, out_specs=out_specs, check_vma=False)
```

```python
import jax
import jax.numpy as jnp
from jax import lax
from jax.experimental import pallas as pl
from jax.experimental.pallas import tpu as pltpu
from jax.sharding import PartitionSpec as P


EPS = 1e-06
LOW = jnp.bfloat16
F32 = jnp.float32
VMEM_BYTES = 20 * 1024 * 1024


def contract(left, right, dims):
    return lax.dot_general(left, right, ((dims[0], dims[1]), ((), ())), preferred_element_type=F32)


def dot(left, right, on_left, on_right):
    return contract(left, right, ((on_left,), (on_right,)))


def call(body, outs, *args, scratch=(), far=()):
    places = [
        pltpu.SMEM if arg.ndim == 1 else pltpu.HBM if index in far else pltpu.VMEM
        for index, arg in enumerate(args)
    ]
    args = [
        pltpu.with_memory_space_constraint(arg, pltpu.HBM) if index in far else arg
        for index, arg in enumerate(args)
    ]
    return pl.pallas_call(
        body,
        out_shape=[jax.ShapeDtypeStruct(shape, kind) for shape, kind in outs],
        in_specs=[pl.BlockSpec(memory_space=place) for place in places],
        out_specs=[pl.BlockSpec(memory_space=pltpu.VMEM) for _ in outs],
        scratch_shapes=list(scratch),
        compiler_params=pltpu.CompilerParams(vmem_limit_bytes=VMEM_BYTES),
    )(*args)


def side_by_side(ref):
    return jnp.concatenate([ref[m] for m in range(ref.shape[0])], axis=1)


def norm_of(united):
    return lax.rsqrt(jnp.mean(united * united, axis=0, keepdims=True) + EPS)


def sigmoid(value):
    return 1.0 / (1.0 + jnp.exp(-value))


def encode_body(*refs):
    distant, (embed_out, value_out), kept, local, sems = (
        refs[:6], refs[6:8], refs[8:12], refs[12:14], refs[14],
    )
    local = (*local, *kept)
    copies = [
        pltpu.make_async_copy(source, target, sems.at[index])
        for index, (source, target) in enumerate(zip(distant, local))
    ]
    for copy in copies:
        copy.start()
    times, table, w_skip, inputs, w_in, w_out = local
    encoder = lax.axis_index("section") < 2

    @pl.when(encoder)
    def _():
        copies[0].wait()
        levels = lax.broadcasted_iota(jnp.int32, (table.shape[1], times.shape[1]), 0)
        hot = [
            jnp.where(levels == times[m : m + 1, :], 1.0, 0.0).astype(LOW)
            for m in range(times.shape[0])
        ]
        copies[1].wait()
        embed = dot(table[...], jnp.concatenate(hot, axis=1), 1, 0).astype(LOW)
        embed_out[...] = embed
        copies[2].wait()
        copies[3].wait()
        united = side_by_side(inputs).astype(F32) + dot(w_skip[...], embed, 0, 0)
        normed = (united * norm_of(united)).astype(LOW)
        copies[4].wait()
        preact = dot(w_in[...], normed, 0, 0)
        active = (preact * sigmoid(preact)).astype(LOW)
        copies[5].wait()
        value_out[...] = (united + dot(w_out[...], active, 1, 0)).astype(LOW)

    @pl.when(jnp.logical_not(encoder))
    def _():
        for copy in copies:
            copy.wait()


def active_in(section):
    return pl.when(lax.axis_index("section") == section)


def early_body(upstream, w_out, low_out, grad_act_out):
    low = side_by_side(upstream)
    low_out[...] = low

    @active_in(3)
    def _():
        grad_act_out[...] = dot(w_out[...], low, 0, 0)


def back_through(grad_out, grad_act, united, slope, w_in):
    grad_pre = (grad_act * slope).astype(LOW)
    grad_norm = dot(w_in[...], grad_pre, 1, 0)
    recip = norm_of(united)
    along = jnp.mean(grad_norm * united, axis=0, keepdims=True)
    return (grad_out + recip * grad_norm - united * (recip * recip * recip * along)).astype(LOW)


def decode_body(
    received, embed, inputs, top_low, grad_act, w_skip, w_in,
    source_out, normed_out, united_out, slope_out, chain_out,
):
    source = jnp.where(lax.axis_index("section") >= 2, received[...], embed[...])
    source_out[...] = source
    united = side_by_side(inputs).astype(F32) + dot(w_skip[...], source, 0, 0)
    united_out[...] = united
    normed = (united * norm_of(united)).astype(LOW)
    normed_out[...] = normed
    preact = dot(w_in[...], normed, 0, 0)
    sigma = sigmoid(preact)
    slope = sigma * (1.0 + preact * (1.0 - sigma))
    slope_out[...] = slope

    @active_in(3)
    def _():
        chain_out[...] = back_through(
            top_low[...].astype(F32), grad_act[...], united, slope, w_in
        )


def back_body(chain, w_skip, back_out):
    @active_in(3)
    def _():
        back_out[...] = dot(w_skip[...], chain[...], 1, 0).astype(LOW)


def prior_body(chain_2, chain_3, w_skip, prior_out):
    @active_in(2)
    def _():
        back = dot(w_skip[...], chain_2[...], 1, 0).astype(LOW)
        prior_out[...] = (chain_2[...].astype(F32) + back.astype(F32)).astype(LOW)

    @active_in(3)
    def _():
        prior_out[...] = chain_3[...]


def tick_body(received, united, slope, w_in, w_out, chain_out):
    @active_in(2)
    def _():
        low = received[...]
        grad_act = dot(w_out[...], low, 0, 0)
        chain_out[...] = back_through(low.astype(F32), grad_act, united[...], slope[...], w_in)


def mirror_tick_body(
    received, w_mirror, united, slope, w_in, w_out, skip_far, chain_out, low_out, next_out,
):
    @active_in(1)
    def _():
        back = dot(w_mirror[...], received[...], 1, 0).astype(LOW)
        grad_out = received[...].astype(F32) + back.astype(F32)
        low = grad_out.astype(LOW)
        low_out[...] = low
        grad_act = dot(w_out[...], low, 0, 0)
        chain = back_through(grad_out, grad_act, united[...], slope[...], w_in)
        chain_out[...] = chain
        next_out[...] = (chain.astype(F32) + skip_far[...].astype(F32)).astype(LOW)


def pick_body(received, skip_far, low_1, low_2, top_low, grad_low_out):
    own = (received[...].astype(F32) + skip_far[...].astype(F32)).astype(LOW)
    section = lax.axis_index("section")
    own = jnp.where(section == 1, low_1[...], own)
    own = jnp.where(section == 2, low_2[...], own)
    grad_low_out[...] = jnp.where(section == 3, top_low[...], own)


def merge_body(late, middle, top, out):
    section = lax.axis_index("section")
    out[...] = jnp.where(section == 0, late[...], jnp.where(section == 3, top[...], middle[...]))


def own_body(low_1, low_2, out):
    out[...] = jnp.where(lax.axis_index("section") == 1, low_1[...], low_2[...])


def last_body(
    grad_low, received, skip_far, united, slope, w_in, w_out, source, chain_1, chain_2,
    chain_3, kept_out, keep_out, give_out,
):
    @active_in(0)
    def _():
        grad_out = received[...].astype(F32) + skip_far[...].astype(F32)
        grad_act = dot(w_out[...], grad_low[...], 0, 0)
        kept_out[...] = back_through(grad_out, grad_act, united[...], slope[...], w_in)

    for owner, chain in enumerate((chain_1, chain_2, chain_3), 1):

        @active_in(owner)
        def _():
            kept_out[...] = chain[...]

    product = dot(source[...], kept_out[...], 1, 1)
    size = keep_out.shape[1]
    first_core = lax.axis_index("dp") % 2 == 0
    for block in range(keep_out.shape[0]):
        start = 2 * block * size
        even = product[start : start + size, :]
        odd = product[start + size : start + 2 * size, :]
        keep_out[block] = jnp.where(first_core, even, odd)
        give_out[block] = jnp.where(first_core, odd, even).astype(LOW)


def join_body(keep, given, own_out, *piece_outs):
    chip = lax.axis_index("dp") // 2
    own_out[...] = keep[chip] + given[chip].astype(F32)
    for mask, piece_out in enumerate(piece_outs, 1):
        far = chip ^ mask
        piece_out[...] = (keep[far] + given[far].astype(F32)).astype(LOW)


def flatten(total, out, lanes, square):
    lanes[0] = total[:, :128]
    lanes[1] = total[:, 128:256]
    lanes[2] = jnp.concatenate([total[:, 256:], total[:, 256:]], axis=1)
    half = total.shape[0] // 2
    even = [lanes[part, pl.ds(0, half, stride=2), :] for part in range(3)]
    odd = [lanes[part, pl.ds(1, half, stride=2), :] for part in range(3)]
    lines = [
        even[0],
        even[1],
        jnp.concatenate([even[2][:, :64], odd[0][:, :64]], axis=1),
        jnp.concatenate([odd[0][:, 64:], odd[1][:, :64]], axis=1),
        jnp.concatenate([odd[1][:, 64:], odd[2][:, :64]], axis=1),
    ]
    for place, line in enumerate(lines):
        square[pl.ds(place, half, stride=5), :] = line
    for row in range(square.shape[0]):
        out[:, row * 128 : (row + 1) * 128] = square[row : row + 1, :]


def cut_body(w_in, w_out, own_in, own_out):
    part = own_in.shape[1]
    place = lax.axis_index("dp")
    for index in range(w_in.shape[1] // part):

        @pl.when(place == index)
        def _():
            columns = slice(index * part, (index + 1) * part)
            own_in[...] = w_in[:, columns]
            own_out[...] = w_out[:, columns]


def slice_forward_body(own_in, *refs):
    blocks, active_out, slope_out = refs[:-2], refs[-2], refs[-1]
    rows = blocks[0].shape[1]
    for place, block in enumerate(blocks):
        columns = slice(place * rows, (place + 1) * rows)
        preact = dot(own_in[...], block[...], 0, 0)
        sigma = sigmoid(preact)
        active_out[:, columns] = (preact * sigma).astype(LOW)
        slope_out[:, columns] = sigma * (1.0 + preact * (1.0 - sigma))


def slice_grad(own_out, active, slope, normed, low, first):
    rows = low[0].shape[1]
    columns = slice(first * rows, (first + len(low)) * rows)
    lows = jnp.concatenate([block[...] for block in low], axis=1)
    grad_pre = (dot(own_out[...], lows, 0, 0) * slope[:, columns]).astype(LOW)
    normeds = jnp.concatenate([block[...] for block in normed], axis=1)
    return dot(grad_pre, normeds, 1, 1), dot(active[:, columns], lows, 1, 1)


def half_grad_body(own_out, active, slope, *refs):
    half = (len(refs) - 2) // 2
    refs[-2][...], refs[-1][...] = slice_grad(
        own_out, active, slope, refs[:half], refs[half : 2 * half], 0
    )


def rest_grad_body(
    own_out, active, slope, sum_in, sum_out, normed_0, normed_1, low_0, low_1, own, piece_1,
    piece_2, piece_3, kept, in_out, out_out, skip_out, kept_out, lanes, square,
):
    span = kept_out.shape[2]
    for m in range(kept_out.shape[0]):
        kept_out[m] = kept[:, m * span : (m + 1) * span]
    total = own[...]
    for piece in (piece_1, piece_2, piece_3):
        total = total + piece[...].astype(F32)
    flatten(total, skip_out, lanes, square)
    first = active.shape[1] // normed_0.shape[1] - 2
    part_in, part_out = slice_grad(
        own_out, active, slope, (normed_0, normed_1), (low_0, low_1), first
    )
    in_out[...] = sum_in[...] + part_in
    out_out[...] = sum_out[...] + part_out


def hop(value, pairs):
    return lax.ppermute(value, "section", pairs)


def in_turn(near, swapped):
    return [*near[:3], *swapped[:3], near[3], swapped[3]]


def exchange(value, count, mask):
    return lax.ppermute(value, "dp", [(i, i ^ mask) for i in range(count)])


def from_next(value, sections, count, mask):
    pairs = [
        ((section + 1) * count + i, section * count + (i ^ mask))
        for section in sections
        for i in range(count)
    ]
    return lax.ppermute(value, ("section", "dp"), pairs)


def within(value, sections, count, mask):
    pairs = [
        (section * count + i, section * count + (i ^ mask))
        for section in sections
        for i in range(count)
    ]
    return lax.ppermute(value, ("section", "dp"), pairs)


def program(saved_inputs, timesteps, time_table, skip_weight, ff_in, ff_out, output_cotangent):
    section = lax.axis_index("section")
    count = lax.axis_size("dp")
    n_micro = saved_inputs.shape[1]
    width = saved_inputs.shape[3]
    span = saved_inputs.shape[2]
    rows = n_micro * span
    hidden = ff_in.shape[1]
    inputs = jnp.swapaxes(saved_inputs[0], 1, 2)
    upstream = jnp.swapaxes(output_cotangent, 1, 2)
    table = time_table.T
    w_skip = skip_weight[0]
    w_in = ff_in[0].T
    w_out = ff_out[0].T
    low = ((width, rows), LOW)
    wide = ((hidden, rows), F32)

    distant = (timesteps, table, w_skip, inputs, w_in, w_out)
    embed, value, w_skip, inputs, w_in, w_out = call(
        encode_body, [low, low] + [(arg.shape, arg.dtype) for arg in distant[2:]],
        *distant,
        scratch=[pltpu.VMEM(arg.shape, arg.dtype) for arg in distant[:2]]
        + [pltpu.SemaphoreType.DMA((len(distant),))],
        far=range(len(distant)),
    )
    received = hop(value, [(0, 3), (1, 2)])
    top_low, grad_act = call(early_body, [low, wide], upstream, w_out)
    source, normed, united, slope, chain_3 = call(
        decode_body, [low, low, ((width, rows), F32), wide, low],
        received, embed, inputs, top_low, grad_act, w_skip, w_in,
    )
    chain = hop(chain_3, [(3, 2)])
    w_mirror = hop(w_skip, [(2, 1)])
    (back,) = call(back_body, [low], chain_3, w_skip)
    skip_far = hop(back, [(3, 0)])
    skip_next = hop(back, [(3, 1)])
    low_2 = chain
    (chain_2,) = call(tick_body, [low], chain, united, slope, w_in, w_out)
    chain = hop(chain_2, [(2, 1)])
    (prior,) = call(prior_body, [low], chain_2, chain_3, w_skip)
    chain_1, low_1, ahead = call(
        mirror_tick_body, [low, low, low],
        chain, w_mirror, united, slope, w_in, w_out, skip_next,
    )
    chain = hop(chain_1, [(1, 0)])
    (grad_low,) = call(pick_body, [low], chain, skip_far, low_1, low_2, top_low)

    if not (count == 8 and count * rows <= 4096 and width % 128 == 64 and width // 128 == 2):
        return by_reduction(
            section, chain, skip_far, united, slope, w_in, w_out, source, normed, grad_low,
            (chain_1, chain_2, chain_3), saved_inputs.shape,
        )

    part = hidden // count
    own_in, own_out = call(cut_body, [((width, part), LOW)] * 2, w_in, w_out)
    normed_near = [normed] + [exchange(normed, count, m) for m in (2, 6, 4)]
    normed_all = in_turn(
        normed_near,
        [exchange(x, count, 1) for x in normed_near],
    )
    active_all, slope_all = call(
        slice_forward_body,
        [((part, count * rows), LOW), ((part, count * rows), F32)], own_in, *normed_all,
    )
    tops = {mask: within(top_low, [3], count, mask) for mask in (2, 4)}
    tops[6] = within(tops[4], [3], count, 2)
    (own_low,) = call(own_body, [low], low_1, low_2)
    middle = {m: from_next(prior, [1, 2], count, m) for m in (2, 6)}
    middle[4] = within(own_low, [1, 2], count, 4)
    late = {m: from_next(ahead, [0], count, m) for m in (2, 6)}
    late[4] = within(grad_low, [0], count, 4)
    low_2, low_4, low_6 = (
        call(merge_body, [low], late[mask], middle[mask], tops[mask])[0]
        for mask in (2, 4, 6)
    )
    low_near = [grad_low, low_2, low_6, low_4]
    low_all = in_turn(low_near, [exchange(x, count, 1) for x in low_near])
    block = (count // 2, width // count, width)
    kept, keep, give = call(
        last_body, [low, (block, F32), (block, LOW)],
        grad_low, chain, skip_far, united, slope, w_in, w_out, source, chain_1, chain_2,
        chain_3,
    )
    given = exchange(give, count, 1)
    piece = block[1:]
    own, *pieces = call(
        join_body, [(piece, F32)] + [(piece, LOW)] * (count // 2 - 1),
        keep, given,
    )
    pieces = [exchange(value, count, 2 * i) for i, value in enumerate(pieces, 1)]
    grads = ((part, width), F32)
    half = 6
    sums = call(
        half_grad_body, [grads] * 2,
        own_out, active_all, slope_all, *normed_all[:half], *low_all[:half],
    )
    grad_in, grad_out_w, grad_skip, kept = call(
        rest_grad_body,
        [grads, grads, ((1, piece[0] * piece[1]), F32), ((n_micro, width, span), LOW)],
        own_out, active_all, slope_all, *sums, *normed_all[half:], *low_all[half:], own, *pieces,
        kept,
        scratch=[
            pltpu.VMEM((3, piece[0], 128), F32),
            pltpu.VMEM((piece[0] * piece[1] // 128, 128), F32),
        ],
    )
    kept = jnp.swapaxes(kept, 1, 2)
    return (kept[None], grad_skip, grad_in[None], grad_out_w[None])


def by_reduction(
    section, chain, skip_far, united, slope, w_in, w_out, source, normed, grad_low, chains,
    shape,
):
    grad_out = chain.astype(F32) + skip_far.astype(F32)
    grad_pre = (dot(w_out, grad_low, 0, 0) * slope).astype(LOW)
    preact = dot(w_in, normed, 0, 0)
    active = (preact * jax.nn.sigmoid(preact)).astype(LOW)
    own_pre = (dot(w_out, grad_out.astype(LOW), 0, 0) * slope).astype(LOW)
    grad_norm = dot(w_in, own_pre, 1, 0)
    recip = norm_of(united)
    along = jnp.mean(grad_norm * united, axis=0, keepdims=True)
    kept = (grad_out + recip * grad_norm - united * (recip * recip * recip * along)).astype(LOW)
    for owner, other in enumerate(chains, 1):
        kept = jnp.where(section == owner, other, kept)
    grad_in, grad_out_w, grad_skip = (
        lax.psum_scatter(value, "dp", scatter_dimension=0, tiled=True)
        for value in (
            dot(grad_pre, normed, 1, 1),
            dot(active, grad_low, 1, 1),
            dot(source, kept, 1, 1).reshape(-1),
        )
    )
    kept = kept.reshape(shape[3], shape[1], shape[2]).transpose(1, 2, 0)
    return (kept[None], grad_skip[None], grad_in[None], grad_out_w[None])


def solution(mesh):
    in_specs = (
        P("section", None, "dp", None),
        P(None, "dp"),
        P(),
        P("section", None, None),
        P("section", None, None),
        P("section", None, None),
        P(None, "dp", None),
    )
    out_specs = (
        P("section", None, "dp", None),
        P("section", "dp"),
        P("section", "dp", None),
        P("section", "dp", None),
    )
    return jax.shard_map(program, mesh=mesh, in_specs=in_specs, out_specs=out_specs, check_vma=False)
```

```python
import jax
import jax.numpy as jnp
from jax import lax
from jax.experimental import pallas as pl
from jax.experimental.pallas import tpu as pltpu
from jax.sharding import PartitionSpec as P


EPS = 1e-06
LOW = jnp.bfloat16
F32 = jnp.float32
VMEM_BYTES = 20 * 1024 * 1024


def contract(left, right, dims):
    return lax.dot_general(left, right, ((dims[0], dims[1]), ((), ())), preferred_element_type=F32)


def dot(left, right, on_left, on_right):
    return contract(left, right, ((on_left,), (on_right,)))


def call(body, outs, *args, scratch=(), far=()):
    places = [
        pltpu.SMEM if arg.ndim == 1 else pltpu.HBM if index in far else pltpu.VMEM
        for index, arg in enumerate(args)
    ]
    args = [
        pltpu.with_memory_space_constraint(arg, pltpu.HBM) if index in far else arg
        for index, arg in enumerate(args)
    ]
    return pl.pallas_call(
        body,
        out_shape=[jax.ShapeDtypeStruct(shape, kind) for shape, kind in outs],
        in_specs=[pl.BlockSpec(memory_space=place) for place in places],
        out_specs=[pl.BlockSpec(memory_space=pltpu.VMEM) for _ in outs],
        scratch_shapes=list(scratch),
        compiler_params=pltpu.CompilerParams(vmem_limit_bytes=VMEM_BYTES),
    )(*args)


def side_by_side(ref):
    return jnp.concatenate([ref[m] for m in range(ref.shape[0])], axis=1)


def norm_of(united):
    return lax.rsqrt(jnp.mean(united * united, axis=0, keepdims=True) + EPS)


def sigmoid(value):
    return 1.0 / (1.0 + jnp.exp(-value))


def encode_body(*refs):
    distant, (embed_out, value_out), kept, local, sems = (
        refs[:6], refs[6:8], refs[8:12], refs[12:14], refs[14],
    )
    local = (*local, *kept)
    copies = [
        pltpu.make_async_copy(source, target, sems.at[index])
        for index, (source, target) in enumerate(zip(distant, local))
    ]
    times, table, w_skip, inputs, w_in, w_out = local
    encoder = lax.axis_index("section") < 2

    @pl.when(encoder)
    def _():
        for copy in copies[:2]:
            copy.start()

    for copy in copies[2:]:
        copy.start()

    @pl.when(encoder)
    def _():
        copies[0].wait()
        levels = lax.broadcasted_iota(jnp.int32, (table.shape[1], times.shape[1]), 0)
        hot = [
            jnp.where(levels == times[m : m + 1, :], 1.0, 0.0).astype(LOW)
            for m in range(times.shape[0])
        ]
        copies[1].wait()
        embed = dot(table[...], jnp.concatenate(hot, axis=1), 1, 0).astype(LOW)
        embed_out[...] = embed
        copies[2].wait()
        copies[3].wait()
        united = side_by_side(inputs).astype(F32) + dot(w_skip[...], embed, 0, 0)
        normed = (united * norm_of(united)).astype(LOW)
        copies[4].wait()
        preact = dot(w_in[...], normed, 0, 0)
        active = (preact * sigmoid(preact)).astype(LOW)
        copies[5].wait()
        value_out[...] = (united + dot(w_out[...], active, 1, 0)).astype(LOW)

    @pl.when(jnp.logical_not(encoder))
    def _():
        for copy in copies[2:]:
            copy.wait()


def active_in(section):
    return pl.when(lax.axis_index("section") == section)


def early_body(upstream, w_out, low_out, grad_act_out):
    low = side_by_side(upstream)
    low_out[...] = low

    @active_in(3)
    def _():
        grad_act_out[...] = dot(w_out[...], low, 0, 0)


def back_through(grad_out, grad_act, united, slope, w_in):
    grad_pre = (grad_act * slope).astype(LOW)
    grad_norm = dot(w_in[...], grad_pre, 1, 0)
    recip = norm_of(united)
    along = jnp.mean(grad_norm * united, axis=0, keepdims=True)
    return (grad_out + recip * grad_norm - united * (recip * recip * recip * along)).astype(LOW)


def decode_body(
    received, embed, inputs, top_low, grad_act, w_skip, w_in,
    source_out, normed_out, united_out, slope_out, chain_out,
):
    source = jnp.where(lax.axis_index("section") >= 2, received[...], embed[...])
    source_out[...] = source
    united = side_by_side(inputs).astype(F32) + dot(w_skip[...], source, 0, 0)
    united_out[...] = united
    normed = (united * norm_of(united)).astype(LOW)
    normed_out[...] = normed
    preact = dot(w_in[...], normed, 0, 0)
    sigma = sigmoid(preact)
    slope = sigma * (1.0 + preact * (1.0 - sigma))
    slope_out[...] = slope

    @active_in(3)
    def _():
        chain_out[...] = back_through(
            top_low[...].astype(F32), grad_act[...], united, slope, w_in
        )


def back_body(chain, w_skip, back_out):
    @active_in(3)
    def _():
        back_out[...] = dot(w_skip[...], chain[...], 1, 0).astype(LOW)


def prior_body(chain_2, chain_3, w_skip, prior_out):
    @active_in(2)
    def _():
        back = dot(w_skip[...], chain_2[...], 1, 0).astype(LOW)
        prior_out[...] = (chain_2[...].astype(F32) + back.astype(F32)).astype(LOW)

    @active_in(3)
    def _():
        prior_out[...] = chain_3[...]


def tick_body(received, united, slope, w_in, w_out, chain_out):
    @active_in(2)
    def _():
        low = received[...]
        grad_act = dot(w_out[...], low, 0, 0)
        chain_out[...] = back_through(low.astype(F32), grad_act, united[...], slope[...], w_in)


def mirror_tick_body(
    received, w_mirror, united, slope, w_in, w_out, skip_far, chain_out, low_out, next_out,
):
    @active_in(1)
    def _():
        back = dot(w_mirror[...], received[...], 1, 0).astype(LOW)
        grad_out = received[...].astype(F32) + back.astype(F32)
        low = grad_out.astype(LOW)
        low_out[...] = low
        grad_act = dot(w_out[...], low, 0, 0)
        chain = back_through(grad_out, grad_act, united[...], slope[...], w_in)
        chain_out[...] = chain
        next_out[...] = (chain.astype(F32) + skip_far[...].astype(F32)).astype(LOW)


def pick_body(received, skip_far, low_1, low_2, top_low, grad_low_out):
    own = (received[...].astype(F32) + skip_far[...].astype(F32)).astype(LOW)
    section = lax.axis_index("section")
    own = jnp.where(section == 1, low_1[...], own)
    own = jnp.where(section == 2, low_2[...], own)
    grad_low_out[...] = jnp.where(section == 3, top_low[...], own)


def merge_body(late, middle, top, out):
    section = lax.axis_index("section")
    out[...] = jnp.where(section == 0, late[...], jnp.where(section == 3, top[...], middle[...]))


def own_body(low_1, low_2, out):
    out[...] = jnp.where(lax.axis_index("section") == 1, low_1[...], low_2[...])


def last_body(
    grad_low, received, skip_far, united, slope, w_in, w_out, source, chain_1, chain_2,
    chain_3, kept_out, keep_out, give_out,
):
    @active_in(0)
    def _():
        grad_out = received[...].astype(F32) + skip_far[...].astype(F32)
        grad_act = dot(w_out[...], grad_low[...], 0, 0)
        kept_out[...] = back_through(grad_out, grad_act, united[...], slope[...], w_in)

    for owner, chain in enumerate((chain_1, chain_2, chain_3), 1):

        @active_in(owner)
        def _():
            kept_out[...] = chain[...]

    product = dot(source[...], kept_out[...], 1, 1)
    size = keep_out.shape[1]
    first_core = lax.axis_index("dp") % 2 == 0
    for block in range(keep_out.shape[0]):
        start = 2 * block * size
        even = product[start : start + size, :]
        odd = product[start + size : start + 2 * size, :]
        keep_out[block] = jnp.where(first_core, even, odd)
        give_out[block] = jnp.where(first_core, odd, even).astype(LOW)


def join_body(keep, given, own_out, *piece_outs):
    chip = lax.axis_index("dp") // 2
    own_out[...] = keep[chip] + given[chip].astype(F32)
    for mask, piece_out in enumerate(piece_outs, 1):
        far = chip ^ mask
        piece_out[...] = (keep[far] + given[far].astype(F32)).astype(LOW)


def flatten(total, out, lanes, square):
    lanes[0] = total[:, :128]
    lanes[1] = total[:, 128:256]
    lanes[2] = jnp.concatenate([total[:, 256:], total[:, 256:]], axis=1)
    half = total.shape[0] // 2
    even = [lanes[part, pl.ds(0, half, stride=2), :] for part in range(3)]
    odd = [lanes[part, pl.ds(1, half, stride=2), :] for part in range(3)]
    lines = [
        even[0],
        even[1],
        jnp.concatenate([even[2][:, :64], odd[0][:, :64]], axis=1),
        jnp.concatenate([odd[0][:, 64:], odd[1][:, :64]], axis=1),
        jnp.concatenate([odd[1][:, 64:], odd[2][:, :64]], axis=1),
    ]
    for place, line in enumerate(lines):
        square[pl.ds(place, half, stride=5), :] = line
    for row in range(square.shape[0]):
        out[:, row * 128 : (row + 1) * 128] = square[row : row + 1, :]


def cut_body(w_in, w_out, own_in, own_out):
    part = own_in.shape[1]
    place = lax.axis_index("dp")
    for index in range(w_in.shape[1] // part):

        @pl.when(place == index)
        def _():
            columns = slice(index * part, (index + 1) * part)
            own_in[...] = w_in[:, columns]
            own_out[...] = w_out[:, columns]


def slice_forward_body(own_in, *refs):
    blocks, active_out, slope_out = refs[:-2], refs[-2], refs[-1]
    rows = blocks[0].shape[1]
    for place, block in enumerate(blocks):
        columns = slice(place * rows, (place + 1) * rows)
        preact = dot(own_in[...], block[...], 0, 0)
        sigma = sigmoid(preact)
        active_out[:, columns] = (preact * sigma).astype(LOW)
        slope_out[:, columns] = sigma * (1.0 + preact * (1.0 - sigma))


def slice_grad(own_out, active, slope, normed, low, first):
    rows = low[0].shape[1]
    columns = slice(first * rows, (first + len(low)) * rows)
    lows = jnp.concatenate([block[...] for block in low], axis=1)
    grad_pre = (dot(own_out[...], lows, 0, 0) * slope[:, columns]).astype(LOW)
    normeds = jnp.concatenate([block[...] for block in normed], axis=1)
    return dot(grad_pre, normeds, 1, 1), dot(active[:, columns], lows, 1, 1)


def half_grad_body(own_out, active, slope, *refs):
    half = (len(refs) - 2) // 2
    refs[-2][...], refs[-1][...] = slice_grad(
        own_out, active, slope, refs[:half], refs[half : 2 * half], 0
    )


def rest_grad_body(
    own_out, active, slope, sum_in, sum_out, normed_0, normed_1, low_0, low_1, own, piece_1,
    piece_2, piece_3, kept, in_out, out_out, skip_out, kept_out, lanes, square,
):
    span = kept_out.shape[2]
    for m in range(kept_out.shape[0]):
        kept_out[m] = kept[:, m * span : (m + 1) * span]
    total = own[...]
    for piece in (piece_1, piece_2, piece_3):
        total = total + piece[...].astype(F32)
    flatten(total, skip_out, lanes, square)
    first = active.shape[1] // normed_0.shape[1] - 2
    part_in, part_out = slice_grad(
        own_out, active, slope, (normed_0, normed_1), (low_0, low_1), first
    )
    in_out[...] = sum_in[...] + part_in
    out_out[...] = sum_out[...] + part_out


def hop(value, pairs):
    return lax.ppermute(value, "section", pairs)


def in_turn(near, swapped):
    return [*near[:3], *swapped[:3], near[3], swapped[3]]


def exchange(value, count, mask):
    return lax.ppermute(value, "dp", [(i, i ^ mask) for i in range(count)])


def from_next(value, sections, count, mask):
    pairs = [
        ((section + 1) * count + i, section * count + (i ^ mask))
        for section in sections
        for i in range(count)
    ]
    return lax.ppermute(value, ("section", "dp"), pairs)


def within(value, sections, count, mask):
    pairs = [
        (section * count + i, section * count + (i ^ mask))
        for section in sections
        for i in range(count)
    ]
    return lax.ppermute(value, ("section", "dp"), pairs)


def program(saved_inputs, timesteps, time_table, skip_weight, ff_in, ff_out, output_cotangent):
    section = lax.axis_index("section")
    count = lax.axis_size("dp")
    n_micro = saved_inputs.shape[1]
    width = saved_inputs.shape[3]
    span = saved_inputs.shape[2]
    rows = n_micro * span
    hidden = ff_in.shape[1]
    inputs = jnp.swapaxes(saved_inputs[0], 1, 2)
    upstream = jnp.swapaxes(output_cotangent, 1, 2)
    table = time_table.T
    w_skip = skip_weight[0]
    w_in = ff_in[0].T
    w_out = ff_out[0].T
    low = ((width, rows), LOW)
    wide = ((hidden, rows), F32)

    distant = (timesteps, table, w_skip, inputs, w_in, w_out)
    embed, value, w_skip, inputs, w_in, w_out = call(
        encode_body, [low, low] + [(arg.shape, arg.dtype) for arg in distant[2:]],
        *distant,
        scratch=[pltpu.VMEM(arg.shape, arg.dtype) for arg in distant[:2]]
        + [pltpu.SemaphoreType.DMA((len(distant),))],
        far=range(len(distant)),
    )
    received = hop(value, [(0, 3), (1, 2)])
    top_low, grad_act = call(early_body, [low, wide], upstream, w_out)
    source, normed, united, slope, chain_3 = call(
        decode_body, [low, low, ((width, rows), F32), wide, low],
        received, embed, inputs, top_low, grad_act, w_skip, w_in,
    )
    chain = hop(chain_3, [(3, 2)])
    w_mirror = hop(w_skip, [(2, 1)])
    (back,) = call(back_body, [low], chain_3, w_skip)
    skip_far = hop(back, [(3, 0)])
    skip_next = hop(back, [(3, 1)])
    low_2 = chain
    (chain_2,) = call(tick_body, [low], chain, united, slope, w_in, w_out)
    chain = hop(chain_2, [(2, 1)])
    (prior,) = call(prior_body, [low], chain_2, chain_3, w_skip)
    chain_1, low_1, ahead = call(
        mirror_tick_body, [low, low, low],
        chain, w_mirror, united, slope, w_in, w_out, skip_next,
    )
    chain = hop(chain_1, [(1, 0)])
    (grad_low,) = call(pick_body, [low], chain, skip_far, low_1, low_2, top_low)

    if not (count == 8 and count * rows <= 4096 and width % 128 == 64 and width // 128 == 2):
        return by_reduction(
            section, chain, skip_far, united, slope, w_in, w_out, source, normed, grad_low,
            (chain_1, chain_2, chain_3), saved_inputs.shape,
        )

    part = hidden // count
    own_in, own_out = call(cut_body, [((width, part), LOW)] * 2, w_in, w_out)
    normed_near = [normed] + [exchange(normed, count, m) for m in (2, 6, 4)]
    normed_all = in_turn(
        normed_near,
        [exchange(x, count, 1) for x in normed_near],
    )
    active_all, slope_all = call(
        slice_forward_body,
        [((part, count * rows), LOW), ((part, count * rows), F32)], own_in, *normed_all,
    )
    tops = {mask: within(top_low, [3], count, mask) for mask in (2, 4)}
    tops[6] = within(tops[4], [3], count, 2)
    (own_low,) = call(own_body, [low], low_1, low_2)
    middle = {m: from_next(prior, [1, 2], count, m) for m in (2, 6)}
    middle[4] = within(own_low, [1, 2], count, 4)
    late = {m: within(grad_low, [0], count, m) for m in (2, 4)}
    late[6] = from_next(ahead, [0], count, 6)
    low_2, low_4, low_6 = (
        call(merge_body, [low], late[mask], middle[mask], tops[mask])[0]
        for mask in (2, 4, 6)
    )
    low_near = [grad_low, low_2, low_6, low_4]
    low_all = in_turn(low_near, [exchange(x, count, 1) for x in low_near])
    block = (count // 2, width // count, width)
    kept, keep, give = call(
        last_body, [low, (block, F32), (block, LOW)],
        grad_low, chain, skip_far, united, slope, w_in, w_out, source, chain_1, chain_2,
        chain_3,
    )
    given = exchange(give, count, 1)
    piece = block[1:]
    own, *pieces = call(
        join_body, [(piece, F32)] + [(piece, LOW)] * (count // 2 - 1),
        keep, given,
    )
    pieces = [exchange(value, count, 2 * i) for i, value in enumerate(pieces, 1)]
    grads = ((part, width), F32)
    half = 6
    sums = call(
        half_grad_body, [grads] * 2,
        own_out, active_all, slope_all, *normed_all[:half], *low_all[:half],
    )
    grad_in, grad_out_w, grad_skip, kept = call(
        rest_grad_body,
        [grads, grads, ((1, piece[0] * piece[1]), F32), ((n_micro, width, span), LOW)],
        own_out, active_all, slope_all, *sums, *normed_all[half:], *low_all[half:], own, *pieces,
        kept,
        scratch=[
            pltpu.VMEM((3, piece[0], 128), F32),
            pltpu.VMEM((piece[0] * piece[1] // 128, 128), F32),
        ],
    )
    kept = jnp.swapaxes(kept, 1, 2)
    return (kept[None], grad_skip, grad_in[None], grad_out_w[None])


def by_reduction(
    section, chain, skip_far, united, slope, w_in, w_out, source, normed, grad_low, chains,
    shape,
):
    grad_out = chain.astype(F32) + skip_far.astype(F32)
    grad_pre = (dot(w_out, grad_low, 0, 0) * slope).astype(LOW)
    preact = dot(w_in, normed, 0, 0)
    active = (preact * jax.nn.sigmoid(preact)).astype(LOW)
    own_pre = (dot(w_out, grad_out.astype(LOW), 0, 0) * slope).astype(LOW)
    grad_norm = dot(w_in, own_pre, 1, 0)
    recip = norm_of(united)
    along = jnp.mean(grad_norm * united, axis=0, keepdims=True)
    kept = (grad_out + recip * grad_norm - united * (recip * recip * recip * along)).astype(LOW)
    for owner, other in enumerate(chains, 1):
        kept = jnp.where(section == owner, other, kept)
    grad_in, grad_out_w, grad_skip = (
        lax.psum_scatter(value, "dp", scatter_dimension=0, tiled=True)
        for value in (
            dot(grad_pre, normed, 1, 1),
            dot(active, grad_low, 1, 1),
            dot(source, kept, 1, 1).reshape(-1),
        )
    )
    kept = kept.reshape(shape[3], shape[1], shape[2]).transpose(1, 2, 0)
    return (kept[None], grad_skip[None], grad_in[None], grad_out_w[None])


def solution(mesh):
    in_specs = (
        P("section", None, "dp", None),
        P(None, "dp"),
        P(),
        P("section", None, None),
        P("section", None, None),
        P("section", None, None),
        P(None, "dp", None),
    )
    out_specs = (
        P("section", None, "dp", None),
        P("section", "dp"),
        P("section", "dp", None),
        P("section", "dp", None),
    )
    return jax.shard_map(program, mesh=mesh, in_specs=in_specs, out_specs=out_specs, check_vma=False)
```

```python
import jax
import jax.numpy as jnp
from jax import lax
from jax.experimental import pallas as pl
from jax.experimental.pallas import tpu as pltpu
from jax.sharding import PartitionSpec as P


EPS = 1e-06
LOW = jnp.bfloat16
F32 = jnp.float32
VMEM_BYTES = 20 * 1024 * 1024


def contract(left, right, dims):
    return lax.dot_general(left, right, ((dims[0], dims[1]), ((), ())), preferred_element_type=F32)


def dot(left, right, on_left, on_right):
    return contract(left, right, ((on_left,), (on_right,)))


def call(body, outs, *args, scratch=(), far=()):
    places = [
        pltpu.SMEM if arg.ndim == 1 else pltpu.HBM if index in far else pltpu.VMEM
        for index, arg in enumerate(args)
    ]
    args = [
        pltpu.with_memory_space_constraint(arg, pltpu.HBM) if index in far else arg
        for index, arg in enumerate(args)
    ]
    return pl.pallas_call(
        body,
        out_shape=[jax.ShapeDtypeStruct(shape, kind) for shape, kind in outs],
        in_specs=[pl.BlockSpec(memory_space=place) for place in places],
        out_specs=[pl.BlockSpec(memory_space=pltpu.VMEM) for _ in outs],
        scratch_shapes=list(scratch),
        compiler_params=pltpu.CompilerParams(vmem_limit_bytes=VMEM_BYTES),
    )(*args)


def side_by_side(ref):
    return jnp.concatenate([ref[m] for m in range(ref.shape[0])], axis=1)


def norm_of(united):
    return lax.rsqrt(jnp.mean(united * united, axis=0, keepdims=True) + EPS)


def sigmoid(value):
    return 1.0 / (1.0 + jnp.exp(-value))


def encode_body(*refs):
    distant, (embed_out, value_out), kept, local, sems = (
        refs[:6], refs[6:8], refs[8:12], refs[12:14], refs[14],
    )
    local = (*local, *kept)
    copies = [
        pltpu.make_async_copy(source, target, sems.at[index])
        for index, (source, target) in enumerate(zip(distant, local))
    ]
    times, table, w_skip, inputs, w_in, w_out = local
    encoder = lax.axis_index("section") < 2

    @pl.when(encoder)
    def _():
        for copy in copies[:2]:
            copy.start()

    for copy in copies[2:]:
        copy.start()

    @pl.when(encoder)
    def _():
        copies[0].wait()
        levels = lax.broadcasted_iota(jnp.int32, (table.shape[1], times.shape[1]), 0)
        hot = [
            jnp.where(levels == times[m : m + 1, :], 1.0, 0.0).astype(LOW)
            for m in range(times.shape[0])
        ]
        copies[1].wait()
        embed = dot(table[...], jnp.concatenate(hot, axis=1), 1, 0).astype(LOW)
        embed_out[...] = embed
        copies[2].wait()
        copies[3].wait()
        united = side_by_side(inputs).astype(F32) + dot(w_skip[...], embed, 0, 0)
        normed = (united * norm_of(united)).astype(LOW)
        copies[4].wait()
        preact = dot(w_in[...], normed, 0, 0)
        active = (preact * sigmoid(preact)).astype(LOW)
        copies[5].wait()
        value_out[...] = (united + dot(w_out[...], active, 1, 0)).astype(LOW)

    @pl.when(jnp.logical_not(encoder))
    def _():
        for copy in copies[2:]:
            copy.wait()


def active_in(section):
    return pl.when(lax.axis_index("section") == section)


def early_body(upstream, w_out, low_out, grad_act_out):
    low = side_by_side(upstream)
    low_out[...] = low

    @active_in(3)
    def _():
        grad_act_out[...] = dot(w_out[...], low, 0, 0)


def back_through(grad_out, grad_act, united, slope, w_in):
    grad_pre = (grad_act * slope).astype(LOW)
    grad_norm = dot(w_in[...], grad_pre, 1, 0)
    recip = norm_of(united)
    along = jnp.mean(grad_norm * united, axis=0, keepdims=True)
    return (grad_out + recip * grad_norm - united * (recip * recip * recip * along)).astype(LOW)


def decode_body(
    received, embed, inputs, top_low, grad_act, w_skip, w_in,
    source_out, normed_out, united_out, slope_out, chain_out,
):
    source = jnp.where(lax.axis_index("section") >= 2, received[...], embed[...])
    source_out[...] = source
    united = side_by_side(inputs).astype(F32) + dot(w_skip[...], source, 0, 0)
    united_out[...] = united
    normed = (united * norm_of(united)).astype(LOW)
    normed_out[...] = normed
    preact = dot(w_in[...], normed, 0, 0)
    sigma = sigmoid(preact)
    slope = sigma * (1.0 + preact * (1.0 - sigma))
    slope_out[...] = slope

    @active_in(3)
    def _():
        chain_out[...] = back_through(
            top_low[...].astype(F32), grad_act[...], united, slope, w_in
        )


def back_body(chain, w_skip, back_out):
    @active_in(3)
    def _():
        back_out[...] = dot(w_skip[...], chain[...], 1, 0).astype(LOW)


def prior_body(chain_2, chain_3, w_skip, prior_out):
    @active_in(2)
    def _():
        back = dot(w_skip[...], chain_2[...], 1, 0).astype(LOW)
        prior_out[...] = (chain_2[...].astype(F32) + back.astype(F32)).astype(LOW)

    @active_in(3)
    def _():
        prior_out[...] = chain_3[...]


def tick_body(received, united, slope, w_in, w_out, chain_out):
    @active_in(2)
    def _():
        low = received[...]
        grad_act = dot(w_out[...], low, 0, 0)
        chain_out[...] = back_through(low.astype(F32), grad_act, united[...], slope[...], w_in)


def mirror_tick_body(
    received, w_mirror, united, slope, w_in, w_out, skip_far, chain_out, low_out, next_out,
):
    @active_in(1)
    def _():
        back = dot(w_mirror[...], received[...], 1, 0).astype(LOW)
        grad_out = received[...].astype(F32) + back.astype(F32)
        low = grad_out.astype(LOW)
        low_out[...] = low
        grad_act = dot(w_out[...], low, 0, 0)
        chain = back_through(grad_out, grad_act, united[...], slope[...], w_in)
        chain_out[...] = chain
        next_out[...] = (chain.astype(F32) + skip_far[...].astype(F32)).astype(LOW)


def pick_body(received, skip_far, low_1, low_2, top_low, grad_low_out):
    own = (received[...].astype(F32) + skip_far[...].astype(F32)).astype(LOW)
    section = lax.axis_index("section")
    own = jnp.where(section == 1, low_1[...], own)
    own = jnp.where(section == 2, low_2[...], own)
    grad_low_out[...] = jnp.where(section == 3, top_low[...], own)


def merge_body(late, middle, top, out):
    section = lax.axis_index("section")
    out[...] = jnp.where(section == 0, late[...], jnp.where(section == 3, top[...], middle[...]))


def own_body(low_1, low_2, out):
    out[...] = jnp.where(lax.axis_index("section") == 1, low_1[...], low_2[...])


def last_body(
    grad_low, received, skip_far, united, slope, w_in, w_out, source, chain_1, chain_2,
    chain_3, kept_out, keep_out, give_out,
):
    @active_in(0)
    def _():
        grad_out = received[...].astype(F32) + skip_far[...].astype(F32)
        grad_act = dot(w_out[...], grad_low[...], 0, 0)
        kept_out[...] = back_through(grad_out, grad_act, united[...], slope[...], w_in)

    for owner, chain in enumerate((chain_1, chain_2, chain_3), 1):

        @active_in(owner)
        def _():
            kept_out[...] = chain[...]

    product = dot(source[...], kept_out[...], 1, 1)
    size = keep_out.shape[1]
    first_core = lax.axis_index("dp") % 2 == 0
    for block in range(keep_out.shape[0]):
        start = 2 * block * size
        even = product[start : start + size, :]
        odd = product[start + size : start + 2 * size, :]
        keep_out[block] = jnp.where(first_core, even, odd)
        give_out[block] = jnp.where(first_core, odd, even).astype(LOW)


def join_body(keep, given, own_out, *piece_outs):
    chip = lax.axis_index("dp") // 2
    own_out[...] = keep[chip] + given[chip].astype(F32)
    for mask, piece_out in enumerate(piece_outs, 1):
        far = chip ^ mask
        piece_out[...] = (keep[far] + given[far].astype(F32)).astype(LOW)


def flatten(total, out, lanes, square):
    lanes[0] = total[:, :128]
    lanes[1] = total[:, 128:256]
    lanes[2] = jnp.concatenate([total[:, 256:], total[:, 256:]], axis=1)
    half = total.shape[0] // 2
    even = [lanes[part, pl.ds(0, half, stride=2), :] for part in range(3)]
    odd = [lanes[part, pl.ds(1, half, stride=2), :] for part in range(3)]
    lines = [
        even[0],
        even[1],
        jnp.concatenate([even[2][:, :64], odd[0][:, :64]], axis=1),
        jnp.concatenate([odd[0][:, 64:], odd[1][:, :64]], axis=1),
        jnp.concatenate([odd[1][:, 64:], odd[2][:, :64]], axis=1),
    ]
    for place, line in enumerate(lines):
        square[pl.ds(place, half, stride=5), :] = line
    for row in range(square.shape[0]):
        out[:, row * 128 : (row + 1) * 128] = square[row : row + 1, :]


def cut_body(w_in, w_out, own_in, own_out):
    part = own_in.shape[1]
    place = lax.axis_index("dp")
    for index in range(w_in.shape[1] // part):

        @pl.when(place == index)
        def _():
            columns = slice(index * part, (index + 1) * part)
            own_in[...] = w_in[:, columns]
            own_out[...] = w_out[:, columns]


def slice_forward_body(own_in, *refs):
    blocks, active_out, slope_out = refs[:-2], refs[-2], refs[-1]
    rows = blocks[0].shape[1]
    for place, block in enumerate(blocks):
        columns = slice(place * rows, (place + 1) * rows)
        preact = dot(own_in[...], block[...], 0, 0)
        sigma = sigmoid(preact)
        active_out[:, columns] = (preact * sigma).astype(LOW)
        slope_out[:, columns] = sigma * (1.0 + preact * (1.0 - sigma))


def slice_grad(own_out, active, slope, normed, low, first):
    rows = low[0].shape[1]
    columns = slice(first * rows, (first + len(low)) * rows)
    lows = jnp.concatenate([block[...] for block in low], axis=1)
    grad_pre = (dot(own_out[...], lows, 0, 0) * slope[:, columns]).astype(LOW)
    normeds = jnp.concatenate([block[...] for block in normed], axis=1)
    return dot(grad_pre, normeds, 1, 1), dot(active[:, columns], lows, 1, 1)


def half_grad_body(own_out, active, slope, *refs):
    half = (len(refs) - 2) // 2
    refs[-2][...], refs[-1][...] = slice_grad(
        own_out, active, slope, refs[:half], refs[half : 2 * half], 0
    )


def rest_grad_body(
    own_out, active, slope, sum_in, sum_out, normed_0, normed_1, low_0, low_1, own, piece_1,
    piece_2, piece_3, kept, in_out, out_out, skip_out, kept_out, lanes, square,
):
    span = kept_out.shape[2]
    for m in range(kept_out.shape[0]):
        kept_out[m] = kept[:, m * span : (m + 1) * span]
    total = own[...]
    for piece in (piece_1, piece_2, piece_3):
        total = total + piece[...].astype(F32)
    flatten(total, skip_out, lanes, square)
    first = active.shape[1] // normed_0.shape[1] - 2
    part_in, part_out = slice_grad(
        own_out, active, slope, (normed_0, normed_1), (low_0, low_1), first
    )
    in_out[...] = sum_in[...] + part_in
    out_out[...] = sum_out[...] + part_out


def hop(value, pairs):
    return lax.ppermute(value, "section", pairs)


def in_turn(near, swapped):
    return [*near[:3], *swapped[:3], near[3], swapped[3]]


def exchange(value, count, mask):
    return lax.ppermute(value, "dp", [(i, i ^ mask) for i in range(count)])


def from_next(value, sections, count, mask):
    pairs = [
        ((section + 1) * count + i, section * count + (i ^ mask))
        for section in sections
        for i in range(count)
    ]
    return lax.ppermute(value, ("section", "dp"), pairs)


def within(value, sections, count, mask):
    pairs = [
        (section * count + i, section * count + (i ^ mask))
        for section in sections
        for i in range(count)
    ]
    return lax.ppermute(value, ("section", "dp"), pairs)


def program(saved_inputs, timesteps, time_table, skip_weight, ff_in, ff_out, output_cotangent):
    section = lax.axis_index("section")
    count = lax.axis_size("dp")
    n_micro = saved_inputs.shape[1]
    width = saved_inputs.shape[3]
    span = saved_inputs.shape[2]
    rows = n_micro * span
    hidden = ff_in.shape[1]
    inputs = jnp.swapaxes(saved_inputs[0], 1, 2)
    upstream = jnp.swapaxes(output_cotangent, 1, 2)
    table = time_table.T
    w_skip = skip_weight[0]
    w_in = ff_in[0].T
    w_out = ff_out[0].T
    low = ((width, rows), LOW)
    wide = ((hidden, rows), F32)

    distant = (timesteps, table, w_skip, inputs, w_in, w_out)
    embed, value, w_skip, inputs, w_in, w_out = call(
        encode_body, [low, low] + [(arg.shape, arg.dtype) for arg in distant[2:]],
        *distant,
        scratch=[pltpu.VMEM(arg.shape, arg.dtype) for arg in distant[:2]]
        + [pltpu.SemaphoreType.DMA((len(distant),))],
        far=range(len(distant)),
    )
    received = hop(value, [(0, 3), (1, 2)])
    top_low, grad_act = call(early_body, [low, wide], upstream, w_out)
    source, normed, united, slope, chain_3 = call(
        decode_body, [low, low, ((width, rows), F32), wide, low],
        received, embed, inputs, top_low, grad_act, w_skip, w_in,
    )
    chain = hop(chain_3, [(3, 2)])
    w_mirror = hop(w_skip, [(2, 1)])
    (back,) = call(back_body, [low], chain_3, w_skip)
    skip_far = hop(back, [(3, 0)])
    skip_next = hop(back, [(3, 1)])
    low_2 = chain
    (chain_2,) = call(tick_body, [low], chain, united, slope, w_in, w_out)
    chain = hop(chain_2, [(2, 1)])
    (prior,) = call(prior_body, [low], chain_2, chain_3, w_skip)
    chain_1, low_1, ahead = call(
        mirror_tick_body, [low, low, low],
        chain, w_mirror, united, slope, w_in, w_out, skip_next,
    )
    chain = hop(chain_1, [(1, 0)])
    (grad_low,) = call(pick_body, [low], chain, skip_far, low_1, low_2, top_low)

    if not (count == 8 and count * rows <= 4096 and width % 128 == 64 and width // 128 == 2):
        return by_reduction(
            section, chain, skip_far, united, slope, w_in, w_out, source, normed, grad_low,
            (chain_1, chain_2, chain_3), saved_inputs.shape,
        )

    part = hidden // count
    own_in, own_out = call(cut_body, [((width, part), LOW)] * 2, w_in, w_out)
    normed_near = [normed] + [exchange(normed, count, m) for m in (2, 4, 6)]
    normed_all = in_turn(
        normed_near,
        [exchange(x, count, 1) for x in normed_near],
    )
    active_all, slope_all = call(
        slice_forward_body,
        [((part, count * rows), LOW), ((part, count * rows), F32)], own_in, *normed_all,
    )
    tops = {mask: within(top_low, [3], count, mask) for mask in (2, 4)}
    tops[6] = within(tops[4], [3], count, 2)
    (own_low,) = call(own_body, [low], low_1, low_2)
    middle = {m: from_next(prior, [1, 2], count, m) for m in (2, 6)}
    middle[4] = within(own_low, [1, 2], count, 4)
    late = {m: from_next(ahead, [0], count, m) for m in (2, 6)}
    late[4] = within(grad_low, [0], count, 4)
    low_2, low_4, low_6 = (
        call(merge_body, [low], late[mask], middle[mask], tops[mask])[0]
        for mask in (2, 4, 6)
    )
    low_near = [grad_low, low_2, low_4, low_6]
    low_all = in_turn(low_near, [exchange(x, count, 1) for x in low_near])
    block = (count // 2, width // count, width)
    kept, keep, give = call(
        last_body, [low, (block, F32), (block, LOW)],
        grad_low, chain, skip_far, united, slope, w_in, w_out, source, chain_1, chain_2,
        chain_3,
    )
    given = exchange(give, count, 1)
    piece = block[1:]
    own, *pieces = call(
        join_body, [(piece, F32)] + [(piece, LOW)] * (count // 2 - 1),
        keep, given,
    )
    pieces = [exchange(value, count, 2 * i) for i, value in enumerate(pieces, 1)]
    grads = ((part, width), F32)
    half = 6
    sums = call(
        half_grad_body, [grads] * 2,
        own_out, active_all, slope_all, *normed_all[:half], *low_all[:half],
    )
    grad_in, grad_out_w, grad_skip, kept = call(
        rest_grad_body,
        [grads, grads, ((1, piece[0] * piece[1]), F32), ((n_micro, width, span), LOW)],
        own_out, active_all, slope_all, *sums, *normed_all[half:], *low_all[half:], own, *pieces,
        kept,
        scratch=[
            pltpu.VMEM((3, piece[0], 128), F32),
            pltpu.VMEM((piece[0] * piece[1] // 128, 128), F32),
        ],
    )
    kept = jnp.swapaxes(kept, 1, 2)
    return (kept[None], grad_skip, grad_in[None], grad_out_w[None])


def by_reduction(
    section, chain, skip_far, united, slope, w_in, w_out, source, normed, grad_low, chains,
    shape,
):
    grad_out = chain.astype(F32) + skip_far.astype(F32)
    grad_pre = (dot(w_out, grad_low, 0, 0) * slope).astype(LOW)
    preact = dot(w_in, normed, 0, 0)
    active = (preact * jax.nn.sigmoid(preact)).astype(LOW)
    own_pre = (dot(w_out, grad_out.astype(LOW), 0, 0) * slope).astype(LOW)
    grad_norm = dot(w_in, own_pre, 1, 0)
    recip = norm_of(united)
    along = jnp.mean(grad_norm * united, axis=0, keepdims=True)
    kept = (grad_out + recip * grad_norm - united * (recip * recip * recip * along)).astype(LOW)
    for owner, other in enumerate(chains, 1):
        kept = jnp.where(section == owner, other, kept)
    grad_in, grad_out_w, grad_skip = (
        lax.psum_scatter(value, "dp", scatter_dimension=0, tiled=True)
        for value in (
            dot(grad_pre, normed, 1, 1),
            dot(active, grad_low, 1, 1),
            dot(source, kept, 1, 1).reshape(-1),
        )
    )
    kept = kept.reshape(shape[3], shape[1], shape[2]).transpose(1, 2, 0)
    return (kept[None], grad_skip[None], grad_in[None], grad_out_w[None])


def solution(mesh):
    in_specs = (
        P("section", None, "dp", None),
        P(None, "dp"),
        P(),
        P("section", None, None),
        P("section", None, None),
        P("section", None, None),
        P(None, "dp", None),
    )
    out_specs = (
        P("section", None, "dp", None),
        P("section", "dp"),
        P("section", "dp", None),
        P("section", "dp", None),
    )
    return jax.shard_map(program, mesh=mesh, in_specs=in_specs, out_specs=out_specs, check_vma=False)
```
